32 devices in a mesh: seq: 4 (over y, x), fsdp: 8 (over z, core).
Axes of the slice: x: 2, y: 2, z: 4, core: 2. Of those that a mesh axis runs over, the one named last changes fastest.
Arguments:
- tokens: bfloat16 [8, 1024, 1024], P('fsdp', 'seq'), may hold values from -6 to 6
- lengths: int32 [8, 8], P('fsdp'), may hold values from 1 to 512, 1024 in all within a row
- packing: int32 [8, 1024], P('fsdp'), may hold values from 0 to 1023, as said below
- norm_in: bfloat16 [1024], P('fsdp'), may hold values from 0.25 to 1.75
- w_query: bfloat16 [1024, 2048], P('fsdp'), may hold values from -0.1875 to 0.1875
- key_projection: bfloat16 [1024, 1024], P('fsdp'), may hold values from -0.1875 to 0.1875
- value_projection: bfloat16 [1024, 1024], P('fsdp'), may hold values from -0.1875 to 0.1875
- norm_query: bfloat16 [128], P('fsdp'), may hold values from 1 to 1.796875
- norm_key: bfloat16 [128], P('fsdp'), may hold values from 1 to 1.796875
- w_out: bfloat16 [2048, 1024], P('fsdp'), may hold values from -1 to 1
- norm_post: bfloat16 [1024], P('fsdp'), may hold values from 0.25 to 1.75
- w_gate: bfloat16 [1024, 3072], P('fsdp'), may hold values from -0.1875 to 0.1875
- w_up: bfloat16 [1024, 3072], P('fsdp'), may hold values from -0.1875 to 0.1875
- w_down: bfloat16 [3072, 1024], P('fsdp'), may hold values from -0.109375 to 0.109375
- cotangent: bfloat16 [8, 1024, 1024], P('fsdp', 'seq'), may hold values from -6 to 6
Outputs:
- output: bfloat16 [8, 1024, 1024], P('fsdp', 'seq')
- input_grad: bfloat16 [8, 1024, 1024], P('fsdp', 'seq')
- grad_norm_in: float32 [1024], P('fsdp')
- grad_w_query: float32 [1024, 2048], P('fsdp')
- grad_w_key: float32 [1024, 1024], P('fsdp')
- grad_w_value: float32 [1024, 1024], P('fsdp')
- grad_norm_query: float32 [128], P('fsdp')
- grad_norm_key: float32 [128], P('fsdp')
- grad_w_out: float32 [2048, 1024], P('fsdp')
- grad_norm_post: float32 [1024], P('fsdp')
- grad_w_gate: float32 [1024, 3072], P('fsdp')
- grad_w_up: float32 [1024, 3072], P('fsdp')
- grad_w_down: float32 [3072, 1024], P('fsdp')
The draws below stay inside these ranges and needn't reach their ends.
Inputs may be any that keep to these rules, and one draw needn't show every extreme that they name: The 8 lengths of each row add up to 1024, and the longest is exactly 512. Each row of packing names every token of its row once. Of the given-order positions s * 256 to (s + 1) * 256 - 1, exactly 64 are named in each aligned block of 256 packed positions.
All inputs are finite; a program needn't handle non-finite values.
Results may differ from the reference program's by a relative error of at most 0.02.
Values may be sent and summed in bfloat16 or wider, within the bound.
A program may use at most 192 MiB of HBM per device.

```python
import math
import jax
import jax.numpy as jnp
import numpy as np
from jax import lax

MODEL_WIDTH = 1024
HQ = 16
KEY_VALUE_HEADS = 8
HEAD_SIZE = 128
FF = 3072
TOK_DEV = 256
DOCUMENT_COUNT = 8
PACKED_ROWS = 8
ROW_TOKENS = 1024
LONGEST_LENGTH = 512
N_SEQ = 4


def shuffled_row(key):
    group = TOK_DEV // N_SEQ
    key_source, key_place = jax.random.split(key)
    source_perms = jax.vmap(lambda sub: jax.random.permutation(sub, jnp.arange(TOK_DEV, dtype=jnp.int32)))(jax.random.split(key_source, N_SEQ))
    place_perms = jax.vmap(lambda sub: jax.random.permutation(sub, jnp.arange(TOK_DEV, dtype=jnp.int32)))(jax.random.split(key_place, N_SEQ))
    target = jnp.arange(N_SEQ, dtype=jnp.int32)[:, None, None]
    source = jnp.arange(N_SEQ, dtype=jnp.int32)[None, :, None]
    member = jnp.arange(group, dtype=jnp.int32)[None, None, :]
    target_b = jnp.broadcast_to(target, (N_SEQ, N_SEQ, group))
    source_b = jnp.broadcast_to(source, (N_SEQ, N_SEQ, group))
    member_b = jnp.broadcast_to(member, (N_SEQ, N_SEQ, group))
    token_positions = target_b * TOK_DEV + place_perms[target_b, source_b * group + member_b]
    value_tensor = source_b * TOK_DEV + source_perms[source_b, target_b * group + member_b]
    filled_rows = jnp.zeros((ROW_TOKENS,), jnp.int32).at[token_positions.reshape(-1)].set(value_tensor.reshape(-1).astype(jnp.int32))
    return filled_rows


def draw_packing(key, part):
    return jax.vmap(shuffled_row)(jax.random.split(jax.random.fold_in(key, 17), PACKED_ROWS)).astype(jnp.int32)


def with_spikes(values, stream_key, source, target, parts, factor):
    owner, partner = [(jnp.arange(values.shape[axis_at]) // (values.shape[axis_at] // parts)).reshape([-1 if axis == axis_at else 1 for axis in range(values.ndim)]) for axis_at in (source, target)]
    chosen = jax.random.permutation(stream_key, parts)[partner]
    strong = (owner == chosen) | (owner == (partner + parts // 2) % parts)
    return jnp.where(strong, factor * values, values)


def block_levels(key, shape, cuts, least, high):
    gain, own = 1.0, jax.random.fold_in(key, 6)
    for position, shards_of in cuts:
        heights = jnp.exp(jax.random.uniform(jax.random.fold_in(own, position), (shards_of,), jnp.float32, least / len(cuts), high / len(cuts)))
        gain = gain * jnp.repeat(heights, shape[position] // shards_of).reshape([-1 if axis == position else 1 for axis in range(len(shape))])
    return gain


def profile(number_of, total, most, lean):
    weights = [(1 << 20) // math.isqrt(standing ** lean) + 1 for standing in range(2, number_of + 1)]
    spare, given = total - most - (number_of - 1), [1] * (number_of - 1)
    while spare > 0:
        candidates = [i for i in range(number_of - 1) if given[i] < most]
        pool, budget = sum([weights[i] for i in candidates]), spare
        for i in candidates:
            more = min(most - given[i], max(1, budget * weights[i] // pool), spare)
            given[i] = given[i] + more
            spare = spare - more
    return np.array([most] + given)


def uneven(stream_key, number_of, total, most, slope):
    if number_of == 2:
        one = jax.random.randint(stream_key, (), max(1, total - most), min(most, total - 1) + 1)
        return jnp.stack([one, total - one])
    sizes = jnp.asarray(profile(number_of, total, most, slope), jnp.int32)
    pairs = (number_of - 1) // 2
    giver, sink = sizes[1:1 + 2 * pairs:2], sizes[2:2 + 2 * pairs:2]
    room = jnp.minimum(giver - 1, most - sink)
    shifted = jax.random.randint(jax.random.fold_in(stream_key, 1), (pairs,), 0, 1 << 20) % (room + 1)
    sizes = sizes.at[1:1 + 2 * pairs:2].set(giver - shifted).at[2:2 + 2 * pairs:2].set(sink + shifted)
    return sizes[jax.random.permutation(jax.random.fold_in(stream_key, 2), number_of)]


def scatter_about(stream_key, dims, width, bound, cuts=(), kind=jnp.bfloat16):
    factor_of = block_levels(stream_key, dims, cuts, -0.22, 0.18) if cuts else 1.0
    entries = jax.random.normal(stream_key, dims, jnp.float32) * width * factor_of
    return jnp.minimum(jnp.maximum(entries, -bound), bound).astype(kind)


def gaussian_with(key, extent, scale, limit, cuts, heavy, kind=jnp.bfloat16):
    values = scale * jax.random.normal(key, extent, jnp.float32)
    if cuts:
        values = values * block_levels(key, extent, cuts, -0.22, 0.18)
    return jnp.clip(with_spikes(values, jax.random.fold_in(key, 3), *heavy), -limit, limit).astype(kind)


def setup_inputs(seed: int = 0) -> dict:
    seeds = jax.random.split(jax.random.key(seed), 16)
    return {
        "tokens": gaussian_with(seeds[0], (PACKED_ROWS, ROW_TOKENS, MODEL_WIDTH), 1.0, 6.0, ((0, 8), (1, 4)), (0, 2, 8, 2.0)),
        "lengths": jax.vmap(lambda own: uneven(own, DOCUMENT_COUNT, ROW_TOKENS, LONGEST_LENGTH, 2))(jax.random.split(seeds[1], PACKED_ROWS)).reshape((PACKED_ROWS, DOCUMENT_COUNT)).astype(jnp.int32),
        "packing": draw_packing(jax.random.fold_in(seeds[15], 71), 0),
        "norm_in": jnp.clip(1.0 + 0.15 * jax.random.normal(seeds[3], (MODEL_WIDTH,), jnp.float32), 0.25, 1.75).astype(jnp.bfloat16),
        "w_query": scatter_about(seeds[4], (MODEL_WIDTH, HQ * HEAD_SIZE), MODEL_WIDTH ** -0.5, 0.1875, ((0, 8),)),
        "key_projection": scatter_about(seeds[5], (MODEL_WIDTH, KEY_VALUE_HEADS * HEAD_SIZE), MODEL_WIDTH ** -0.5, 0.1875, ((0, 8),)),
        "value_projection": scatter_about(seeds[6], (MODEL_WIDTH, KEY_VALUE_HEADS * HEAD_SIZE), MODEL_WIDTH ** -0.5, 0.1875, ((0, 8),)),
        "norm_query": jnp.clip(1.0 + 0.796875 * jax.random.uniform(seeds[7], (HEAD_SIZE,), jnp.float32) ** block_levels(seeds[7], (HEAD_SIZE,), ((0, 8),), -0.2, 0.2), 1.0, 1.796875).astype(jnp.bfloat16),
        "norm_key": jnp.clip(1.0 + 0.796875 * jax.random.uniform(seeds[8], (HEAD_SIZE,), jnp.float32) ** block_levels(seeds[8], (HEAD_SIZE,), ((0, 8),), -0.2, 0.2), 1.0, 1.796875).astype(jnp.bfloat16),
        "w_out": scatter_about(seeds[9], (HQ * HEAD_SIZE, MODEL_WIDTH), (HQ * HEAD_SIZE // 64) ** -0.5, 1.0, ((0, 8),)),
        "norm_post": jnp.clip(1.0 + 0.15 * jax.random.normal(seeds[10], (MODEL_WIDTH,), jnp.float32), 0.25, 1.75).astype(jnp.bfloat16),
        "w_gate": scatter_about(seeds[11], (MODEL_WIDTH, FF), MODEL_WIDTH ** -0.5, 0.1875, ((0, 8),)),
        "w_up": scatter_about(seeds[12], (MODEL_WIDTH, FF), MODEL_WIDTH ** -0.5, 0.1875, ((0, 8),)),
        "w_down": scatter_about(seeds[13], (FF, MODEL_WIDTH), FF ** -0.5, 0.109375, ((0, 8),)),
        "cotangent": scatter_about(seeds[14], (PACKED_ROWS, ROW_TOKENS, MODEL_WIDTH), 1.0, 6.0, ((0, 8), (1, 4))),
    }


ROPE_BASE = 1000000.0
EPSILON = 1e-06
MASKED = -1e+30

@jax.custom_vjp
def reduced_precision(v):
    return lax.optimization_barrier(v.astype(jnp.bfloat16)).astype(jnp.float32)

@jax.custom_vjp
def reduced_backward(v):
    return v

def low_keep(v):
    return (reduced_precision(v), None)

def low_pass(kept, grad):
    return (grad,)

def back_keep(v):
    return (v, None)

def back_low(kept, grad):
    return (reduced_precision(grad),)
reduced_precision.defvjp(low_keep, low_pass)
reduced_backward.defvjp(back_keep, back_low)

def matrix_product(left, right):
    return jnp.dot(left, right, precision=lax.Precision.HIGHEST)

def rms_scale(value_tensor, gain_values):
    return value_tensor * lax.rsqrt(lax.optimization_barrier(jnp.mean(value_tensor * value_tensor, axis=-1, keepdims=True)) + EPSILON) * gain_values

def rotary(value_tensor, start_offset):
    half_width = value_tensor.shape[-1] // 2
    inv_freq = ROPE_BASE ** (-jnp.arange(half_width, dtype=jnp.float32) / half_width)
    angles = start_offset.astype(jnp.float32)[:, None] * inv_freq[None, :]
    cosine = jnp.cos(angles)[:, None, :]
    sine_part = jnp.sin(angles)[:, None, :]
    first_half = value_tensor[..., :half_width]
    second = value_tensor[..., half_width:]
    return jnp.concatenate([first_half * cosine - second * sine_part, second * cosine + first_half * sine_part], axis=-1)

def row_lookup_tables(row_lengths, count_of_rows):
    places = jnp.arange(count_of_rows, dtype=jnp.int32)
    doc_ends = jnp.cumsum(row_lengths).astype(jnp.int32)
    passed = (places[:, None] >= doc_ends[None, :]).astype(jnp.int32)
    document_segment = lax.optimization_barrier(jnp.sum(passed, axis=1)).astype(jnp.int32)
    start_offset = (places - lax.optimization_barrier(jnp.sum(passed * row_lengths[None, :], axis=1))).astype(jnp.int32)
    return (document_segment, start_offset)

def attend(queries, key_rows, row_values, document_segment):
    count_of_rows = queries.shape[0]
    head_count = queries.shape[1]
    head_width = queries.shape[2]
    block_rows = min(512, count_of_rows)
    block_count = count_of_rows // block_rows
    group_size = head_count // key_rows.shape[1]
    key_full = jnp.repeat(key_rows, group_size, axis=1)
    value_full = jnp.repeat(row_values, group_size, axis=1)
    score_scale = head_width ** (-0.5)
    places = jnp.arange(count_of_rows, dtype=jnp.int32)

    def one_block(pieces):
        query_block, segment_block, place_block = pieces
        scores = jnp.einsum('qhd,khd->hqk', query_block, key_full, precision=lax.Precision.HIGHEST) * score_scale
        scores = reduced_backward(scores)
        allowed = (segment_block[:, None] == document_segment[None, :]) & (place_block[:, None] >= places[None, :])
        scores = jnp.where(allowed[None, :, :], scores, MASKED)
        row_top = lax.optimization_barrier(jnp.max(scores, axis=-1, keepdims=True))
        exp_values = jnp.exp(scores - row_top)
        weights = reduced_precision(exp_values / lax.optimization_barrier(jnp.sum(exp_values, axis=-1, keepdims=True)))
        return jnp.einsum('hqk,khd->qhd', weights, value_full, precision=lax.Precision.HIGHEST)
    outputs = lax.map(jax.checkpoint(one_block), (queries.reshape(block_count, block_rows, head_count, head_width), document_segment.reshape(block_count, block_rows), places.reshape(block_count, block_rows)))
    return outputs.reshape(count_of_rows, head_count, head_width)

def layer(inputs, norm_in, w_query, key_projection, value_projection, norm_query, norm_key, w_out, norm_post, w_gate, w_up, w_down, document_segment, start_offset):
    count_of_rows = inputs.shape[0]
    normalized = reduced_precision(rms_scale(inputs, norm_in))
    query_pre = reduced_backward(matrix_product(normalized, w_query)).reshape(count_of_rows, HQ, HEAD_SIZE)
    key_before_norm = reduced_backward(matrix_product(normalized, key_projection)).reshape(count_of_rows, KEY_VALUE_HEADS, HEAD_SIZE)
    row_values = reduced_backward(reduced_precision(matrix_product(normalized, value_projection))).reshape(count_of_rows, KEY_VALUE_HEADS, HEAD_SIZE)
    queries = reduced_backward(reduced_precision(rotary(rms_scale(query_pre, norm_query), start_offset)))
    key_rows = reduced_backward(reduced_precision(rotary(rms_scale(key_before_norm, norm_key), start_offset)))
    attended = attend(queries, key_rows, row_values, document_segment)
    attended = reduced_backward(reduced_precision(attended.reshape(count_of_rows, HQ * HEAD_SIZE)))
    middle = inputs + reduced_backward(matrix_product(attended, w_out))
    normed_post = reduced_precision(rms_scale(middle, norm_post))
    gate_sum = reduced_backward(matrix_product(normed_post, w_gate))
    up_sum = reduced_backward(matrix_product(normed_post, w_up))
    hidden = reduced_precision(gate_sum / (1.0 + jnp.exp(-gate_sum)) * up_sum)
    return middle + reduced_backward(matrix_product(hidden, w_down))

def reference(tokens, lengths, packing, norm_in, w_query, key_projection, value_projection, norm_query, norm_key, w_out, norm_post, w_gate, w_up, w_down, cotangent):
    weights = tuple((member.astype(jnp.float32) for member in (norm_in, w_query, key_projection, value_projection, norm_query, norm_key, w_out, norm_post, w_gate, w_up, w_down)))

    def row_step(totals, row_pieces):
        token_row, grad_row, row_lengths, order_row = row_pieces
        document_segment, start_offset = row_lookup_tables(row_lengths, ROW_TOKENS)
        chosen = order_row.astype(jnp.int32)
        packed = jnp.take(token_row, chosen, axis=0).astype(jnp.float32)
        packed_grad = jnp.take(grad_row, chosen, axis=0).astype(jnp.float32)

        def forward(inputs, *members):
            return layer(inputs, *members, document_segment, start_offset)
        result, pullback = jax.vjp(forward, packed, *weights)
        grads = pullback(packed_grad)
        inverse = jnp.argsort(chosen).astype(jnp.int32)
        output_row = jnp.take(result, inverse, axis=0).astype(jnp.bfloat16)
        input_row = jnp.take(grads[0], inverse, axis=0).astype(jnp.bfloat16)
        totals = tuple((total + grad for total, grad in zip(totals, grads[1:])))
        return (totals, (output_row, input_row))
    start = tuple((jnp.zeros(member.shape, jnp.float32) for member in weights))
    totals, (output, input_grad) = lax.scan(row_step, start, (tokens, cotangent, lengths, packing))
    return (output, input_grad, totals[0], totals[1], totals[2], totals[3], totals[4], totals[5], totals[6], totals[7], totals[8], totals[9], totals[10])
```

```python
import functools

import jax
import jax.numpy as jnp
from jax import lax
from jax.experimental import pallas as pl
from jax.experimental.pallas import tpu as pltpu
from jax.sharding import PartitionSpec as P

HQ = 16
KEY_VALUE_HEADS = 8
HEAD_SIZE = 128
GROUP = HQ // KEY_VALUE_HEADS

ROPE_BASE = 1000000.0
EPSILON = 1e-06
MASKED = -1e30
SCALE = HEAD_SIZE ** (-0.5)
MESH = pl.DeviceIdType.MESH
QUERY_BLOCK = 256
BF16 = jnp.bfloat16
F32 = jnp.float32


def matrix_product(left, right):
    return jnp.dot(left, right, preferred_element_type=F32)


def outer_sum(left, right):
    return lax.dot_general(left, right, (((0,), (0,)), ((), ())), preferred_element_type=F32)


def back_matmul(left, right):
    return lax.dot_general(left, right, (((1,), (1,)), ((), ())), preferred_element_type=F32)


def inverse_rms(values):
    return lax.rsqrt(jnp.mean(values * values, axis=-1, keepdims=True) + EPSILON)


def rms_backward(values, gain, grad):
    c = inverse_rms(values)
    scaled = grad * gain
    inner = jnp.mean(values * scaled, axis=-1, keepdims=True)
    return c * scaled - values * (c * c * c) * inner, grad * values * c


def greet(n):
    me = lax.axis_index("seq")
    barrier = pltpu.get_barrier_semaphore()
    for step in range(1, n):
        pl.semaphore_signal(
            barrier, inc=1, device_id={"seq": lax.rem(me + step, n)}, device_id_type=MESH
        )
    pl.semaphore_wait(barrier, n - 1)
    return me


def gather_kernel(n, x_ref, o_ref, send_sem, recv_sem):
    me = greet(n)
    rows = x_ref.shape[0]
    mine = pl.ds(pl.multiple_of(me * rows, rows), rows)
    copies = []
    for step in range(1, n):
        copy = pltpu.make_async_remote_copy(
            src_ref=x_ref,
            dst_ref=o_ref.at[mine],
            send_sem=send_sem.at[step - 1],
            recv_sem=recv_sem.at[step - 1],
            device_id={"seq": lax.rem(me + step, n)},
            device_id_type=MESH,
        )
        copy.start()
        copies.append(copy)
    o_ref[mine, :] = x_ref[...]
    for copy in copies:
        copy.wait()


def gather_rows(x, n, call_id):
    rows, width = x.shape
    return pl.pallas_call(
        functools.partial(gather_kernel, n),
        out_shape=jax.ShapeDtypeStruct((n * rows, width), x.dtype),
        in_specs=[pl.BlockSpec(memory_space=pltpu.VMEM)],
        out_specs=pl.BlockSpec(memory_space=pltpu.VMEM),
        scratch_shapes=[pltpu.SemaphoreType.DMA((n - 1,)), pltpu.SemaphoreType.DMA((n - 1,))],
        compiler_params=pltpu.CompilerParams(collective_id=call_id, has_side_effects=True),
        name=f"gather_rows_{call_id}",
    )(x)


def scatter_kernel(n, p_ref, o_ref, landed, send_sem, recv_sem):
    me = greet(n)
    rows = o_ref.shape[0]
    copies = []
    for step in range(1, n):
        peer = lax.rem(me + step, n)
        copy = pltpu.make_async_remote_copy(
            src_ref=p_ref.at[pl.ds(pl.multiple_of(peer * rows, rows), rows)],
            dst_ref=landed.at[step - 1],
            send_sem=send_sem.at[step - 1],
            recv_sem=recv_sem.at[step - 1],
            device_id={"seq": peer},
            device_id_type=MESH,
        )
        copy.start()
        copies.append(copy)
    o_ref[...] = p_ref[pl.ds(pl.multiple_of(me * rows, rows), rows), :].astype(F32)
    for step, copy in enumerate(copies):
        copy.wait()
        o_ref[...] += landed[step].astype(F32)


def scatter_sum(partial, n, call_id):
    total, width = partial.shape
    rows = total // n
    return pl.pallas_call(
        functools.partial(scatter_kernel, n),
        out_shape=jax.ShapeDtypeStruct((rows, width), F32),
        in_specs=[pl.BlockSpec(memory_space=pltpu.VMEM)],
        out_specs=pl.BlockSpec(memory_space=pltpu.VMEM),
        scratch_shapes=[
            pltpu.VMEM((n - 1, rows, width), partial.dtype),
            pltpu.SemaphoreType.DMA((n - 1,)),
            pltpu.SemaphoreType.DMA((n - 1,)),
        ],
        compiler_params=pltpu.CompilerParams(collective_id=call_id, has_side_effects=True),
        name=f"scatter_sum_{call_id}",
    )(partial)


def rope(values, cosine, sine):
    return values * cosine + pltpu.roll(values, HEAD_SIZE // 2, 1) * sine


def rope_back(grad, cosine, sine):
    return grad * cosine - pltpu.roll(grad, HEAD_SIZE // 2, 1) * sine


def forward_kernel(
    q_pre, k_pre, v_ref, gain_q, gain_k, cos_q, sin_q, cos_k, sin_k, place_k, place_q, start_q,
    out_ref, p_ref, q_ref, k_ref, v_turned,
):
    @pl.when((pl.program_id(1) == 0) & (pl.program_id(2) == 0))
    def _():
        pre = k_pre[...]
        k_ref[...] = rope(pre * inverse_rms(pre) * gain_k[...], cos_k[...], sin_k[...]).astype(BF16)
        v_turned[...] = v_ref[...].astype(F32).T.astype(BF16)

    pre = q_pre[...]
    query = rope(pre * inverse_rms(pre) * gain_q[...], cos_q[...], sin_q[...]).astype(BF16)
    q_ref[...] = query
    scores = back_matmul(k_ref[...], query) * SCALE
    keys = place_k[...]
    allowed = (keys <= place_q[...]) & (keys >= start_q[...])
    scores = jnp.where(allowed, scores, MASKED)
    top = jnp.max(scores, axis=0, keepdims=True)
    weights = jnp.exp(scores - top)
    total = jnp.sum(weights, axis=0, keepdims=True)
    weights = (weights * (1.0 / total)).astype(BF16)
    p_ref[0] = weights
    out_ref[...] = matrix_product(v_turned[...], weights).T.astype(BF16)


def attend_forward(q_pre, k_pre, value, gain_q, gain_k, cosine, sine, place, start):
    rows = q_pre.shape[0]
    heads = q_pre.shape[1] // HEAD_SIZE
    kv = heads // GROUP
    block = QUERY_BLOCK
    q_spec = pl.BlockSpec((block, HEAD_SIZE), lambda k, g, b: (b, k * GROUP + g))
    k_spec = pl.BlockSpec((rows, HEAD_SIZE), lambda k, g, b: (0, k))
    gain_spec = pl.BlockSpec((1, HEAD_SIZE), lambda k, g, b: (0, 0))
    trig_q = pl.BlockSpec((block, HEAD_SIZE), lambda k, g, b: (b, 0))
    trig_k = pl.BlockSpec((rows, HEAD_SIZE), lambda k, g, b: (0, 0))
    column = pl.BlockSpec((rows, 1), lambda k, g, b: (0, 0))
    row = pl.BlockSpec((1, block), lambda k, g, b: (0, b))
    return pl.pallas_call(
        forward_kernel,
        grid=(kv, GROUP, rows // block),
        out_shape=(
            jax.ShapeDtypeStruct((rows, heads * HEAD_SIZE), BF16),
            jax.ShapeDtypeStruct((heads, rows, rows), BF16),
            jax.ShapeDtypeStruct((rows, heads * HEAD_SIZE), BF16),
            jax.ShapeDtypeStruct((rows, kv * HEAD_SIZE), BF16),
        ),
        in_specs=[
            q_spec, k_spec, k_spec, gain_spec, gain_spec, trig_q, trig_q, trig_k, trig_k,
            column, row, row,
        ],
        out_specs=(
            q_spec,
            pl.BlockSpec((1, rows, block), lambda k, g, b: (k * GROUP + g, 0, b)),
            q_spec,
            k_spec,
        ),
        scratch_shapes=[pltpu.VMEM((HEAD_SIZE, rows), BF16)],
        name="attend_forward",
    )(
        q_pre, k_pre, value, gain_q, gain_k, cosine, sine, cosine, sine,
        place[:, None], place[None, :], start[None, :],
    )


def backward_kernel(
    p_ref, q_ref, k_ref, v_ref, grad_ref, q_pre, k_pre, gain_q, gain_k, cos_q, sin_q, cos_k, sin_k,
    dq_ref, dk_ref, dv_ref, dgain_q, dgain_k, k_turned, dk_sum, dv_sum,
):
    kv, group, block = pl.program_id(0), pl.program_id(1), pl.program_id(2)
    first = (group == 0) & (block == 0)
    last = (group == pl.num_programs(1) - 1) & (block == pl.num_programs(2) - 1)

    @pl.when(first & (kv == 0))
    def _():
        dgain_q[...] = jnp.zeros_like(dgain_q)
        dgain_k[...] = jnp.zeros_like(dgain_k)

    @pl.when(first)
    def _():
        k_turned[...] = k_ref[...].astype(F32).T.astype(BF16)
        dk_sum[...] = jnp.zeros_like(dk_sum)
        dv_sum[...] = jnp.zeros_like(dv_sum)

    rounded = p_ref[0]
    weights = rounded.astype(F32)
    grad = grad_ref[...]
    grad_weights = back_matmul(v_ref[...], grad)
    delta = jnp.sum(weights * grad_weights, axis=0, keepdims=True)
    grad_scores = (weights * (grad_weights - delta)).astype(BF16)
    dk_sum[...] += matrix_product(grad_scores, q_ref[...])
    dv_sum[...] += matrix_product(rounded, grad)
    dq = (matrix_product(k_turned[...], grad_scores).T * SCALE).astype(BF16).astype(F32)
    dq, gain_rows = rms_backward(q_pre[...], gain_q[...], rope_back(dq, cos_q[...], sin_q[...]))
    dq_ref[...] = dq.astype(BF16)
    dgain_q[...] += jnp.sum(gain_rows, axis=0, keepdims=True)

    @pl.when(last)
    def _():
        dk = (dk_sum[...] * SCALE).astype(BF16).astype(F32)
        dk, gain_rows = rms_backward(k_pre[...], gain_k[...], rope_back(dk, cos_k[...], sin_k[...]))
        dk_ref[...] = dk.astype(BF16)
        dgain_k[...] += jnp.sum(gain_rows, axis=0, keepdims=True)
        dv_ref[...] = dv_sum[...].astype(BF16)


def attend_backward(weights, query, key, value, grad, q_pre, k_pre, gain_q, gain_k, cosine, sine):
    rows = q_pre.shape[0]
    heads = q_pre.shape[1] // HEAD_SIZE
    kv = heads // GROUP
    block = QUERY_BLOCK
    q_spec = pl.BlockSpec((block, HEAD_SIZE), lambda k, g, b: (b, k * GROUP + g))
    k_spec = pl.BlockSpec((rows, HEAD_SIZE), lambda k, g, b: (0, k))
    gain_spec = pl.BlockSpec((1, HEAD_SIZE), lambda k, g, b: (0, 0))
    trig_q = pl.BlockSpec((block, HEAD_SIZE), lambda k, g, b: (b, 0))
    trig_k = pl.BlockSpec((rows, HEAD_SIZE), lambda k, g, b: (0, 0))
    return pl.pallas_call(
        backward_kernel,
        grid=(kv, GROUP, rows // block),
        out_shape=(
            jax.ShapeDtypeStruct((rows, heads * HEAD_SIZE), BF16),
            jax.ShapeDtypeStruct((rows, kv * HEAD_SIZE), BF16),
            jax.ShapeDtypeStruct((rows, kv * HEAD_SIZE), BF16),
            jax.ShapeDtypeStruct((1, HEAD_SIZE), F32),
            jax.ShapeDtypeStruct((1, HEAD_SIZE), F32),
        ),
        in_specs=[
            pl.BlockSpec((1, rows, block), lambda k, g, b: (k * GROUP + g, 0, b)),
            q_spec, k_spec, k_spec, q_spec, q_spec, k_spec, gain_spec, gain_spec,
            trig_q, trig_q, trig_k, trig_k,
        ],
        out_specs=(q_spec, k_spec, k_spec, gain_spec, gain_spec),
        scratch_shapes=[
            pltpu.VMEM((HEAD_SIZE, rows), BF16),
            pltpu.VMEM((rows, HEAD_SIZE), F32),
            pltpu.VMEM((rows, HEAD_SIZE), F32),
        ],
        name="attend_backward",
    )(weights, query, key, value, grad, q_pre, k_pre, gain_q, gain_k, cosine, sine, cosine, sine)


def on_device(
    tokens, lengths, packing, norm_in, w_query, key_projection, value_projection, norm_query,
    norm_key, w_out, norm_post, w_gate, w_up, w_down, cotangent,
):
    n = lax.axis_size("seq")
    shards = lax.axis_size("fsdp")
    me = lax.axis_index("seq")
    mine = lax.axis_index("fsdp")
    resident = tokens.shape[1]
    width = tokens.shape[2]
    rows = resident * n
    heads = HQ // n
    kv = KEY_VALUE_HEADS // n
    hidden_piece = w_down.shape[0] // n
    out_piece = width // n

    def columns(weight, pieces):
        size = weight.shape[1] // pieces
        return lax.dynamic_slice_in_dim(weight, me * size, size, axis=1)

    def spread_columns(weight):
        pieces = weight.reshape(weight.shape[0], shards, n, hidden_piece)
        return lax.dynamic_index_in_dim(pieces, me, axis=2, keepdims=False).reshape(
            weight.shape[0], shards * hidden_piece
        )

    gains = lax.all_gather(
        jnp.concatenate([norm_in, norm_post, norm_query, norm_key])[None, :], "fsdp", axis=0, tiled=True
    ).astype(F32)
    part, small = norm_in.shape[0], norm_query.shape[0]
    gain_in = gains[:, :part].reshape(1, -1)
    gain_post = gains[:, part : 2 * part].reshape(1, -1)
    gain_query = gains[:, 2 * part : 2 * part + small].reshape(1, -1)
    gain_key = gains[:, 2 * part + small :].reshape(1, -1)

    qkv_weight = lax.all_gather(
        jnp.concatenate(
            [columns(w_query, n), columns(key_projection, n), columns(value_projection, n)], axis=1
        ),
        "fsdp", axis=0, tiled=True,
    )
    out_columns = lax.all_gather(columns(w_out, n), "fsdp", axis=0, tiled=True)
    gate_up_weight = lax.all_gather(
        jnp.concatenate([spread_columns(w_gate), spread_columns(w_up)], axis=1), "fsdp", axis=0, tiled=True
    )
    down_weight = lax.all_gather(
        lax.dynamic_slice_in_dim(w_down, me * hidden_piece, hidden_piece, axis=0),
        "fsdp", axis=0, tiled=True,
    )
    out_weight = lax.all_to_all(out_columns, "seq", split_axis=0, concat_axis=1, tiled=True)

    order = packing[0]
    places = jnp.arange(rows, dtype=jnp.int32)
    place = jnp.sum(jnp.where(order[None, :] == places[:, None], places[None, :], 0), axis=1)
    ends = jnp.cumsum(lengths[0])
    start = jnp.sum(jnp.where(place[:, None] >= ends[None, :], lengths[0][None, :], 0), axis=1)
    half = HEAD_SIZE // 2
    inv_freq = ROPE_BASE ** (-jnp.arange(half, dtype=F32) / half)
    angles = (place - start).astype(F32)[:, None] * inv_freq[None, :]
    cosine, sine = jnp.cos(angles), jnp.sin(angles)
    cosine = jnp.concatenate([cosine, cosine], axis=1)
    sine = jnp.concatenate([-sine, sine], axis=1)

    whole = gather_rows(tokens[0], n, 0)
    inputs = tokens[0].astype(F32)
    whole_f32 = whole.astype(F32)
    unit = whole_f32 * inverse_rms(whole_f32)
    normalized = (unit * gain_in).astype(BF16)
    qkv = matrix_product(normalized, qkv_weight)
    split = heads * HEAD_SIZE
    q_pre = qkv[:, :split]
    k_pre = qkv[:, split : split + kv * HEAD_SIZE]
    value = qkv[:, split + kv * HEAD_SIZE :].astype(BF16)
    attended, weights, query, key = attend_forward(
        q_pre, k_pre, value, gain_query, gain_key, cosine, sine, place, start
    )
    middle = inputs + scatter_sum(matrix_product(attended, out_weight).astype(BF16), n, 1)
    normed_post_mine = (middle * inverse_rms(middle) * gain_post).astype(BF16)
    normed_post = gather_rows(normed_post_mine, n, 2)
    grad_mlp = gather_rows(cotangent[0], n, 3)

    gate_up = matrix_product(normed_post, gate_up_weight)
    units = shards * hidden_piece
    gate, up = gate_up[:, :units], gate_up[:, units:]
    logistic = 1.0 / (1.0 + jnp.exp(-gate))
    hidden = (gate / (1.0 + jnp.exp(-gate)) * up).astype(BF16)
    result = middle + scatter_sum(matrix_product(hidden, down_weight).astype(BF16), n, 4)
    output = result.astype(BF16)[None]

    grad_hidden = back_matmul(grad_mlp, down_weight)
    grad_down = outer_sum(hidden, grad_mlp).astype(BF16)
    grad_gate = (grad_hidden * up * (logistic + gate * logistic * (1.0 - logistic))).astype(BF16)
    grad_up = (grad_hidden * gate * logistic).astype(BF16)
    grad_gate_up = jnp.concatenate([grad_gate, grad_up], axis=1)
    grad_gate_up_weight = outer_sum(normed_post, grad_gate_up).astype(BF16)
    grad_normed_post = scatter_sum(back_matmul(grad_gate_up, gate_up_weight).astype(BF16), n, 5)
    grad_middle, gain_rows = rms_backward(middle, gain_post, grad_normed_post)
    grad_middle = cotangent[0].astype(F32) + grad_middle
    grad_gain_post = jnp.sum(gain_rows, axis=0)
    grad_branch = gather_rows(grad_middle.astype(BF16), n, 6)

    grad_out = outer_sum(attended, grad_branch).astype(BF16)
    grad_attended = back_matmul(grad_branch, out_weight).astype(BF16)
    grad_q, grad_k, grad_v, grad_gain_query, grad_gain_key = attend_backward(
        weights, query, key, value, grad_attended, q_pre, k_pre, gain_query, gain_key, cosine, sine
    )
    grad_qkv = jnp.concatenate([grad_q, grad_k, grad_v], axis=1)
    grad_qkv_weight = outer_sum(normalized, grad_qkv).astype(BF16)
    partial = back_matmul(grad_qkv, qkv_weight)
    grad_gain_in = jnp.sum(partial * unit, axis=0)
    grad_normed = scatter_sum(partial.astype(BF16), n, 7)
    grad_inputs, _ = rms_backward(inputs, gain_in, grad_normed)
    input_grad = (grad_middle + grad_inputs).astype(BF16)[None]

    def shared(grad):
        return lax.all_gather(
            lax.psum_scatter(grad, "fsdp", scatter_dimension=0, tiled=True), "seq", axis=0
        ).astype(F32)

    def beside(pieces):
        return jnp.swapaxes(pieces, 0, 1).reshape(pieces.shape[1], -1)

    final_down = shared(grad_down).reshape(-1, width)
    gate_up_all = shared(grad_gate_up_weight)

    def spread_back(pieces):
        pieces = pieces.reshape(n, pieces.shape[1], shards, hidden_piece)
        return jnp.transpose(pieces, (1, 2, 0, 3)).reshape(pieces.shape[1], -1)

    final_gate = spread_back(gate_up_all[:, :, :units])
    final_up = spread_back(gate_up_all[:, :, units:])
    final_out = beside(
        shared(lax.all_to_all(grad_out, "seq", split_axis=1, concat_axis=0, tiled=True))
    )
    qkv_all = shared(grad_qkv_weight)
    final_query = beside(qkv_all[:, :, :split])
    final_key = beside(qkv_all[:, :, split : split + kv * HEAD_SIZE])
    final_value = beside(qkv_all[:, :, split + kv * HEAD_SIZE :])

    sums = lax.psum(
        jnp.concatenate([grad_gain_in, grad_gain_post, grad_gain_query[0], grad_gain_key[0]]),
        ("seq", "fsdp"),
    )

    def share(offset, size):
        return lax.dynamic_slice_in_dim(sums, offset + mine * size, size)

    return (
        output,
        input_grad,
        share(0, part),
        final_query,
        final_key,
        final_value,
        share(2 * width, small),
        share(2 * width + HEAD_SIZE, small),
        final_out,
        share(width, part),
        final_gate,
        final_up,
        final_down,
    )


def solution(mesh):
    flat, wide = P("fsdp"), P("fsdp", None)
    whole = P("fsdp", "seq", None)
    in_specs = (
        whole, wide, wide, flat, wide, wide, wide, flat, flat, wide, flat, wide, wide, wide, whole,
    )
    out_specs = (whole, whole, flat, wide, wide, wide, flat, flat, wide, flat, wide, wide, wide)
    return jax.shard_map(
        on_device, mesh=mesh, in_specs=in_specs, out_specs=out_specs, check_vma=False
    )
```

```python
import functools

import jax
import jax.numpy as jnp
from jax import lax
from jax.experimental import pallas as pl
from jax.experimental.pallas import tpu as pltpu
from jax.sharding import PartitionSpec as P

HQ = 16
KEY_VALUE_HEADS = 8
HEAD_SIZE = 128
GROUP = HQ // KEY_VALUE_HEADS

ROPE_BASE = 1000000.0
EPSILON = 1e-06
MASKED = -1e30
SCALE = HEAD_SIZE ** (-0.5)
MESH = pl.DeviceIdType.MESH
BF16 = jnp.bfloat16
F32 = jnp.float32


def matrix_product(left, right):
    return jnp.dot(left, right, preferred_element_type=F32)


def outer_sum(left, right):
    return lax.dot_general(left, right, (((0,), (0,)), ((), ())), preferred_element_type=F32)


def back_matmul(left, right):
    return lax.dot_general(left, right, (((1,), (1,)), ((), ())), preferred_element_type=F32)


def inverse_rms(values):
    return lax.rsqrt(jnp.mean(values * values, axis=-1, keepdims=True) + EPSILON)


def rms_backward(values, gain, grad):
    c = inverse_rms(values)
    scaled = grad * gain
    inner = jnp.mean(values * scaled, axis=-1, keepdims=True)
    return c * scaled - values * (c * c * c) * inner, grad * values * c


def greet(*axes):
    barrier = pltpu.get_barrier_semaphore()
    count = 0
    for axis in axes:
        n = lax.axis_size(axis)
        me = lax.axis_index(axis)
        for step in range(1, n):
            pl.semaphore_signal(
                barrier, inc=1, device_id={axis: lax.rem(me + step, n)}, device_id_type=MESH
            )
        count += n - 1
    pl.semaphore_wait(barrier, count)


def block_of(index, size):
    return pl.ds(pl.multiple_of(index * size, size), size)


def start_to_peers(axis, source, target, send_sem, recv_sem):
    n = lax.axis_size(axis)
    me = lax.axis_index(axis)
    copies = []
    for step in range(1, n):
        peer = lax.rem(me + step, n)
        copy = pltpu.make_async_remote_copy(
            src_ref=source(peer),
            dst_ref=target(step),
            send_sem=send_sem.at[step - 1],
            recv_sem=recv_sem.at[step - 1],
            device_id={axis: peer},
            device_id_type=MESH,
        )
        copy.start()
        copies.append(copy)
    return copies


def semaphores(*counts):
    return [pltpu.SemaphoreType.DMA((count,)) for count in counts]


VMEM_SPEC = pl.BlockSpec(memory_space=pltpu.VMEM)
ANY_SPEC = pl.BlockSpec(memory_space=pl.ANY)


def communicating(call_id, **more):
    return pltpu.CompilerParams(collective_id=call_id, has_side_effects=True, **more)


def gather_kernel(x_ref, o_ref, send_sem, recv_sem):
    greet("seq")
    mine = block_of(lax.axis_index("seq"), x_ref.shape[0])
    copies = start_to_peers(
        "seq", lambda peer: x_ref, lambda step: o_ref.at[mine], send_sem, recv_sem
    )
    o_ref[mine, :] = x_ref[...]
    for copy in copies:
        copy.wait()


def gather_rows(x, n, call_id):
    rows, width = x.shape
    return pl.pallas_call(
        gather_kernel,
        out_shape=jax.ShapeDtypeStruct((n * rows, width), x.dtype),
        in_specs=[VMEM_SPEC],
        out_specs=VMEM_SPEC,
        scratch_shapes=semaphores(n - 1, n - 1),
        compiler_params=communicating(call_id),
        name=f"gather_rows_{call_id}",
    )(x)


def gather_first_kernel(x_ref, gains_ref, o_ref, all_gains, send, recv, gain_send, gain_recv):
    greet("seq", "fsdp")
    place = lax.axis_index("fsdp")
    gain_copies = start_to_peers(
        "fsdp", lambda peer: gains_ref, lambda step: all_gains.at[place], gain_send, gain_recv
    )
    mine = block_of(lax.axis_index("seq"), x_ref.shape[0])
    copies = start_to_peers("seq", lambda peer: x_ref, lambda step: o_ref.at[mine], send, recv)
    o_ref[mine, :] = x_ref[...]
    all_gains[place] = gains_ref[...]
    for copy in gain_copies + copies:
        copy.wait()


def gather_first(x, gains, n, shards, call_id):
    rows, width = x.shape
    return pl.pallas_call(
        gather_first_kernel,
        out_shape=(
            jax.ShapeDtypeStruct((n * rows, width), x.dtype),
            jax.ShapeDtypeStruct((shards,) + gains.shape, gains.dtype),
        ),
        in_specs=[VMEM_SPEC, VMEM_SPEC],
        out_specs=(VMEM_SPEC, VMEM_SPEC),
        scratch_shapes=semaphores(n - 1, n - 1, shards - 1, shards - 1),
        compiler_params=communicating(call_id),
        name="gather_first",
    )(x, gains)


def scatter_kernel(p_ref, o_ref, landed, send_sem, recv_sem):
    greet("seq")
    rows = o_ref.shape[0]
    copies = start_to_peers(
        "seq",
        lambda peer: p_ref.at[block_of(peer, rows)],
        lambda step: landed.at[step - 1],
        send_sem,
        recv_sem,
    )
    o_ref[...] = p_ref[block_of(lax.axis_index("seq"), rows), :].astype(F32)
    for step, copy in enumerate(copies):
        copy.wait()
        o_ref[...] += landed[step].astype(F32)


def scatter_sum(partial, n, call_id):
    total, width = partial.shape
    rows = total // n
    return pl.pallas_call(
        scatter_kernel,
        out_shape=jax.ShapeDtypeStruct((rows, width), F32),
        in_specs=[VMEM_SPEC],
        out_specs=VMEM_SPEC,
        scratch_shapes=[pltpu.VMEM((n - 1, rows, width), partial.dtype)] + semaphores(n - 1, n - 1),
        compiler_params=communicating(call_id),
        name=f"scatter_sum_{call_id}",
    )(partial)


def scatter_last_kernel(
    p_ref, small_ref, o_ref, small_out, landed, part_landed, part_sum, row_landed,
    send, recv, part_send, part_recv, row_send, row_recv,
):
    greet("seq", "fsdp")
    rows = o_ref.shape[0]
    part_copies = start_to_peers(
        "fsdp",
        lambda peer: small_ref.at[peer],
        lambda step: part_landed.at[step - 1],
        part_send,
        part_recv,
    )
    copies = start_to_peers(
        "seq",
        lambda peer: p_ref.at[block_of(peer, rows)],
        lambda step: landed.at[step - 1],
        send,
        recv,
    )
    total = small_ref[lax.axis_index("fsdp")]
    for step, copy in enumerate(part_copies):
        copy.wait()
        total = total + part_landed[step]
    part_sum[...] = total
    o_ref[...] = p_ref[block_of(lax.axis_index("seq"), rows), :].astype(F32)
    row_copies = start_to_peers(
        "seq", lambda peer: part_sum, lambda step: row_landed.at[step - 1], row_send, row_recv
    )
    for step, copy in enumerate(copies):
        copy.wait()
        o_ref[...] += landed[step].astype(F32)
    for step, copy in enumerate(row_copies):
        copy.wait()
        total = total + row_landed[step]
    small_out[...] = total


def scatter_last(partial, small, n, shards, call_id):
    total, width = partial.shape
    rows = total // n
    piece = small.shape[1:]
    return pl.pallas_call(
        scatter_last_kernel,
        out_shape=(jax.ShapeDtypeStruct((rows, width), F32), jax.ShapeDtypeStruct(piece, F32)),
        in_specs=[VMEM_SPEC, VMEM_SPEC],
        out_specs=(VMEM_SPEC, VMEM_SPEC),
        scratch_shapes=[
            pltpu.VMEM((n - 1, rows, width), partial.dtype),
            pltpu.VMEM((shards - 1,) + piece, F32),
            pltpu.VMEM(piece, F32),
            pltpu.VMEM((n - 1,) + piece, F32),
        ]
        + semaphores(n - 1, n - 1, shards - 1, shards - 1, n - 1, n - 1),
        compiler_params=communicating(call_id),
        name="scatter_last",
    )(partial, small)


def rope(values, cosine, sine):
    return values * cosine + pltpu.roll(values, HEAD_SIZE // 2, 1) * sine


def rope_back(grad, cosine, sine):
    return grad * cosine - pltpu.roll(grad, HEAD_SIZE // 2, 1) * sine


def head_columns(index):
    return pl.ds(pl.multiple_of(index * HEAD_SIZE, HEAD_SIZE), HEAD_SIZE)


def turned_block(shift):
    def block(i):
        return lax.rem(lax.axis_index("seq") + shift + i, lax.axis_size("seq"))

    return block


def forward_kernel(
    q_pre, k_pre, v_ref, gain_q, gain_k, cos_q, sin_q, cos_k, sin_k, place_k, place_q, start_q, cot,
    out_ref, p_ref, q_ref, k_ref, cot_all,
    v_turned, outs, cot_send, cot_recv, cot_local, send, recv, local,
):
    i, head = pl.program_id(0), pl.program_id(1)
    n, heads = pl.num_programs(0), pl.num_programs(1)
    seq = lax.axis_size("seq")
    me = lax.axis_index("seq")
    kv = outs.shape[1] // GROUP
    rows = cot.shape[0]
    mine = block_of(me, rows)

    def cot_copies():
        return [
            pltpu.make_async_remote_copy(
                src_ref=cot,
                dst_ref=cot_all.at[mine],
                send_sem=cot_send.at[step - 1],
                recv_sem=cot_recv.at[step - 1],
                device_id={"seq": lax.rem(me + step, seq)},
                device_id_type=MESH,
            )
            for step in range(1, seq)
        ]

    cot_own = pltpu.make_async_copy(cot, cot_all.at[mine], cot_local)

    def out_copy(step, which):
        return pltpu.make_async_remote_copy(
            src_ref=outs.at[step, which],
            dst_ref=out_ref.at[:, head_columns(me * heads + which)],
            send_sem=send.at[step, which],
            recv_sem=recv.at[step, which],
            device_id={"seq": lax.rem(me + 1 + step, seq)},
            device_id_type=MESH,
        )

    def own_copy(which):
        return pltpu.make_async_copy(
            outs.at[seq - 1, which], out_ref.at[:, head_columns(me * heads + which)], local.at[which]
        )

    @pl.when((i == 0) & (head == 0))
    def _():
        greet("seq")
        for copy in cot_copies():
            copy.start()
        cot_own.start()
        for which in range(kv):
            own = pl.ds(which * HEAD_SIZE, HEAD_SIZE)
            pre = k_pre[:, own]
            k_ref[:, own] = rope(
                pre * inverse_rms(pre) * gain_k[...], cos_k[...], sin_k[...]
            ).astype(BF16)
            v_turned[which] = v_ref[:, own].astype(F32).T.astype(BF16)

    @pl.when((head > 0) & (i < n - 1))
    def _():
        out_copy(i, head - 1).start()

    @pl.when((head == 0) & (i > 0))
    def _():
        out_copy(i - 1, heads - 1).start()

    pre = q_pre[...]
    query = rope(pre * inverse_rms(pre) * gain_q[...], cos_q[...], sin_q[...]).astype(BF16)
    q_ref[...] = query
    pair = head // GROUP
    scores = back_matmul(k_ref[:, head_columns(pair)], query) * SCALE
    keys = place_k[...]
    allowed = (keys <= place_q[...]) & (keys >= start_q[...])
    scores = jnp.where(allowed, scores, MASKED)
    top = jnp.max(scores, axis=0, keepdims=True)
    weights = jnp.exp(scores - top)
    total = jnp.sum(weights, axis=0, keepdims=True)
    weights = (weights * (1.0 / total)).astype(BF16)
    p_ref[0] = weights
    outs[i, head] = matrix_product(v_turned[pair], weights).T.astype(BF16)

    @pl.when((i == n - 1) & (head == heads - 1))
    def _():
        for which in range(outs.shape[1]):
            own_copy(which).start()
        for copy in cot_copies():
            copy.wait()
        cot_own.wait()
        for step in range(seq - 1):
            for which in range(outs.shape[1]):
                out_copy(step, which).wait()
        for which in range(outs.shape[1]):
            own_copy(which).wait()


def attend_forward(
    q_pre, k_pre, value, gain_q, gain_k, cosine, sine, place, start, cotangent, n, call_id
):
    rows = q_pre.shape[0]
    heads = q_pre.shape[1] // HEAD_SIZE
    kv = heads // GROUP
    block = rows // n
    width = cotangent.shape[1]
    turn = turned_block(1)
    q_spec = pl.BlockSpec((block, HEAD_SIZE), lambda i, h: (turn(i), h))
    k_spec = pl.BlockSpec((rows, kv * HEAD_SIZE), lambda i, h: (0, 0))
    gain_spec = pl.BlockSpec((1, HEAD_SIZE), lambda i, h: (0, 0))
    trig_q = pl.BlockSpec((block, HEAD_SIZE), lambda i, h: (turn(i), 0))
    trig_k = pl.BlockSpec((rows, HEAD_SIZE), lambda i, h: (0, 0))
    column = pl.BlockSpec((rows, 1), lambda i, h: (0, 0))
    row = pl.BlockSpec((1, block), lambda i, h: (0, turn(i)))
    return pl.pallas_call(
        forward_kernel,
        grid=(n, heads),
        out_shape=(
            jax.ShapeDtypeStruct((block, n * heads * HEAD_SIZE), BF16),
            jax.ShapeDtypeStruct((heads, rows, rows), BF16),
            jax.ShapeDtypeStruct((rows, heads * HEAD_SIZE), BF16),
            jax.ShapeDtypeStruct((rows, kv * HEAD_SIZE), BF16),
            jax.ShapeDtypeStruct((rows, width), BF16),
        ),
        in_specs=[
            q_spec, k_spec, k_spec, gain_spec, gain_spec, trig_q, trig_q, trig_k, trig_k,
            column, row, row, ANY_SPEC,
        ],
        out_specs=(
            ANY_SPEC,
            pl.BlockSpec((1, rows, block), lambda i, h: (h, 0, turn(i))),
            q_spec,
            k_spec,
            ANY_SPEC,
        ),
        scratch_shapes=[
            pltpu.VMEM((kv, HEAD_SIZE, rows), BF16),
            pltpu.VMEM((n, heads, block, HEAD_SIZE), BF16),
            pltpu.SemaphoreType.DMA((n - 1,)),
            pltpu.SemaphoreType.DMA((n - 1,)),
            pltpu.SemaphoreType.DMA,
            pltpu.SemaphoreType.DMA((n - 1, heads)),
            pltpu.SemaphoreType.DMA((n - 1, heads)),
            pltpu.SemaphoreType.DMA((heads,)),
        ],
        compiler_params=communicating(call_id),
        name="attend_forward",
    )(
        q_pre, k_pre, value, gain_q, gain_k, cosine, sine, cosine, sine,
        place[:, None], place[None, :], start[None, :], cotangent,
    )


def backward_kernel(
    p_ref, q_ref, k_ref, v_ref, q_pre, k_pre, gain_q, gain_k, cos_q, sin_q, cos_k, sin_k,
    grad_own, bulk,
    dq_ref, dk_ref, dv_ref, dgain_q, dgain_k, bulk_landed,
    k_turned, dk_sum, dv_sum, grads, send, recv, local, bulk_send, bulk_recv,
):
    i, head = pl.program_id(0), pl.program_id(1)
    n, heads = pl.num_programs(0), pl.num_programs(1)
    seq = lax.axis_size("seq")
    me = lax.axis_index("seq")
    kv = k_turned.shape[0]
    rows = grads.shape[1]
    span = grads.shape[2]
    first = (i == 0) & (head == 0)
    last = (i == n - 1) & (head == heads - 1)

    def grad_copy(step):
        peer = lax.rem(me + step, seq)
        return pltpu.make_async_remote_copy(
            src_ref=grad_own.at[:, block_of(peer, span)],
            dst_ref=grads.at[step],
            send_sem=send.at[step - 1],
            recv_sem=recv.at[step - 1],
            device_id={"seq": peer},
            device_id_type=MESH,
        )

    def bulk_copy(step):
        peer = lax.rem(me + step, seq)
        return pltpu.make_async_remote_copy(
            src_ref=bulk.at[block_of(peer, rows)],
            dst_ref=bulk_landed.at[step - 1],
            send_sem=bulk_send.at[step - 1],
            recv_sem=bulk_recv.at[step - 1],
            device_id={"seq": peer},
            device_id_type=MESH,
        )

    own_copy = pltpu.make_async_copy(grad_own.at[:, block_of(me, span)], grads.at[0], local)

    @pl.when(first)
    def _():
        greet("seq")
        own_copy.start()
        for step in range(1, seq):
            grad_copy(step).start()
        for step in range(1, seq):
            bulk_copy(step).start()
        dgain_q[...] = jnp.zeros_like(dgain_q)
        dgain_k[...] = jnp.zeros_like(dgain_k)
        dk_sum[...] = jnp.zeros_like(dk_sum)
        dv_sum[...] = jnp.zeros_like(dv_sum)
        for which in range(kv):
            own = pl.ds(which * HEAD_SIZE, HEAD_SIZE)
            k_turned[which] = k_ref[:, own].astype(F32).T.astype(BF16)
        own_copy.wait()

    for step in range(1, seq):
        @pl.when((head == 0) & (i == seq - step))
        def _():
            grad_copy(step).wait_recv()

    slot = lax.rem(seq - i, seq)
    pair = head // GROUP
    rounded = p_ref[0]
    weights = rounded.astype(F32)
    grad = grads[slot, :, head_columns(head)]
    grad_weights = back_matmul(v_ref[:, head_columns(pair)], grad)
    delta = jnp.sum(weights * grad_weights, axis=0, keepdims=True)
    grad_scores = (weights * (grad_weights - delta)).astype(BF16)
    dk_sum[pair] += matrix_product(grad_scores, q_ref[...])
    dv_sum[pair] += matrix_product(rounded, grad)
    dq = (matrix_product(k_turned[pair], grad_scores).T * SCALE).astype(BF16).astype(F32)
    dq, gain_rows = rms_backward(q_pre[...], gain_q[...], rope_back(dq, cos_q[...], sin_q[...]))
    dq_ref[...] = dq.astype(BF16)
    dgain_q[...] += jnp.sum(gain_rows, axis=0, keepdims=True)

    @pl.when(last)
    def _():
        for which in range(kv):
            own = pl.ds(which * HEAD_SIZE, HEAD_SIZE)
            dk = (dk_sum[which] * SCALE).astype(BF16).astype(F32)
            dk, gain_rows = rms_backward(
                k_pre[:, own], gain_k[...], rope_back(dk, cos_k[...], sin_k[...])
            )
            dk_ref[:, own] = dk.astype(BF16)
            dgain_k[...] += jnp.sum(gain_rows, axis=0, keepdims=True)
            dv_ref[:, own] = dv_sum[which].astype(BF16)
        for step in range(1, seq):
            grad_copy(step).wait_send()
            bulk_copy(step).wait()


def attend_backward(
    weights, query, key, value, grad_own, bulk, q_pre, k_pre, gain_q, gain_k, cosine, sine, n, call_id
):
    rows = q_pre.shape[0]
    heads = q_pre.shape[1] // HEAD_SIZE
    kv = heads // GROUP
    block = rows // n
    turn = turned_block(0)
    q_spec = pl.BlockSpec((block, HEAD_SIZE), lambda i, h: (turn(i), h))
    k_spec = pl.BlockSpec((rows, kv * HEAD_SIZE), lambda i, h: (0, 0))
    gain_spec = pl.BlockSpec((1, HEAD_SIZE), lambda i, h: (0, 0))
    trig_q = pl.BlockSpec((block, HEAD_SIZE), lambda i, h: (turn(i), 0))
    trig_k = pl.BlockSpec((rows, HEAD_SIZE), lambda i, h: (0, 0))
    return pl.pallas_call(
        backward_kernel,
        grid=(n, heads),
        out_shape=(
            jax.ShapeDtypeStruct((rows, heads * HEAD_SIZE), BF16),
            jax.ShapeDtypeStruct((rows, kv * HEAD_SIZE), BF16),
            jax.ShapeDtypeStruct((rows, kv * HEAD_SIZE), BF16),
            jax.ShapeDtypeStruct((1, HEAD_SIZE), F32),
            jax.ShapeDtypeStruct((1, HEAD_SIZE), F32),
            jax.ShapeDtypeStruct((n - 1, block, bulk.shape[1]), BF16),
        ),
        in_specs=[
            pl.BlockSpec((1, rows, block), lambda i, h: (h, 0, turn(i))),
            q_spec, k_spec, k_spec, q_spec, k_spec, gain_spec, gain_spec,
            trig_q, trig_q, trig_k, trig_k, ANY_SPEC, ANY_SPEC,
        ],
        out_specs=(q_spec, k_spec, k_spec, gain_spec, gain_spec, ANY_SPEC),
        scratch_shapes=[
            pltpu.VMEM((kv, HEAD_SIZE, rows), BF16),
            pltpu.VMEM((kv, rows, HEAD_SIZE), F32),
            pltpu.VMEM((kv, rows, HEAD_SIZE), F32),
            pltpu.VMEM((n, block, heads * HEAD_SIZE), BF16),
            pltpu.SemaphoreType.DMA((n - 1,)),
            pltpu.SemaphoreType.DMA((n - 1,)),
            pltpu.SemaphoreType.DMA,
            pltpu.SemaphoreType.DMA((n - 1,)),
            pltpu.SemaphoreType.DMA((n - 1,)),
        ],
        compiler_params=communicating(call_id),
        name="attend_backward",
    )(
        weights, query, key, value, q_pre, k_pre, gain_q, gain_k, cosine, sine, cosine, sine,
        grad_own, bulk,
    )


def on_device(
    tokens, lengths, packing, norm_in, w_query, key_projection, value_projection, norm_query,
    norm_key, w_out, norm_post, w_gate, w_up, w_down, cotangent,
):
    n = lax.axis_size("seq")
    shards = lax.axis_size("fsdp")
    me = lax.axis_index("seq")
    resident = tokens.shape[1]
    width = tokens.shape[2]
    rows = resident * n
    heads = HQ // n
    kv = KEY_VALUE_HEADS // n
    hidden_piece = w_down.shape[0] // n

    def columns(weight, pieces):
        size = weight.shape[1] // pieces
        return lax.dynamic_slice_in_dim(weight, me * size, size, axis=1)

    def spread_columns(weight):
        pieces = weight.reshape(weight.shape[0], shards, n, hidden_piece)
        return lax.dynamic_index_in_dim(pieces, me, axis=2, keepdims=False).reshape(
            weight.shape[0], shards * hidden_piece
        )

    def tile_of(values):
        pad = 1024 - values.shape[-1]
        values = jnp.concatenate([values, jnp.zeros(values.shape[:-1] + (pad,), F32)], axis=-1)
        return values.reshape(values.shape[:-1] + (8, 128))

    part, small = norm_in.shape[0], norm_query.shape[0]
    whole, gains = gather_first(
        tokens[0],
        tile_of(jnp.concatenate([norm_in, norm_post, norm_query, norm_key]).astype(F32)),
        n, shards, 0,
    )
    gains = gains.reshape(shards, -1)
    gain_in = gains[:, :part].reshape(1, -1)
    gain_post = gains[:, part : 2 * part].reshape(1, -1)
    gain_query = gains[:, 2 * part : 2 * part + small].reshape(1, -1)
    gain_key = gains[:, 2 * part + small : 2 * part + 2 * small].reshape(1, -1)

    qkv_weight = lax.all_gather(
        jnp.concatenate(
            [columns(w_query, n), columns(key_projection, n), columns(value_projection, n)], axis=1
        ),
        "fsdp", axis=0, tiled=True,
    )
    out_weight = lax.all_gather(w_out, "fsdp", axis=0, tiled=True)
    gate_up_weight = lax.all_gather(
        jnp.concatenate([spread_columns(w_gate), spread_columns(w_up)], axis=1), "fsdp", axis=0, tiled=True
    )
    down_weight = lax.all_gather(
        lax.dynamic_slice_in_dim(w_down, me * hidden_piece, hidden_piece, axis=0),
        "fsdp", axis=0, tiled=True,
    )

    order = packing[0]
    places = jnp.arange(rows, dtype=jnp.int32)
    place = jnp.sum(jnp.where(order[None, :] == places[:, None], places[None, :], 0), axis=1)
    ends = jnp.cumsum(lengths[0])
    start = jnp.sum(jnp.where(place[:, None] >= ends[None, :], lengths[0][None, :], 0), axis=1)
    half = HEAD_SIZE // 2
    inv_freq = ROPE_BASE ** (-jnp.arange(half, dtype=F32) / half)
    angles = (place - start).astype(F32)[:, None] * inv_freq[None, :]
    cosine, sine = jnp.cos(angles), jnp.sin(angles)
    cosine = jnp.concatenate([cosine, cosine], axis=1)
    sine = jnp.concatenate([-sine, sine], axis=1)

    inputs = tokens[0].astype(F32)
    whole_f32 = whole.astype(F32)
    unit = whole_f32 * inverse_rms(whole_f32)
    normalized = (unit * gain_in).astype(BF16)
    qkv = matrix_product(normalized, qkv_weight)
    split = heads * HEAD_SIZE
    q_pre = qkv[:, :split]
    k_pre = qkv[:, split : split + kv * HEAD_SIZE]
    value = qkv[:, split + kv * HEAD_SIZE :].astype(BF16)
    attended, weights, query, key, grad_mlp = attend_forward(
        q_pre, k_pre, value, gain_query, gain_key, cosine, sine, place, start, cotangent[0], n, 1
    )
    middle = inputs + matrix_product(attended, out_weight)
    normed_post_mine = (middle * inverse_rms(middle) * gain_post).astype(BF16)
    normed_post = gather_rows(normed_post_mine, n, 2)

    gate_up = matrix_product(normed_post, gate_up_weight)
    units = shards * hidden_piece
    gate, up = gate_up[:, :units], gate_up[:, units:]
    logistic = 1.0 / (1.0 + jnp.exp(-gate))
    hidden = (gate / (1.0 + jnp.exp(-gate)) * up).astype(BF16)
    mlp_partial = matrix_product(hidden, down_weight).astype(BF16)

    grad_hidden = back_matmul(grad_mlp, down_weight)
    grad_down = outer_sum(hidden, grad_mlp).astype(BF16)
    grad_gate = (grad_hidden * up * (logistic + gate * logistic * (1.0 - logistic))).astype(BF16)
    grad_up = (grad_hidden * gate * logistic).astype(BF16)
    grad_gate_up = jnp.concatenate([grad_gate, grad_up], axis=1)
    grad_gate_up_weight = outer_sum(normed_post, grad_gate_up).astype(BF16)
    grad_partial, grad_down, grad_gate_up_weight = lax.optimization_barrier(
        (back_matmul(grad_gate_up, gate_up_weight).astype(BF16), grad_down, grad_gate_up_weight)
    )
    grad_normed_post = scatter_sum(grad_partial, n, 3)
    grad_middle, gain_rows = rms_backward(middle, gain_post, grad_normed_post)
    grad_middle = cotangent[0].astype(F32) + grad_middle
    grad_gain_post = jnp.sum(gain_rows, axis=0)
    grad_branch = grad_middle.astype(BF16)
    grad_out = outer_sum(attended, grad_branch).astype(BF16)
    grad_attended = back_matmul(grad_branch, out_weight).astype(BF16)
    grad_q, grad_k, grad_v, grad_gain_query, grad_gain_key, mlp_landed = attend_backward(
        weights, query, key, value, grad_attended, mlp_partial, q_pre, k_pre, gain_query, gain_key,
        cosine, sine, n, 4,
    )
    result = middle + lax.dynamic_slice_in_dim(mlp_partial, me * resident, resident).astype(F32)
    output = (result + jnp.sum(mlp_landed.astype(F32), axis=0)).astype(BF16)[None]
    grad_qkv = jnp.concatenate([grad_q, grad_k, grad_v], axis=1)
    grad_qkv_weight = outer_sum(normalized, grad_qkv).astype(BF16)
    partial = back_matmul(grad_qkv, qkv_weight)
    grad_gain_in = jnp.sum(partial * unit, axis=0)
    small_grads = [grad_gain_in, grad_gain_post, grad_gain_query, grad_gain_key]
    small_grads = tile_of(jnp.concatenate([g.reshape(shards, -1) for g in small_grads], axis=1))
    grad_normed, gain_shares = scatter_last(partial.astype(BF16), small_grads, n, shards, 5)
    gain_shares = gain_shares.reshape(-1)
    grad_inputs, _ = rms_backward(inputs, gain_in, grad_normed)
    input_grad = (grad_middle + grad_inputs).astype(BF16)[None]

    def shared(grad):
        return lax.all_gather(
            lax.psum_scatter(grad, "fsdp", scatter_dimension=0, tiled=True), "seq", axis=0
        ).astype(F32)

    def beside(pieces):
        return jnp.swapaxes(pieces, 0, 1).reshape(pieces.shape[1], -1)

    final_down = shared(grad_down).reshape(-1, width)
    gate_up_all = shared(grad_gate_up_weight)

    def spread_back(pieces):
        pieces = pieces.reshape(n, pieces.shape[1], shards, hidden_piece)
        return jnp.transpose(pieces, (1, 2, 0, 3)).reshape(pieces.shape[1], -1)

    final_gate = spread_back(gate_up_all[:, :, :units])
    final_up = spread_back(gate_up_all[:, :, units:])
    final_out = lax.psum(
        lax.psum_scatter(grad_out, "fsdp", scatter_dimension=0, tiled=True), "seq"
    ).astype(F32)
    qkv_all = shared(grad_qkv_weight)
    final_query = beside(qkv_all[:, :, :split])
    final_key = beside(qkv_all[:, :, split : split + kv * HEAD_SIZE])
    final_value = beside(qkv_all[:, :, split + kv * HEAD_SIZE :])

    return (
        output,
        input_grad,
        gain_shares[:part],
        final_query,
        final_key,
        final_value,
        gain_shares[2 * part : 2 * part + small],
        gain_shares[2 * part + small : 2 * part + 2 * small],
        final_out,
        gain_shares[part : 2 * part],
        final_gate,
        final_up,
        final_down,
    )


def solution(mesh):
    flat, wide = P("fsdp"), P("fsdp", None)
    whole = P("fsdp", "seq", None)
    in_specs = (
        whole, wide, wide, flat, wide, wide, wide, flat, flat, wide, flat, wide, wide, wide, whole,
    )
    out_specs = (whole, whole, flat, wide, wide, wide, flat, flat, wide, flat, wide, wide, wide)
    return jax.shard_map(
        on_device, mesh=mesh, in_specs=in_specs, out_specs=out_specs, check_vma=False
    )
```

```python
import functools

import jax
import jax.numpy as jnp
from jax import lax
from jax.experimental import pallas as pl
from jax.experimental.pallas import tpu as pltpu
from jax.sharding import PartitionSpec as P


HQ = 16
KEY_VALUE_HEADS = 8
HEAD_SIZE = 128
GROUP = HQ // KEY_VALUE_HEADS

ROPE_BASE = 1000000.0
EPSILON = 1e-06
MASKED = -1e30
SCALE = HEAD_SIZE ** (-0.5)
MESH = pl.DeviceIdType.MESH
BF16 = jnp.bfloat16
F32 = jnp.float32


def matrix_product(left, right):
    return jnp.dot(left, right, preferred_element_type=F32)


def outer_sum(left, right):
    return lax.dot_general(left, right, (((0,), (0,)), ((), ())), preferred_element_type=F32)


def back_matmul(left, right):
    return lax.dot_general(left, right, (((1,), (1,)), ((), ())), preferred_element_type=F32)


def inverse_rms(values):
    return lax.rsqrt(jnp.mean(values * values, axis=-1, keepdims=True) + EPSILON)


def rms_backward(values, gain, grad):
    c = inverse_rms(values)
    scaled = grad * gain
    inner = jnp.mean(values * scaled, axis=-1, keepdims=True)
    return c * scaled - values * (c * c * c) * inner, grad * values * c


def greet(*axes):
    barrier = pltpu.get_barrier_semaphore()
    count = 0
    for axis in axes:
        n = lax.axis_size(axis)
        me = lax.axis_index(axis)
        for step in range(1, n):
            pl.semaphore_signal(
                barrier, inc=1, device_id={axis: lax.rem(me + step, n)}, device_id_type=MESH
            )
        count += n - 1
    pl.semaphore_wait(barrier, count)


def block_of(index, size):
    return pl.ds(pl.multiple_of(index * size, size), size)


def start_to_peers(axis, source, target, send_sem, recv_sem):
    n = lax.axis_size(axis)
    me = lax.axis_index(axis)
    copies = []
    for step in range(1, n):
        peer = lax.rem(me + step, n)
        copy = pltpu.make_async_remote_copy(
            src_ref=source(peer),
            dst_ref=target(step),
            send_sem=send_sem.at[step - 1],
            recv_sem=recv_sem.at[step - 1],
            device_id={axis: peer},
            device_id_type=MESH,
        )
        copy.start()
        copies.append(copy)
    return copies


def semaphores(*counts):
    return [pltpu.SemaphoreType.DMA((count,)) for count in counts]


VMEM_SPEC = pl.BlockSpec(memory_space=pltpu.VMEM)
ANY_SPEC = pl.BlockSpec(memory_space=pl.ANY)


def communicating(call_id, **more):
    return pltpu.CompilerParams(collective_id=call_id, has_side_effects=True, **more)


def gather_kernel(x_ref, o_ref, send_sem, recv_sem):
    greet("seq")
    mine = block_of(lax.axis_index("seq"), x_ref.shape[0])
    copies = start_to_peers(
        "seq", lambda peer: x_ref, lambda step: o_ref.at[mine], send_sem, recv_sem
    )
    o_ref[mine, :] = x_ref[...]
    for copy in copies:
        copy.wait()


def gather_rows(x, n, call_id):
    rows, width = x.shape
    return pl.pallas_call(
        gather_kernel,
        out_shape=jax.ShapeDtypeStruct((n * rows, width), x.dtype),
        in_specs=[VMEM_SPEC],
        out_specs=VMEM_SPEC,
        scratch_shapes=semaphores(n - 1, n - 1),
        compiler_params=communicating(call_id),
    )(x)


def gather_first_kernel(x_ref, gains_ref, o_ref, all_gains, send, recv, gain_send, gain_recv):
    greet("seq", "fsdp")
    place = lax.axis_index("fsdp")
    gain_copies = start_to_peers(
        "fsdp", lambda peer: gains_ref, lambda step: all_gains.at[place], gain_send, gain_recv
    )
    mine = block_of(lax.axis_index("seq"), x_ref.shape[0])
    copies = start_to_peers("seq", lambda peer: x_ref, lambda step: o_ref.at[mine], send, recv)
    o_ref[mine, :] = x_ref[...]
    all_gains[place] = gains_ref[...]
    for copy in gain_copies + copies:
        copy.wait()


def gather_first(x, gains, n, shards, call_id):
    rows, width = x.shape
    return pl.pallas_call(
        gather_first_kernel,
        out_shape=(
            jax.ShapeDtypeStruct((n * rows, width), x.dtype),
            jax.ShapeDtypeStruct((shards,) + gains.shape, gains.dtype),
        ),
        in_specs=[VMEM_SPEC, VMEM_SPEC],
        out_specs=(VMEM_SPEC, VMEM_SPEC),
        scratch_shapes=semaphores(n - 1, n - 1, shards - 1, shards - 1),
        compiler_params=communicating(call_id),
        name="gather_first",
    )(x, gains)


def scatter_kernel(p_ref, o_ref, landed, send_sem, recv_sem):
    greet("seq")
    rows = o_ref.shape[0]
    copies = start_to_peers(
        "seq",
        lambda peer: p_ref.at[block_of(peer, rows)],
        lambda step: landed.at[step - 1],
        send_sem,
        recv_sem,
    )
    o_ref[...] = p_ref[block_of(lax.axis_index("seq"), rows), :].astype(F32)
    for step, copy in enumerate(copies):
        copy.wait()
        o_ref[...] += landed[step].astype(F32)


def scatter_sum(partial, n, call_id):
    total, width = partial.shape
    rows = total // n
    return pl.pallas_call(
        scatter_kernel,
        out_shape=jax.ShapeDtypeStruct((rows, width), F32),
        in_specs=[VMEM_SPEC],
        out_specs=VMEM_SPEC,
        scratch_shapes=[pltpu.VMEM((n - 1, rows, width), partial.dtype)] + semaphores(n - 1, n - 1),
        compiler_params=communicating(call_id),
    )(partial)


def scatter_last_kernel(
    p_ref, small_ref, down_ref, gate_up_ref, o_ref, small_out, down_all, gate_up_all,
    landed, part_landed, part_sum, row_landed,
    send, recv, part_send, part_recv, row_send, row_recv, down_send, down_recv, wide_send, wide_recv,
):
    greet("seq", "fsdp")
    me = lax.axis_index("seq")
    rows = o_ref.shape[0]
    part_copies = start_to_peers(
        "fsdp",
        lambda peer: small_ref.at[peer],
        lambda step: part_landed.at[step - 1],
        part_send,
        part_recv,
    )
    copies = start_to_peers(
        "seq",
        lambda peer: p_ref.at[block_of(peer, rows)],
        lambda step: landed.at[step - 1],
        send,
        recv,
    )
    total = small_ref[lax.axis_index("fsdp")]
    for step, copy in enumerate(part_copies):
        copy.wait()
        total = total + part_landed[step]
    part_sum[...] = total
    o_ref[...] = p_ref[block_of(me, rows), :].astype(F32)
    row_copies = start_to_peers(
        "seq", lambda peer: part_sum, lambda step: row_landed.at[step - 1], row_send, row_recv
    )
    share_copies = start_to_peers(
        "seq", lambda peer: down_ref, lambda step: down_all.at[me], down_send, down_recv
    ) + start_to_peers(
        "seq", lambda peer: gate_up_ref, lambda step: gate_up_all.at[me], wide_send, wide_recv
    )
    down_all[me] = down_ref[...]
    gate_up_all[me] = gate_up_ref[...]
    for step, copy in enumerate(copies):
        copy.wait()
        o_ref[...] += landed[step].astype(F32)
    for step, copy in enumerate(row_copies):
        copy.wait()
        total = total + row_landed[step]
    small_out[...] = total
    for copy in share_copies:
        copy.wait()


def scatter_last(partial, small, down, gate_up, n, shards, call_id):
    total, width = partial.shape
    rows = total // n
    piece = small.shape[1:]
    return pl.pallas_call(
        scatter_last_kernel,
        out_shape=(
            jax.ShapeDtypeStruct((rows, width), F32),
            jax.ShapeDtypeStruct(piece, F32),
            jax.ShapeDtypeStruct((n,) + down.shape, BF16),
            jax.ShapeDtypeStruct((n,) + gate_up.shape, BF16),
        ),
        in_specs=[VMEM_SPEC] * 4,
        out_specs=(VMEM_SPEC,) * 4,
        scratch_shapes=[
            pltpu.VMEM((n - 1, rows, width), partial.dtype),
            pltpu.VMEM((shards - 1,) + piece, F32),
            pltpu.VMEM(piece, F32),
            pltpu.VMEM((n - 1,) + piece, F32),
        ]
        + semaphores(n - 1, n - 1, shards - 1, shards - 1, *([n - 1] * 6)),
        compiler_params=communicating(call_id),
        name="scatter_last",
    )(partial, small, down, gate_up)


def finish_kernel(
    qkv_ref, out_ref, q_final, k_final, v_final, out_final,
    qkv_landed, out_landed, out_mine, out_back,
    qkv_send, qkv_recv, first_send, first_recv, second_send, second_recv,
):
    greet("seq")
    n = lax.axis_size("seq")
    me = lax.axis_index("seq")
    piece = out_mine.shape[0]
    split = q_final.shape[1] // n
    narrow = k_final.shape[1] // n
    first = start_to_peers(
        "seq",
        lambda peer: out_ref.at[block_of(peer, piece)],
        lambda step: out_landed.at[step - 1],
        first_send,
        first_recv,
    )
    beside = start_to_peers(
        "seq", lambda peer: qkv_ref, lambda step: qkv_landed.at[step - 1], qkv_send, qkv_recv
    )

    def place(values, owner):
        values = values.astype(F32)
        q_final[:, block_of(owner, split)] = values[:, :split]
        k_final[:, block_of(owner, narrow)] = values[:, split : split + narrow]
        v_final[:, block_of(owner, narrow)] = values[:, split + narrow :]

    total = out_ref[block_of(me, piece), :].astype(F32)
    for step, copy in enumerate(first):
        copy.wait()
        total = total + out_landed[step].astype(F32)
    out_mine[...] = total.astype(BF16)
    out_final[block_of(me, piece), :] = out_mine[...].astype(F32)
    place(qkv_ref[...], me)
    second = start_to_peers(
        "seq", lambda peer: out_mine, lambda step: out_back.at[step - 1], second_send, second_recv
    )
    for step, copy in enumerate(beside):
        copy.wait()
        place(qkv_landed[step], lax.rem(me + n - 1 - step, n))
    for step, copy in enumerate(second):
        copy.wait()
        owner = lax.rem(me + n - 1 - step, n)
        out_final[block_of(owner, piece), :] = out_back[step].astype(F32)


def finish(qkv, out, widths, n, call_id):
    rows, width = out.shape
    return pl.pallas_call(
        finish_kernel,
        out_shape=tuple(jax.ShapeDtypeStruct((qkv.shape[0], size), F32) for size in widths)
        + (jax.ShapeDtypeStruct(out.shape, F32),),
        in_specs=[VMEM_SPEC] * 2,
        out_specs=(VMEM_SPEC,) * 4,
        scratch_shapes=[
            pltpu.VMEM((n - 1,) + qkv.shape, BF16),
            pltpu.VMEM((n - 1, rows // n, width), BF16),
            pltpu.VMEM((rows // n, width), BF16),
            pltpu.VMEM((n - 1, rows // n, width), BF16),
        ]
        + semaphores(*([n - 1] * 6)),
        compiler_params=communicating(call_id),
        name="finish",
    )(qkv, out)


def spread_kernel(hidden_piece, pieces_ref, gate_ref, up_ref):
    n, _, width = pieces_ref.shape
    units = width // 2
    span = n * hidden_piece
    for target, base in ((gate_ref, 0), (up_ref, units)):
        for shard in range(units // hidden_piece):
            at = base + shard * hidden_piece
            target[:, shard * span : (shard + 1) * span] = jnp.concatenate(
                [pieces_ref[s, :, at : at + hidden_piece].astype(F32) for s in range(n)], axis=1
            )


def spread_back(pieces, hidden_piece):
    n, rows, width = pieces.shape
    shape = jax.ShapeDtypeStruct((rows, n * width // 2), F32)
    return pl.pallas_call(
        functools.partial(spread_kernel, hidden_piece),
        out_shape=(shape, shape),
        in_specs=[VMEM_SPEC],
        out_specs=(VMEM_SPEC, VMEM_SPEC),
        name="spread_back",
    )(pieces)


def rope(values, cosine, sine):
    return values * cosine + pltpu.roll(values, HEAD_SIZE // 2, 1) * sine


def rope_back(grad, cosine, sine):
    return grad * cosine - pltpu.roll(grad, HEAD_SIZE // 2, 1) * sine


def head_columns(index):
    return pl.ds(pl.multiple_of(index * HEAD_SIZE, HEAD_SIZE), HEAD_SIZE)


def turned_block(shift):
    def block(i):
        return lax.rem(lax.axis_index("seq") + shift + i, lax.axis_size("seq"))

    return block


def forward_kernel(
    q_pre, k_pre, v_ref, gain_q, gain_k, cos_q, sin_q, cos_k, sin_k, place_k, place_q, start_q, cot,
    out_ref, p_ref, q_ref, k_ref, cot_all,
    v_turned, outs, cot_send, cot_recv, cot_local, send, recv, local,
):
    i, head = pl.program_id(0), pl.program_id(1)
    n, heads = pl.num_programs(0), pl.num_programs(1)
    seq = lax.axis_size("seq")
    me = lax.axis_index("seq")
    kv = outs.shape[1] // GROUP
    rows = cot.shape[0]
    mine = block_of(me, rows)

    def cot_copies():
        return [
            pltpu.make_async_remote_copy(
                src_ref=cot,
                dst_ref=cot_all.at[mine],
                send_sem=cot_send.at[step - 1],
                recv_sem=cot_recv.at[step - 1],
                device_id={"seq": lax.rem(me + step, seq)},
                device_id_type=MESH,
            )
            for step in range(1, seq)
        ]

    cot_own = pltpu.make_async_copy(cot, cot_all.at[mine], cot_local)

    def out_copy(step, which):
        return pltpu.make_async_remote_copy(
            src_ref=outs.at[step, which],
            dst_ref=out_ref.at[:, head_columns(me * heads + which)],
            send_sem=send.at[step, which],
            recv_sem=recv.at[step, which],
            device_id={"seq": lax.rem(me + 1 + step, seq)},
            device_id_type=MESH,
        )

    def own_copy(which):
        return pltpu.make_async_copy(
            outs.at[seq - 1, which], out_ref.at[:, head_columns(me * heads + which)], local.at[which]
        )

    @pl.when((i == 0) & (head == 0))
    def _():
        greet("seq")
        for copy in cot_copies():
            copy.start()
        cot_own.start()
        for which in range(kv):
            own = pl.ds(which * HEAD_SIZE, HEAD_SIZE)
            pre = k_pre[:, own]
            k_ref[:, own] = rope(
                pre * inverse_rms(pre) * gain_k[...], cos_k[...], sin_k[...]
            ).astype(BF16)
            v_turned[which] = v_ref[:, own].astype(F32).T.astype(BF16)

    @pl.when((head > 0) & (i < n - 1))
    def _():
        out_copy(i, head - 1).start()

    @pl.when((head == 0) & (i > 0))
    def _():
        out_copy(i - 1, heads - 1).start()

    pre = q_pre[...]
    query = rope(pre * inverse_rms(pre) * gain_q[...], cos_q[...], sin_q[...]).astype(BF16)
    q_ref[...] = query
    pair = head // GROUP
    scores = back_matmul(k_ref[:, head_columns(pair)], query) * SCALE
    keys = place_k[...]
    allowed = (keys <= place_q[...]) & (keys >= start_q[...])
    scores = jnp.where(allowed, scores, MASKED)
    top = jnp.max(scores, axis=0, keepdims=True)
    weights = jnp.exp(scores - top)
    total = jnp.sum(weights, axis=0, keepdims=True)
    weights = (weights * (1.0 / total)).astype(BF16)
    p_ref[0] = weights
    outs[i, head] = matrix_product(v_turned[pair], weights).T.astype(BF16)

    @pl.when((i == n - 1) & (head == heads - 1))
    def _():
        for which in range(outs.shape[1]):
            own_copy(which).start()
        for copy in cot_copies():
            copy.wait()
        cot_own.wait()
        for step in range(seq - 1):
            for which in range(outs.shape[1]):
                out_copy(step, which).wait()
        for which in range(outs.shape[1]):
            own_copy(which).wait()


def attend_forward(
    q_pre, k_pre, value, gain_q, gain_k, cosine, sine, place, start, cotangent, n, call_id
):
    rows = q_pre.shape[0]
    heads = q_pre.shape[1] // HEAD_SIZE
    kv = heads // GROUP
    block = rows // n
    width = cotangent.shape[1]
    turn = turned_block(1)
    q_spec = pl.BlockSpec((block, HEAD_SIZE), lambda i, h: (turn(i), h))
    k_spec = pl.BlockSpec((rows, kv * HEAD_SIZE), lambda i, h: (0, 0))
    gain_spec = pl.BlockSpec((1, HEAD_SIZE), lambda i, h: (0, 0))
    trig_q = pl.BlockSpec((block, HEAD_SIZE), lambda i, h: (turn(i), 0))
    trig_k = pl.BlockSpec((rows, HEAD_SIZE), lambda i, h: (0, 0))
    column = pl.BlockSpec((rows, 1), lambda i, h: (0, 0))
    row = pl.BlockSpec((1, block), lambda i, h: (0, turn(i)))
    return pl.pallas_call(
        forward_kernel,
        grid=(n, heads),
        out_shape=(
            jax.ShapeDtypeStruct((block, n * heads * HEAD_SIZE), BF16),
            jax.ShapeDtypeStruct((heads, rows, rows), BF16),
            jax.ShapeDtypeStruct((rows, heads * HEAD_SIZE), BF16),
            jax.ShapeDtypeStruct((rows, kv * HEAD_SIZE), BF16),
            jax.ShapeDtypeStruct((rows, width), BF16),
        ),
        in_specs=[
            q_spec, k_spec, k_spec, gain_spec, gain_spec, trig_q, trig_q, trig_k, trig_k,
            column, row, row, ANY_SPEC,
        ],
        out_specs=(
            ANY_SPEC,
            pl.BlockSpec((1, rows, block), lambda i, h: (h, 0, turn(i))),
            q_spec,
            k_spec,
            ANY_SPEC,
        ),
        scratch_shapes=[
            pltpu.VMEM((kv, HEAD_SIZE, rows), BF16),
            pltpu.VMEM((n, heads, block, HEAD_SIZE), BF16),
            pltpu.SemaphoreType.DMA((n - 1,)),
            pltpu.SemaphoreType.DMA((n - 1,)),
            pltpu.SemaphoreType.DMA,
            pltpu.SemaphoreType.DMA((n - 1, heads)),
            pltpu.SemaphoreType.DMA((n - 1, heads)),
            pltpu.SemaphoreType.DMA((heads,)),
        ],
        compiler_params=communicating(call_id),
        name="attend_forward",
    )(
        q_pre, k_pre, value, gain_q, gain_k, cosine, sine, cosine, sine,
        place[:, None], place[None, :], start[None, :], cotangent,
    )


def backward_kernel(
    p_ref, q_ref, k_ref, v_ref, q_pre, k_pre, gain_q, gain_k, cos_q, sin_q, cos_k, sin_k,
    grad_own, bulk,
    dq_ref, dk_ref, dv_ref, dgain_q, dgain_k, bulk_landed,
    k_turned, dk_sum, dv_sum, grads, send, recv, local, bulk_send, bulk_recv,
):
    i, head = pl.program_id(0), pl.program_id(1)
    n, heads = pl.num_programs(0), pl.num_programs(1)
    seq = lax.axis_size("seq")
    me = lax.axis_index("seq")
    kv = k_turned.shape[0]
    rows = grads.shape[1]
    span = grads.shape[2]
    first = (i == 0) & (head == 0)
    last = (i == n - 1) & (head == heads - 1)

    def grad_copy(step):
        peer = lax.rem(me + step, seq)
        return pltpu.make_async_remote_copy(
            src_ref=grad_own.at[:, block_of(peer, span)],
            dst_ref=grads.at[step],
            send_sem=send.at[step - 1],
            recv_sem=recv.at[step - 1],
            device_id={"seq": peer},
            device_id_type=MESH,
        )

    def bulk_copy(step):
        peer = lax.rem(me + step, seq)
        return pltpu.make_async_remote_copy(
            src_ref=bulk.at[block_of(peer, rows)],
            dst_ref=bulk_landed.at[step - 1],
            send_sem=bulk_send.at[step - 1],
            recv_sem=bulk_recv.at[step - 1],
            device_id={"seq": peer},
            device_id_type=MESH,
        )

    own_copy = pltpu.make_async_copy(grad_own.at[:, block_of(me, span)], grads.at[0], local)

    @pl.when(first)
    def _():
        greet("seq")
        own_copy.start()
        for step in range(1, seq):
            grad_copy(step).start()
        for step in range(1, seq):
            bulk_copy(step).start()
        dgain_q[...] = jnp.zeros_like(dgain_q)
        dgain_k[...] = jnp.zeros_like(dgain_k)
        dk_sum[...] = jnp.zeros_like(dk_sum)
        dv_sum[...] = jnp.zeros_like(dv_sum)
        for which in range(kv):
            own = pl.ds(which * HEAD_SIZE, HEAD_SIZE)
            k_turned[which] = k_ref[:, own].astype(F32).T.astype(BF16)
        own_copy.wait()

    for step in range(1, seq):
        @pl.when((head == 0) & (i == seq - step))
        def _():
            grad_copy(step).wait_recv()

    slot = lax.rem(seq - i, seq)
    pair = head // GROUP
    rounded = p_ref[0]
    weights = rounded.astype(F32)
    grad = grads[slot, :, head_columns(head)]
    grad_weights = back_matmul(v_ref[:, head_columns(pair)], grad)
    delta = jnp.sum(weights * grad_weights, axis=0, keepdims=True)
    grad_scores = (weights * (grad_weights - delta)).astype(BF16)
    dk_sum[pair] += matrix_product(grad_scores, q_ref[...])
    dv_sum[pair] += matrix_product(rounded, grad)
    dq = (matrix_product(k_turned[pair], grad_scores).T * SCALE).astype(BF16).astype(F32)
    dq, gain_rows = rms_backward(q_pre[...], gain_q[...], rope_back(dq, cos_q[...], sin_q[...]))
    dq_ref[...] = dq.astype(BF16)
    dgain_q[...] += jnp.sum(gain_rows, axis=0, keepdims=True)

    @pl.when(last)
    def _():
        for which in range(kv):
            own = pl.ds(which * HEAD_SIZE, HEAD_SIZE)
            dk = (dk_sum[which] * SCALE).astype(BF16).astype(F32)
            dk, gain_rows = rms_backward(
                k_pre[:, own], gain_k[...], rope_back(dk, cos_k[...], sin_k[...])
            )
            dk_ref[:, own] = dk.astype(BF16)
            dgain_k[...] += jnp.sum(gain_rows, axis=0, keepdims=True)
            dv_ref[:, own] = dv_sum[which].astype(BF16)
        for step in range(1, seq):
            grad_copy(step).wait_send()
            bulk_copy(step).wait()


def attend_backward(
    weights, query, key, value, grad_own, bulk, q_pre, k_pre, gain_q, gain_k, cosine, sine, n, call_id
):
    rows = q_pre.shape[0]
    heads = q_pre.shape[1] // HEAD_SIZE
    kv = heads // GROUP
    block = rows // n
    turn = turned_block(0)
    q_spec = pl.BlockSpec((block, HEAD_SIZE), lambda i, h: (turn(i), h))
    k_spec = pl.BlockSpec((rows, kv * HEAD_SIZE), lambda i, h: (0, 0))
    gain_spec = pl.BlockSpec((1, HEAD_SIZE), lambda i, h: (0, 0))
    trig_q = pl.BlockSpec((block, HEAD_SIZE), lambda i, h: (turn(i), 0))
    trig_k = pl.BlockSpec((rows, HEAD_SIZE), lambda i, h: (0, 0))
    return pl.pallas_call(
        backward_kernel,
        grid=(n, heads),
        out_shape=(
            jax.ShapeDtypeStruct((rows, heads * HEAD_SIZE), BF16),
            jax.ShapeDtypeStruct((rows, kv * HEAD_SIZE), BF16),
            jax.ShapeDtypeStruct((rows, kv * HEAD_SIZE), BF16),
            jax.ShapeDtypeStruct((1, HEAD_SIZE), F32),
            jax.ShapeDtypeStruct((1, HEAD_SIZE), F32),
            jax.ShapeDtypeStruct((n - 1, block, bulk.shape[1]), BF16),
        ),
        in_specs=[
            pl.BlockSpec((1, rows, block), lambda i, h: (h, 0, turn(i))),
            q_spec, k_spec, k_spec, q_spec, k_spec, gain_spec, gain_spec,
            trig_q, trig_q, trig_k, trig_k, ANY_SPEC, ANY_SPEC,
        ],
        out_specs=(q_spec, k_spec, k_spec, gain_spec, gain_spec, ANY_SPEC),
        scratch_shapes=[
            pltpu.VMEM((kv, HEAD_SIZE, rows), BF16),
            pltpu.VMEM((kv, rows, HEAD_SIZE), F32),
            pltpu.VMEM((kv, rows, HEAD_SIZE), F32),
            pltpu.VMEM((n, block, heads * HEAD_SIZE), BF16),
            pltpu.SemaphoreType.DMA((n - 1,)),
            pltpu.SemaphoreType.DMA((n - 1,)),
            pltpu.SemaphoreType.DMA,
            pltpu.SemaphoreType.DMA((n - 1,)),
            pltpu.SemaphoreType.DMA((n - 1,)),
        ],
        compiler_params=communicating(call_id),
        name="attend_backward",
    )(
        weights, query, key, value, q_pre, k_pre, gain_q, gain_k, cosine, sine, cosine, sine,
        grad_own, bulk,
    )


def on_device(
    tokens, lengths, packing, norm_in, w_query, key_projection, value_projection, norm_query,
    norm_key, w_out, norm_post, w_gate, w_up, w_down, cotangent,
):
    n = lax.axis_size("seq")
    shards = lax.axis_size("fsdp")
    me = lax.axis_index("seq")
    resident = tokens.shape[1]
    width = tokens.shape[2]
    rows = resident * n
    heads = HQ // n
    kv = KEY_VALUE_HEADS // n
    hidden_piece = w_down.shape[0] // n

    def columns(weight, pieces):
        size = weight.shape[1] // pieces
        return lax.dynamic_slice_in_dim(weight, me * size, size, axis=1)

    def spread_columns(weight):
        pieces = weight.reshape(weight.shape[0], shards, n, hidden_piece)
        return lax.dynamic_index_in_dim(pieces, me, axis=2, keepdims=False).reshape(
            weight.shape[0], shards * hidden_piece
        )

    def tile_of(values):
        pad = 1024 - values.shape[-1]
        values = jnp.concatenate([values, jnp.zeros(values.shape[:-1] + (pad,), F32)], axis=-1)
        return values.reshape(values.shape[:-1] + (8, 128))

    part, small = norm_in.shape[0], norm_query.shape[0]
    whole, gains = gather_first(
        tokens[0],
        tile_of(jnp.concatenate([norm_in, norm_post, norm_query, norm_key]).astype(F32)),
        n, shards, 0,
    )
    gains = gains.reshape(shards, -1)
    gain_in = gains[:, :part].reshape(1, -1)
    gain_post = gains[:, part : 2 * part].reshape(1, -1)
    gain_query = gains[:, 2 * part : 2 * part + small].reshape(1, -1)
    gain_key = gains[:, 2 * part + small : 2 * part + 2 * small].reshape(1, -1)

    qkv_weight = lax.all_gather(
        jnp.concatenate(
            [columns(w_query, n), columns(key_projection, n), columns(value_projection, n)], axis=1
        ),
        "fsdp", axis=0, tiled=True,
    )
    out_weight = lax.all_gather(w_out, "fsdp", axis=0, tiled=True)
    gate_up_weight = lax.all_gather(
        jnp.concatenate([spread_columns(w_gate), spread_columns(w_up)], axis=1), "fsdp", axis=0, tiled=True
    )
    down_weight = lax.all_gather(
        lax.dynamic_slice_in_dim(w_down, me * hidden_piece, hidden_piece, axis=0),
        "fsdp", axis=0, tiled=True,
    )

    order = packing[0]
    places = jnp.arange(rows, dtype=jnp.int32)
    place = jnp.sum(jnp.where(order[None, :] == places[:, None], places[None, :], 0), axis=1)
    ends = jnp.cumsum(lengths[0])
    start = jnp.sum(jnp.where(place[:, None] >= ends[None, :], lengths[0][None, :], 0), axis=1)
    half = HEAD_SIZE // 2
    inv_freq = ROPE_BASE ** (-jnp.arange(half, dtype=F32) / half)
    angles = (place - start).astype(F32)[:, None] * inv_freq[None, :]
    cosine, sine = jnp.cos(angles), jnp.sin(angles)
    cosine = jnp.concatenate([cosine, cosine], axis=1)
    sine = jnp.concatenate([-sine, sine], axis=1)

    inputs = tokens[0].astype(F32)
    whole_f32 = whole.astype(F32)
    unit = whole_f32 * inverse_rms(whole_f32)
    normalized = (unit * gain_in).astype(BF16)
    qkv = matrix_product(normalized, qkv_weight)
    split = heads * HEAD_SIZE
    q_pre = qkv[:, :split]
    k_pre = qkv[:, split : split + kv * HEAD_SIZE]
    value = qkv[:, split + kv * HEAD_SIZE :].astype(BF16)
    attended, weights, query, key, grad_mlp = attend_forward(
        q_pre, k_pre, value, gain_query, gain_key, cosine, sine, place, start, cotangent[0], n, 1
    )
    middle = inputs + matrix_product(attended, out_weight)
    normed_post_mine = (middle * inverse_rms(middle) * gain_post).astype(BF16)
    normed_post = gather_rows(normed_post_mine, n, 2)

    gate_up = matrix_product(normed_post, gate_up_weight)
    units = shards * hidden_piece
    gate, up = gate_up[:, :units], gate_up[:, units:]
    logistic = 1.0 / (1.0 + jnp.exp(-gate))
    hidden = (gate / (1.0 + jnp.exp(-gate)) * up).astype(BF16)
    mlp_partial = matrix_product(hidden, down_weight).astype(BF16)

    grad_hidden = back_matmul(grad_mlp, down_weight)
    grad_down = outer_sum(hidden, grad_mlp).astype(BF16)
    grad_gate = (grad_hidden * up * (logistic + gate * logistic * (1.0 - logistic))).astype(BF16)
    grad_up = (grad_hidden * gate * logistic).astype(BF16)
    grad_gate_up = jnp.concatenate([grad_gate, grad_up], axis=1)
    grad_gate_up_weight = outer_sum(normed_post, grad_gate_up).astype(BF16)
    grad_partial, grad_down, grad_gate_up_weight = lax.optimization_barrier(
        (back_matmul(grad_gate_up, gate_up_weight).astype(BF16), grad_down, grad_gate_up_weight)
    )
    down_share = lax.psum_scatter(grad_down, "fsdp", scatter_dimension=0, tiled=True)
    gate_up_share = lax.psum_scatter(grad_gate_up_weight, "fsdp", scatter_dimension=0, tiled=True)
    grad_normed_post = scatter_sum(grad_partial, n, 3)
    grad_middle, gain_rows = rms_backward(middle, gain_post, grad_normed_post)
    grad_middle = cotangent[0].astype(F32) + grad_middle
    grad_gain_post = jnp.sum(gain_rows, axis=0)
    grad_branch = grad_middle.astype(BF16)
    grad_out = outer_sum(attended, grad_branch).astype(BF16)
    out_share = lax.psum_scatter(grad_out, "fsdp", scatter_dimension=0, tiled=True)
    grad_attended = back_matmul(grad_branch, out_weight).astype(BF16)
    grad_q, grad_k, grad_v, grad_gain_query, grad_gain_key, mlp_landed = attend_backward(
        weights, query, key, value, grad_attended, mlp_partial, q_pre, k_pre, gain_query,
        gain_key, cosine, sine, n, 4,
    )
    result = middle + lax.dynamic_slice_in_dim(mlp_partial, me * resident, resident).astype(F32)
    output = (result + jnp.sum(mlp_landed.astype(F32), axis=0)).astype(BF16)[None]
    grad_qkv = jnp.concatenate([grad_q, grad_k, grad_v], axis=1)
    grad_qkv_weight = outer_sum(normalized, grad_qkv).astype(BF16)
    qkv_share = lax.psum_scatter(grad_qkv_weight, "fsdp", scatter_dimension=0, tiled=True)
    partial = back_matmul(grad_qkv, qkv_weight)
    grad_gain_in = jnp.sum(partial * unit, axis=0)
    small_grads = [grad_gain_in, grad_gain_post, grad_gain_query, grad_gain_key]
    small_grads = tile_of(jnp.concatenate([g.reshape(shards, -1) for g in small_grads], axis=1))
    grad_normed, gain_shares, down_all, gate_up_all = scatter_last(
        partial.astype(BF16), small_grads, down_share, gate_up_share, n, shards, 5
    )
    gain_shares = gain_shares.reshape(-1)
    grad_inputs, _ = rms_backward(inputs, gain_in, grad_normed)
    input_grad = (grad_middle + grad_inputs).astype(BF16)[None]

    final_down = down_all.astype(F32).reshape(-1, width)
    final_gate, final_up = spread_back(gate_up_all, hidden_piece)
    final_query, final_key, final_value, final_out = finish(
        qkv_share, out_share, (HQ * HEAD_SIZE,) + (KEY_VALUE_HEADS * HEAD_SIZE,) * 2, n, 6
    )

    return (
        output,
        input_grad,
        gain_shares[:part],
        final_query,
        final_key,
        final_value,
        gain_shares[2 * part : 2 * part + small],
        gain_shares[2 * part + small : 2 * part + 2 * small],
        final_out,
        gain_shares[part : 2 * part],
        final_gate,
        final_up,
        final_down,
    )


def solution(mesh):
    flat, wide = P("fsdp"), P("fsdp", None)
    whole = P("fsdp", "seq", None)
    in_specs = (
        whole, wide, wide, flat, wide, wide, wide, flat, flat, wide, flat, wide, wide, wide, whole,
    )
    out_specs = (whole, whole, flat, wide, wide, wide, flat, flat, wide, flat, wide, wide, wide)

    return jax.shard_map(
        on_device, mesh=mesh, in_specs=in_specs, out_specs=out_specs, check_vma=False
    )
```

```python
import functools

import jax
import jax.numpy as jnp
from jax import lax
from jax.experimental import pallas as pl
from jax.experimental.pallas import tpu as pltpu
from jax.sharding import PartitionSpec as P


HQ = 16
KEY_VALUE_HEADS = 8
HEAD_SIZE = 128
GROUP = HQ // KEY_VALUE_HEADS

ROPE_BASE = 1000000.0
EPSILON = 1e-06
MASKED = -1e30
SCALE = HEAD_SIZE ** (-0.5)
MESH = pl.DeviceIdType.MESH
BF16 = jnp.bfloat16
F32 = jnp.float32


def matrix_product(left, right):
    return jnp.dot(left, right, preferred_element_type=F32)


def outer_sum(left, right):
    return lax.dot_general(left, right, (((0,), (0,)), ((), ())), preferred_element_type=F32)


def back_matmul(left, right):
    return lax.dot_general(left, right, (((1,), (1,)), ((), ())), preferred_element_type=F32)


def inverse_rms(values):
    return lax.rsqrt(jnp.mean(values * values, axis=-1, keepdims=True) + EPSILON)


def rms_backward(values, gain, grad):
    c = inverse_rms(values)
    scaled = grad * gain
    inner = jnp.mean(values * scaled, axis=-1, keepdims=True)
    return c * scaled - values * (c * c * c) * inner, grad * values * c


def greet(*axes):
    barrier = pltpu.get_barrier_semaphore()
    count = 0
    for axis in axes:
        n = lax.axis_size(axis)
        me = lax.axis_index(axis)
        for step in range(1, n):
            pl.semaphore_signal(
                barrier, inc=1, device_id={axis: lax.rem(me + step, n)}, device_id_type=MESH
            )
        count += n - 1
    pl.semaphore_wait(barrier, count)


def block_of(index, size):
    return pl.ds(pl.multiple_of(index * size, size), size)


def start_to_peers(axis, source, target, send_sem, recv_sem):
    n = lax.axis_size(axis)
    me = lax.axis_index(axis)
    copies = []
    for step in range(1, n):
        peer = lax.rem(me + step, n)
        copy = pltpu.make_async_remote_copy(
            src_ref=source(peer),
            dst_ref=target(step),
            send_sem=send_sem.at[step - 1],
            recv_sem=recv_sem.at[step - 1],
            device_id={axis: peer},
            device_id_type=MESH,
        )
        copy.start()
        copies.append(copy)
    return copies


def semaphores(*counts):
    return [pltpu.SemaphoreType.DMA((count,)) for count in counts]


VMEM_SPEC = pl.BlockSpec(memory_space=pltpu.VMEM)
ANY_SPEC = pl.BlockSpec(memory_space=pl.ANY)


def communicating(call_id, **more):
    return pltpu.CompilerParams(collective_id=call_id, has_side_effects=True, **more)


def remote(source, target, send_sem, recv_sem, peer):
    return pltpu.make_async_remote_copy(
        src_ref=source,
        dst_ref=target,
        send_sem=send_sem,
        recv_sem=recv_sem,
        device_id={"seq": peer},
        device_id_type=MESH,
    )


class Plane:
    def __init__(self):
        self.n = lax.axis_size("seq")
        self.ny = self.n // 2
        self.me = lax.axis_index("seq")
        self.x = lax.rem(self.me, 2)
        self.y = self.me // 2

    def at(self, j, across):
        row = lax.rem(self.y + j + self.ny, self.ny)
        return row * 2 + ((1 - self.x) if across else self.x)


class RelayGather(Plane):
    def __init__(self, source, target, sems):
        super().__init__()
        self.source, self.target = source, target
        self.sx, self.rx, self.sy, self.ry, self.sy2, self.ry2, self.sx2, self.rx2 = sems

    @staticmethod
    def semaphores(n):
        ny = n // 2
        dma = pltpu.SemaphoreType.DMA
        return [dma((2,))] * 2 + [dma((ny - 1, 2))] * 2 + [dma((ny - 1,))] * 4

    def x1(self, half):
        return remote(
            self.source(half), self.target(self.me, half), self.sx.at[half], self.rx.at[half],
            self.at(0, True),
        )

    def y1(self, j, half):
        return remote(
            self.source(half), self.target(self.me, half), self.sy.at[j - 1, half],
            self.ry.at[j - 1, half], self.at(j, False),
        )

    def y2(self, j):
        block = self.target(self.at(0, True), 0)
        return remote(block, block, self.sy2.at[j - 1], self.ry2.at[j - 1], self.at(j, False))

    def x2(self, j):
        block = self.target(self.at(-j, False), 1)
        return remote(block, block, self.sx2.at[j - 1], self.rx2.at[j - 1], self.at(0, True))

    def start(self):
        others = range(1, self.ny)
        self.x1(0).start()
        for j in others:
            self.y1(j, 1).start()
        self.x1(1).start()
        for j in others:
            self.y1(j, 0).start()

    def forward(self):
        others = range(1, self.ny)
        self.x1(0).wait_recv()
        for j in others:
            self.y2(j).start()
        for j in others:
            self.y1(j, 1).wait_recv()
            self.x2(j).start()

    def finish(self):
        self.x1(0).wait_send()
        self.x1(1).wait()
        for j in range(1, self.ny):
            self.y1(j, 1).wait_send()
            self.y1(j, 0).wait()
            self.y2(j).wait()
            self.x2(j).wait()


def row_halves(ref, rows, owner, half):
    size = rows // 2
    return ref.at[pl.ds(pl.multiple_of(owner * rows + half * size, size), size)]


def column_halves(ref, half):
    size = ref.shape[-1] // 2
    return ref.at[:, half * size : (half + 1) * size]


def gather_by_rows(x_ref, o_ref, sems):
    rows = x_ref.shape[0]
    return RelayGather(
        lambda half: row_halves(x_ref, rows, 0, half),
        lambda owner, half: row_halves(o_ref, rows, owner, half),
        sems,
    )


def gather_by_columns(x_ref, o_ref, sems):
    return RelayGather(
        lambda half: column_halves(x_ref, half),
        lambda owner, half: column_halves(o_ref.at[owner], half),
        sems,
    )


class RelayScatter(Plane):
    def __init__(self, partial, buffers, sems):
        super().__init__()
        self.partial = partial
        self.rows = partial.shape[0] // self.n
        self.from_x, self.from_y, self.sent_y, self.late_y, self.sent_x, self.late_x = buffers
        self.sx, self.rx, self.sy, self.ry, self.sy2, self.ry2, self.sx2, self.rx2 = sems

    @staticmethod
    def scratch(n, rows, width):
        ny, half = n // 2, rows // 2
        dma = pltpu.SemaphoreType.DMA
        return [
            pltpu.VMEM((ny, half, width), BF16),
            pltpu.VMEM((ny - 1, 2, half, width), BF16),
            pltpu.VMEM((ny - 1, half, width), BF16),
            pltpu.VMEM((ny - 1, half, width), BF16),
            pltpu.VMEM((half, width), BF16),
            pltpu.VMEM((half, width), BF16),
        ] + [dma((ny,))] * 2 + [dma((ny - 1, 2))] * 2 + [dma((ny - 1,))] * 2 + [dma((1,))] * 2

    def piece(self, owner, half):
        return row_halves(self.partial, self.rows, owner, half)

    def x1(self, j):
        return remote(
            self.piece(self.at(j, True), 0), self.from_x.at[j], self.sx.at[j], self.rx.at[j],
            self.at(0, True),
        )

    def y1(self, j, final):
        return remote(
            self.piece(self.at(j, not final), 1), self.from_y.at[j - 1, int(final)],
            self.sy.at[j - 1, int(final)], self.ry.at[j - 1, int(final)], self.at(j, False),
        )

    def y2(self, j):
        return remote(
            self.sent_y.at[j - 1], self.late_y.at[j - 1], self.sy2.at[j - 1], self.ry2.at[j - 1],
            self.at(j, False),
        )

    def x2(self):
        return remote(self.sent_x, self.late_x, self.sx2.at[0], self.rx2.at[0], self.at(0, True))

    def start(self):
        others = range(1, self.ny)
        for j in others:
            self.x1(j).start()
            self.y1(j, False).start()
        self.x1(0).start()
        for j in others:
            self.y1(j, True).start()

    def forward(self, o_ref):
        others = range(1, self.ny)
        half = self.rows // 2
        for j in others:
            self.x1(j).wait_recv()
            own = self.piece(self.at(j, False), 0)[...].astype(F32)
            self.sent_y[j - 1] = (own + self.from_x[j].astype(F32)).astype(BF16)
        total = self.piece(self.at(0, True), 1)[...].astype(F32)
        for j in others:
            self.y1(j, False).wait_recv()
            total = total + self.from_y[j - 1, 0].astype(F32)
        self.sent_x[...] = total.astype(BF16)
        for j in others:
            self.y2(j).start()
        o_ref[:half, :] = self.piece(self.me, 0)[...].astype(F32)
        self.x2().start()
        o_ref[half:, :] = self.piece(self.me, 1)[...].astype(F32)

    def finish(self, o_ref):
        others = range(1, self.ny)
        half = self.rows // 2
        self.x1(0).wait()
        first = o_ref[:half, :] + self.from_x[0].astype(F32)
        second = o_ref[half:, :]
        for j in others:
            self.x1(j).wait_send()
            self.y1(j, False).wait_send()
            self.y1(j, True).wait()
            second = second + self.from_y[j - 1, 1].astype(F32)
        for j in others:
            self.y2(j).wait()
            first = first + self.late_y[j - 1].astype(F32)
        o_ref[:half, :] = first
        self.x2().wait()
        o_ref[half:, :] = second + self.late_x[...].astype(F32)


def gather_kernel(x_ref, o_ref, *sems):
    greet("seq")
    relay = gather_by_rows(x_ref, o_ref, sems)
    relay.start()
    o_ref[block_of(lax.axis_index("seq"), x_ref.shape[0]), :] = x_ref[...]
    relay.forward()
    relay.finish()


def gather_rows(x, n, call_id):
    rows, width = x.shape
    return pl.pallas_call(
        gather_kernel,
        out_shape=jax.ShapeDtypeStruct((n * rows, width), x.dtype),
        in_specs=[VMEM_SPEC],
        out_specs=VMEM_SPEC,
        scratch_shapes=RelayGather.semaphores(n),
        compiler_params=communicating(call_id),
    )(x)


def gather_first_kernel(x_ref, gains_ref, o_ref, all_gains, gain_send, gain_recv, *sems):
    greet("seq", "fsdp")
    place = lax.axis_index("fsdp")
    gain_copies = start_to_peers(
        "fsdp", lambda peer: gains_ref, lambda step: all_gains.at[place], gain_send, gain_recv
    )
    relay = gather_by_rows(x_ref, o_ref, sems)
    relay.start()
    o_ref[block_of(lax.axis_index("seq"), x_ref.shape[0]), :] = x_ref[...]
    all_gains[place] = gains_ref[...]
    relay.forward()
    relay.finish()
    for copy in gain_copies:
        copy.wait()


def gather_first(x, gains, n, shards, call_id):
    rows, width = x.shape
    return pl.pallas_call(
        gather_first_kernel,
        out_shape=(
            jax.ShapeDtypeStruct((n * rows, width), x.dtype),
            jax.ShapeDtypeStruct((shards,) + gains.shape, gains.dtype),
        ),
        in_specs=[VMEM_SPEC, VMEM_SPEC],
        out_specs=(VMEM_SPEC, VMEM_SPEC),
        scratch_shapes=semaphores(shards - 1, shards - 1) + RelayGather.semaphores(n),
        compiler_params=communicating(call_id),
        name="gather_first",
    )(x, gains)


def scatter_kernel(p_ref, o_ref, *scratch):
    greet("seq")
    relay = RelayScatter(p_ref, scratch[:6], scratch[6:])
    relay.start()
    relay.forward(o_ref)
    relay.finish(o_ref)


def scatter_sum(partial, n, call_id):
    total, width = partial.shape
    rows = total // n
    return pl.pallas_call(
        scatter_kernel,
        out_shape=jax.ShapeDtypeStruct((rows, width), F32),
        in_specs=[VMEM_SPEC],
        out_specs=VMEM_SPEC,
        scratch_shapes=RelayScatter.scratch(n, rows, width),
        compiler_params=communicating(call_id),
    )(partial)


def scatter_last_kernel(
    p_ref, small_ref, down_ref, gate_up_ref, o_ref, small_out, down_all, gate_up_all,
    part_landed, part_sum, row_landed, part_send, part_recv, row_send, row_recv, *scratch,
):
    greet("seq", "fsdp")
    me = lax.axis_index("seq")
    part_copies = start_to_peers(
        "fsdp",
        lambda peer: small_ref.at[peer],
        lambda step: part_landed.at[step - 1],
        part_send,
        part_recv,
    )
    relay = RelayScatter(p_ref, scratch[:6], scratch[6:14])
    down = gather_by_columns(down_ref, down_all, scratch[14:22])
    gate_up = gather_by_columns(gate_up_ref, gate_up_all, scratch[22:30])
    relay.start()
    down.start()
    gate_up.start()
    total = small_ref[lax.axis_index("fsdp")]
    for step, copy in enumerate(part_copies):
        copy.wait()
        total = total + part_landed[step]
    part_sum[...] = total
    down_all[me] = down_ref[...]
    gate_up_all[me] = gate_up_ref[...]
    row_copies = start_to_peers(
        "seq", lambda peer: part_sum, lambda step: row_landed.at[step - 1], row_send, row_recv
    )
    relay.forward(o_ref)
    down.forward()
    gate_up.forward()
    relay.finish(o_ref)
    for step, copy in enumerate(row_copies):
        copy.wait()
        total = total + row_landed[step]
    small_out[...] = total
    down.finish()
    gate_up.finish()


def scatter_last(partial, small, down, gate_up, n, shards, call_id):
    total, width = partial.shape
    rows = total // n
    piece = small.shape[1:]
    return pl.pallas_call(
        scatter_last_kernel,
        out_shape=(
            jax.ShapeDtypeStruct((rows, width), F32),
            jax.ShapeDtypeStruct(piece, F32),
            jax.ShapeDtypeStruct((n,) + down.shape, BF16),
            jax.ShapeDtypeStruct((n,) + gate_up.shape, BF16),
        ),
        in_specs=[VMEM_SPEC] * 4,
        out_specs=(VMEM_SPEC,) * 4,
        scratch_shapes=[
            pltpu.VMEM((shards - 1,) + piece, F32),
            pltpu.VMEM(piece, F32),
            pltpu.VMEM((n - 1,) + piece, F32),
        ]
        + semaphores(shards - 1, shards - 1, n - 1, n - 1)
        + RelayScatter.scratch(n, rows, width)
        + RelayGather.semaphores(n) * 2,
        compiler_params=communicating(call_id),
        name="scatter_last",
    )(partial, small, down, gate_up)


def finish_kernel(
    qkv_ref, out_ref, q_final, k_final, v_final, out_final,
    qkv_landed, out_landed, out_mine, out_back,
    first_send, first_recv, second_send, second_recv, *sems,
):
    greet("seq")
    n = lax.axis_size("seq")
    me = lax.axis_index("seq")
    piece = out_mine.shape[0]
    split = q_final.shape[1] // n
    narrow = k_final.shape[1] // n
    first = start_to_peers(
        "seq",
        lambda peer: out_ref.at[block_of(peer, piece)],
        lambda step: out_landed.at[step - 1],
        first_send,
        first_recv,
    )
    relay = gather_by_columns(qkv_ref, qkv_landed, sems)
    relay.start()

    def place(values, owner):
        values = values.astype(F32)
        q_final[:, block_of(owner, split)] = values[:, :split]
        k_final[:, block_of(owner, narrow)] = values[:, split : split + narrow]
        v_final[:, block_of(owner, narrow)] = values[:, split + narrow :]

    total = out_ref[block_of(me, piece), :].astype(F32)
    for step, copy in enumerate(first):
        copy.wait()
        total = total + out_landed[step].astype(F32)
    out_mine[...] = total.astype(BF16)
    out_final[block_of(me, piece), :] = out_mine[...].astype(F32)
    place(qkv_ref[...], me)
    relay.forward()
    second = start_to_peers(
        "seq", lambda peer: out_mine, lambda step: out_back.at[step - 1], second_send, second_recv
    )
    relay.finish()
    for step in range(n - 1):
        owner = lax.rem(me + n - 1 - step, n)
        place(qkv_landed[owner], owner)
    for step, copy in enumerate(second):
        copy.wait()
        owner = lax.rem(me + n - 1 - step, n)
        out_final[block_of(owner, piece), :] = out_back[step].astype(F32)


def finish(qkv, out, widths, n, call_id):
    rows, width = out.shape
    return pl.pallas_call(
        finish_kernel,
        out_shape=tuple(jax.ShapeDtypeStruct((qkv.shape[0], size), F32) for size in widths)
        + (jax.ShapeDtypeStruct(out.shape, F32),),
        in_specs=[VMEM_SPEC] * 2,
        out_specs=(VMEM_SPEC,) * 4,
        scratch_shapes=[
            pltpu.VMEM((n,) + qkv.shape, BF16),
            pltpu.VMEM((n - 1, rows // n, width), BF16),
            pltpu.VMEM((rows // n, width), BF16),
            pltpu.VMEM((n - 1, rows // n, width), BF16),
        ]
        + semaphores(*([n - 1] * 4))
        + RelayGather.semaphores(n),
        compiler_params=communicating(call_id),
        name="finish",
    )(qkv, out)


def spread_kernel(hidden_piece, pieces_ref, gate_ref, up_ref):
    n, _, width = pieces_ref.shape
    units = width // 2
    span = n * hidden_piece
    for target, base in ((gate_ref, 0), (up_ref, units)):
        for shard in range(units // hidden_piece):
            at = base + shard * hidden_piece
            target[:, shard * span : (shard + 1) * span] = jnp.concatenate(
                [pieces_ref[s, :, at : at + hidden_piece].astype(F32) for s in range(n)], axis=1
            )


def spread_back(pieces, hidden_piece):
    n, rows, width = pieces.shape
    shape = jax.ShapeDtypeStruct((rows, n * width // 2), F32)
    return pl.pallas_call(
        functools.partial(spread_kernel, hidden_piece),
        out_shape=(shape, shape),
        in_specs=[VMEM_SPEC],
        out_specs=(VMEM_SPEC, VMEM_SPEC),
        name="spread_back",
    )(pieces)


def rope(values, cosine, sine):
    return values * cosine + pltpu.roll(values, HEAD_SIZE // 2, 1) * sine


def rope_back(grad, cosine, sine):
    return grad * cosine - pltpu.roll(grad, HEAD_SIZE // 2, 1) * sine


def head_columns(index):
    return pl.ds(pl.multiple_of(index * HEAD_SIZE, HEAD_SIZE), HEAD_SIZE)


def turned_block(shift):
    def block(i):
        return lax.rem(lax.axis_index("seq") + shift + i, lax.axis_size("seq"))

    return block


def forward_kernel(
    q_pre, k_pre, v_ref, gain_q, gain_k, cos_q, sin_q, cos_k, sin_k, place_k, place_q, start_q, cot,
    out_ref, p_ref, q_ref, k_ref, cot_all,
    v_turned, outs, cot_local, send, recv, local, *cot_sems,
):
    i, head = pl.program_id(0), pl.program_id(1)
    n, heads = pl.num_programs(0), pl.num_programs(1)
    seq = lax.axis_size("seq")
    me = lax.axis_index("seq")
    kv = outs.shape[1] // GROUP
    rows = cot.shape[0]
    mine = block_of(me, rows)

    cot_relay = gather_by_rows(cot, cot_all, cot_sems)
    cot_own = pltpu.make_async_copy(cot, cot_all.at[mine], cot_local)

    def out_copy(step, which):
        return pltpu.make_async_remote_copy(
            src_ref=outs.at[step, which],
            dst_ref=out_ref.at[:, head_columns(me * heads + which)],
            send_sem=send.at[step, which],
            recv_sem=recv.at[step, which],
            device_id={"seq": lax.rem(me + 1 + step, seq)},
            device_id_type=MESH,
        )

    def own_copy(which):
        return pltpu.make_async_copy(
            outs.at[seq - 1, which], out_ref.at[:, head_columns(me * heads + which)], local.at[which]
        )

    @pl.when((i == 0) & (head == 0))
    def _():
        greet("seq")
        cot_relay.start()
        cot_own.start()
        for which in range(kv):
            own = pl.ds(which * HEAD_SIZE, HEAD_SIZE)
            pre = k_pre[:, own]
            k_ref[:, own] = rope(
                pre * inverse_rms(pre) * gain_k[...], cos_k[...], sin_k[...]
            ).astype(BF16)
            v_turned[which] = v_ref[:, own].astype(F32).T.astype(BF16)

    @pl.when((i == n // 2) & (head == 0))
    def _():
        cot_relay.forward()

    @pl.when((head > 0) & (i < n - 1))
    def _():
        out_copy(i, head - 1).start()

    @pl.when((head == 0) & (i > 0))
    def _():
        out_copy(i - 1, heads - 1).start()

    pre = q_pre[...]
    query = rope(pre * inverse_rms(pre) * gain_q[...], cos_q[...], sin_q[...]).astype(BF16)
    q_ref[...] = query
    pair = head // GROUP
    scores = back_matmul(k_ref[:, head_columns(pair)], query) * SCALE
    keys = place_k[...]
    allowed = (keys <= place_q[...]) & (keys >= start_q[...])
    scores = jnp.where(allowed, scores, MASKED)
    top = jnp.max(scores, axis=0, keepdims=True)
    weights = jnp.exp(scores - top)
    total = jnp.sum(weights, axis=0, keepdims=True)
    weights = (weights * (1.0 / total)).astype(BF16)
    p_ref[0] = weights
    outs[i, head] = matrix_product(v_turned[pair], weights).T.astype(BF16)

    @pl.when((i == n - 1) & (head == heads - 1))
    def _():
        for which in range(outs.shape[1]):
            own_copy(which).start()
        cot_relay.finish()
        cot_own.wait()
        for step in range(seq - 1):
            for which in range(outs.shape[1]):
                out_copy(step, which).wait()
        for which in range(outs.shape[1]):
            own_copy(which).wait()


def attend_forward(
    q_pre, k_pre, value, gain_q, gain_k, cosine, sine, place, start, cotangent, n, call_id
):
    rows = q_pre.shape[0]
    heads = q_pre.shape[1] // HEAD_SIZE
    kv = heads // GROUP
    block = rows // n
    width = cotangent.shape[1]
    turn = turned_block(1)
    q_spec = pl.BlockSpec((block, HEAD_SIZE), lambda i, h: (turn(i), h))
    k_spec = pl.BlockSpec((rows, kv * HEAD_SIZE), lambda i, h: (0, 0))
    gain_spec = pl.BlockSpec((1, HEAD_SIZE), lambda i, h: (0, 0))
    trig_q = pl.BlockSpec((block, HEAD_SIZE), lambda i, h: (turn(i), 0))
    trig_k = pl.BlockSpec((rows, HEAD_SIZE), lambda i, h: (0, 0))
    column = pl.BlockSpec((rows, 1), lambda i, h: (0, 0))
    row = pl.BlockSpec((1, block), lambda i, h: (0, turn(i)))
    return pl.pallas_call(
        forward_kernel,
        grid=(n, heads),
        out_shape=(
            jax.ShapeDtypeStruct((block, n * heads * HEAD_SIZE), BF16),
            jax.ShapeDtypeStruct((heads, rows, rows), BF16),
            jax.ShapeDtypeStruct((rows, heads * HEAD_SIZE), BF16),
            jax.ShapeDtypeStruct((rows, kv * HEAD_SIZE), BF16),
            jax.ShapeDtypeStruct((rows, width), BF16),
        ),
        in_specs=[
            q_spec, k_spec, k_spec, gain_spec, gain_spec, trig_q, trig_q, trig_k, trig_k,
            column, row, row, ANY_SPEC,
        ],
        out_specs=(
            ANY_SPEC,
            pl.BlockSpec((1, rows, block), lambda i, h: (h, 0, turn(i))),
            q_spec,
            k_spec,
            ANY_SPEC,
        ),
        scratch_shapes=[
            pltpu.VMEM((kv, HEAD_SIZE, rows), BF16),
            pltpu.VMEM((n, heads, block, HEAD_SIZE), BF16),
            pltpu.SemaphoreType.DMA,
            pltpu.SemaphoreType.DMA((n - 1, heads)),
            pltpu.SemaphoreType.DMA((n - 1, heads)),
            pltpu.SemaphoreType.DMA((heads,)),
        ]
        + RelayGather.semaphores(n),
        compiler_params=communicating(call_id),
        name="attend_forward",
    )(
        q_pre, k_pre, value, gain_q, gain_k, cosine, sine, cosine, sine,
        place[:, None], place[None, :], start[None, :], cotangent,
    )


def backward_kernel(
    p_ref, q_ref, k_ref, v_ref, q_pre, k_pre, gain_q, gain_k, cos_q, sin_q, cos_k, sin_k,
    grad_own, bulk,
    dq_ref, dk_ref, dv_ref, dgain_q, dgain_k, bulk_sum,
    k_turned, dk_sum, dv_sum, grads, send, recv, local, *scratch,
):
    i, head = pl.program_id(0), pl.program_id(1)
    n, heads = pl.num_programs(0), pl.num_programs(1)
    seq = lax.axis_size("seq")
    me = lax.axis_index("seq")
    kv = k_turned.shape[0]
    span = grads.shape[2]
    first = (i == 0) & (head == 0)
    last = (i == n - 1) & (head == heads - 1)

    def grad_copy(step):
        peer = lax.rem(me + step, seq)
        return pltpu.make_async_remote_copy(
            src_ref=grad_own.at[:, block_of(peer, span)],
            dst_ref=grads.at[step],
            send_sem=send.at[step - 1],
            recv_sem=recv.at[step - 1],
            device_id={"seq": peer},
            device_id_type=MESH,
        )

    bulk_relay = RelayScatter(bulk, scratch[:6], scratch[6:])
    own_copy = pltpu.make_async_copy(grad_own.at[:, block_of(me, span)], grads.at[0], local)

    @pl.when(first)
    def _():
        greet("seq")
        own_copy.start()
        for step in range(1, seq):
            grad_copy(step).start()
        bulk_relay.start()
        dgain_q[...] = jnp.zeros_like(dgain_q)
        dgain_k[...] = jnp.zeros_like(dgain_k)
        dk_sum[...] = jnp.zeros_like(dk_sum)
        dv_sum[...] = jnp.zeros_like(dv_sum)
        for which in range(kv):
            own = pl.ds(which * HEAD_SIZE, HEAD_SIZE)
            k_turned[which] = k_ref[:, own].astype(F32).T.astype(BF16)
        own_copy.wait()

    for step in range(1, seq):
        @pl.when((head == 0) & (i == seq - step))
        def _():
            grad_copy(step).wait_recv()

    @pl.when((i == n - 1) & (head == 0))
    def _():
        bulk_relay.forward(bulk_sum)

    slot = lax.rem(seq - i, seq)
    pair = head // GROUP
    rounded = p_ref[0]
    weights = rounded.astype(F32)
    grad = grads[slot, :, head_columns(head)]
    grad_weights = back_matmul(v_ref[:, head_columns(pair)], grad)
    delta = jnp.sum(weights * grad_weights, axis=0, keepdims=True)
    grad_scores = (weights * (grad_weights - delta)).astype(BF16)
    dk_sum[pair] += matrix_product(grad_scores, q_ref[...])
    dv_sum[pair] += matrix_product(rounded, grad)
    dq = (matrix_product(k_turned[pair], grad_scores).T * SCALE).astype(BF16).astype(F32)
    dq, gain_rows = rms_backward(q_pre[...], gain_q[...], rope_back(dq, cos_q[...], sin_q[...]))
    dq_ref[...] = dq.astype(BF16)
    dgain_q[...] += jnp.sum(gain_rows, axis=0, keepdims=True)

    @pl.when(last)
    def _():
        for which in range(kv):
            own = pl.ds(which * HEAD_SIZE, HEAD_SIZE)
            dk = (dk_sum[which] * SCALE).astype(BF16).astype(F32)
            dk, gain_rows = rms_backward(
                k_pre[:, own], gain_k[...], rope_back(dk, cos_k[...], sin_k[...])
            )
            dk_ref[:, own] = dk.astype(BF16)
            dgain_k[...] += jnp.sum(gain_rows, axis=0, keepdims=True)
            dv_ref[:, own] = dv_sum[which].astype(BF16)
        for step in range(1, seq):
            grad_copy(step).wait_send()
        bulk_relay.finish(bulk_sum)


def attend_backward(
    weights, query, key, value, grad_own, bulk, q_pre, k_pre, gain_q, gain_k, cosine, sine, n, call_id
):
    rows = q_pre.shape[0]
    heads = q_pre.shape[1] // HEAD_SIZE
    kv = heads // GROUP
    block = rows // n
    turn = turned_block(0)
    q_spec = pl.BlockSpec((block, HEAD_SIZE), lambda i, h: (turn(i), h))
    k_spec = pl.BlockSpec((rows, kv * HEAD_SIZE), lambda i, h: (0, 0))
    gain_spec = pl.BlockSpec((1, HEAD_SIZE), lambda i, h: (0, 0))
    trig_q = pl.BlockSpec((block, HEAD_SIZE), lambda i, h: (turn(i), 0))
    trig_k = pl.BlockSpec((rows, HEAD_SIZE), lambda i, h: (0, 0))
    return pl.pallas_call(
        backward_kernel,
        grid=(n, heads),
        out_shape=(
            jax.ShapeDtypeStruct((rows, heads * HEAD_SIZE), BF16),
            jax.ShapeDtypeStruct((rows, kv * HEAD_SIZE), BF16),
            jax.ShapeDtypeStruct((rows, kv * HEAD_SIZE), BF16),
            jax.ShapeDtypeStruct((1, HEAD_SIZE), F32),
            jax.ShapeDtypeStruct((1, HEAD_SIZE), F32),
            jax.ShapeDtypeStruct((block, bulk.shape[1]), F32),
        ),
        in_specs=[
            pl.BlockSpec((1, rows, block), lambda i, h: (h, 0, turn(i))),
            q_spec, k_spec, k_spec, q_spec, k_spec, gain_spec, gain_spec,
            trig_q, trig_q, trig_k, trig_k, ANY_SPEC,
            pl.BlockSpec(bulk.shape, lambda i, h: (0, 0)),
        ],
        out_specs=(
            q_spec, k_spec, k_spec, gain_spec, gain_spec,
            pl.BlockSpec((block, bulk.shape[1]), lambda i, h: (0, 0)),
        ),
        scratch_shapes=[
            pltpu.VMEM((kv, HEAD_SIZE, rows), BF16),
            pltpu.VMEM((kv, rows, HEAD_SIZE), F32),
            pltpu.VMEM((kv, rows, HEAD_SIZE), F32),
            pltpu.VMEM((n, block, heads * HEAD_SIZE), BF16),
            pltpu.SemaphoreType.DMA((n - 1,)),
            pltpu.SemaphoreType.DMA((n - 1,)),
            pltpu.SemaphoreType.DMA,
        ]
        + RelayScatter.scratch(n, block, bulk.shape[1]),
        compiler_params=communicating(call_id),
        name="attend_backward",
    )(
        weights, query, key, value, q_pre, k_pre, gain_q, gain_k, cosine, sine, cosine, sine,
        grad_own, bulk,
    )


def on_device(
    tokens, lengths, packing, norm_in, w_query, key_projection, value_projection, norm_query,
    norm_key, w_out, norm_post, w_gate, w_up, w_down, cotangent,
):
    n = lax.axis_size("seq")
    shards = lax.axis_size("fsdp")
    me = lax.axis_index("seq")
    resident = tokens.shape[1]
    width = tokens.shape[2]
    rows = resident * n
    heads = HQ // n
    kv = KEY_VALUE_HEADS // n
    hidden_piece = w_down.shape[0] // n

    def columns(weight, pieces):
        size = weight.shape[1] // pieces
        return lax.dynamic_slice_in_dim(weight, me * size, size, axis=1)

    def spread_columns(weight):
        pieces = weight.reshape(weight.shape[0], shards, n, hidden_piece)
        return lax.dynamic_index_in_dim(pieces, me, axis=2, keepdims=False).reshape(
            weight.shape[0], shards * hidden_piece
        )

    def tile_of(values):
        pad = 1024 - values.shape[-1]
        values = jnp.concatenate([values, jnp.zeros(values.shape[:-1] + (pad,), F32)], axis=-1)
        return values.reshape(values.shape[:-1] + (8, 128))

    part, small = norm_in.shape[0], norm_query.shape[0]
    whole, gains = gather_first(
        tokens[0],
        tile_of(jnp.concatenate([norm_in, norm_post, norm_query, norm_key]).astype(F32)),
        n, shards, 0,
    )
    gains = gains.reshape(shards, -1)
    gain_in = gains[:, :part].reshape(1, -1)
    gain_post = gains[:, part : 2 * part].reshape(1, -1)
    gain_query = gains[:, 2 * part : 2 * part + small].reshape(1, -1)
    gain_key = gains[:, 2 * part + small : 2 * part + 2 * small].reshape(1, -1)

    qkv_weight = lax.all_gather(
        jnp.concatenate(
            [columns(w_query, n), columns(key_projection, n), columns(value_projection, n)], axis=1
        ),
        "fsdp", axis=0, tiled=True,
    )
    out_weight = lax.all_gather(w_out, "fsdp", axis=0, tiled=True)
    gate_up_weight = lax.all_gather(
        jnp.concatenate([spread_columns(w_gate), spread_columns(w_up)], axis=1), "fsdp", axis=0, tiled=True
    )
    down_weight = lax.all_gather(
        lax.dynamic_slice_in_dim(w_down, me * hidden_piece, hidden_piece, axis=0),
        "fsdp", axis=0, tiled=True,
    )

    order = packing[0]
    places = jnp.arange(rows, dtype=jnp.int32)
    place = jnp.sum(jnp.where(order[None, :] == places[:, None], places[None, :], 0), axis=1)
    ends = jnp.cumsum(lengths[0])
    start = jnp.sum(jnp.where(place[:, None] >= ends[None, :], lengths[0][None, :], 0), axis=1)
    half = HEAD_SIZE // 2
    inv_freq = ROPE_BASE ** (-jnp.arange(half, dtype=F32) / half)
    angles = (place - start).astype(F32)[:, None] * inv_freq[None, :]
    cosine, sine = jnp.cos(angles), jnp.sin(angles)
    cosine = jnp.concatenate([cosine, cosine], axis=1)
    sine = jnp.concatenate([-sine, sine], axis=1)

    inputs = tokens[0].astype(F32)
    whole_f32 = whole.astype(F32)
    unit = whole_f32 * inverse_rms(whole_f32)
    normalized = (unit * gain_in).astype(BF16)
    qkv = matrix_product(normalized, qkv_weight)
    split = heads * HEAD_SIZE
    q_pre = qkv[:, :split]
    k_pre = qkv[:, split : split + kv * HEAD_SIZE]
    value = qkv[:, split + kv * HEAD_SIZE :].astype(BF16)
    attended, weights, query, key, grad_mlp = attend_forward(
        q_pre, k_pre, value, gain_query, gain_key, cosine, sine, place, start, cotangent[0], n, 1
    )
    middle = inputs + matrix_product(attended, out_weight)
    normed_post_mine = (middle * inverse_rms(middle) * gain_post).astype(BF16)
    normed_post = gather_rows(normed_post_mine, n, 2)

    gate_up = matrix_product(normed_post, gate_up_weight)
    units = shards * hidden_piece
    gate, up = gate_up[:, :units], gate_up[:, units:]
    logistic = 1.0 / (1.0 + jnp.exp(-gate))
    hidden = (gate / (1.0 + jnp.exp(-gate)) * up).astype(BF16)
    mlp_partial = matrix_product(hidden, down_weight).astype(BF16)

    grad_hidden = back_matmul(grad_mlp, down_weight)
    grad_down = outer_sum(hidden, grad_mlp).astype(BF16)
    grad_gate = (grad_hidden * up * (logistic + gate * logistic * (1.0 - logistic))).astype(BF16)
    grad_up = (grad_hidden * gate * logistic).astype(BF16)
    grad_gate_up = jnp.concatenate([grad_gate, grad_up], axis=1)
    grad_gate_up_weight = outer_sum(normed_post, grad_gate_up).astype(BF16)
    grad_partial, grad_down, grad_gate_up_weight = lax.optimization_barrier(
        (back_matmul(grad_gate_up, gate_up_weight).astype(BF16), grad_down, grad_gate_up_weight)
    )
    down_share = lax.psum_scatter(grad_down, "fsdp", scatter_dimension=0, tiled=True)
    gate_up_share = lax.psum_scatter(grad_gate_up_weight, "fsdp", scatter_dimension=0, tiled=True)
    grad_normed_post = scatter_sum(grad_partial, n, 3)
    grad_middle, gain_rows = rms_backward(middle, gain_post, grad_normed_post)
    grad_middle = cotangent[0].astype(F32) + grad_middle
    grad_gain_post = jnp.sum(gain_rows, axis=0)
    grad_branch = grad_middle.astype(BF16)
    grad_out = outer_sum(attended, grad_branch).astype(BF16)
    out_share = lax.psum_scatter(grad_out, "fsdp", scatter_dimension=0, tiled=True)
    grad_attended = back_matmul(grad_branch, out_weight).astype(BF16)
    grad_q, grad_k, grad_v, grad_gain_query, grad_gain_key, mlp_sum = attend_backward(
        weights, query, key, value, grad_attended, mlp_partial, q_pre, k_pre, gain_query,
        gain_key, cosine, sine, n, 4,
    )
    output = (middle + mlp_sum).astype(BF16)[None]
    grad_qkv = jnp.concatenate([grad_q, grad_k, grad_v], axis=1)
    grad_qkv_weight = outer_sum(normalized, grad_qkv).astype(BF16)
    qkv_share = lax.psum_scatter(grad_qkv_weight, "fsdp", scatter_dimension=0, tiled=True)
    partial = back_matmul(grad_qkv, qkv_weight)
    grad_gain_in = jnp.sum(partial * unit, axis=0)
    small_grads = [grad_gain_in, grad_gain_post, grad_gain_query, grad_gain_key]
    small_grads = tile_of(jnp.concatenate([g.reshape(shards, -1) for g in small_grads], axis=1))
    grad_normed, gain_shares, down_all, gate_up_all = scatter_last(
        partial.astype(BF16), small_grads, down_share, gate_up_share, n, shards, 5
    )
    gain_shares = gain_shares.reshape(-1)
    grad_inputs, _ = rms_backward(inputs, gain_in, grad_normed)
    input_grad = (grad_middle + grad_inputs).astype(BF16)[None]

    final_down = down_all.astype(F32).reshape(-1, width)
    final_gate, final_up = spread_back(gate_up_all, hidden_piece)
    final_query, final_key, final_value, final_out = finish(
        qkv_share, out_share, (HQ * HEAD_SIZE,) + (KEY_VALUE_HEADS * HEAD_SIZE,) * 2, n, 6
    )

    return (
        output,
        input_grad,
        gain_shares[:part],
        final_query,
        final_key,
        final_value,
        gain_shares[2 * part : 2 * part + small],
        gain_shares[2 * part + small : 2 * part + 2 * small],
        final_out,
        gain_shares[part : 2 * part],
        final_gate,
        final_up,
        final_down,
    )


def solution(mesh):
    flat, wide = P("fsdp"), P("fsdp", None)
    whole = P("fsdp", "seq", None)
    in_specs = (
        whole, wide, wide, flat, wide, wide, wide, flat, flat, wide, flat, wide, wide, wide, whole,
    )
    out_specs = (whole, whole, flat, wide, wide, wide, flat, flat, wide, flat, wide, wide, wide)

    return jax.shard_map(
        on_device, mesh=mesh, in_specs=in_specs, out_specs=out_specs, check_vma=False
    )
```

```python
import functools

import jax
import jax.numpy as jnp
from jax import lax
from jax.experimental import pallas as pl
from jax.experimental.pallas import tpu as pltpu
from jax.sharding import PartitionSpec as P


HQ = 16
KEY_VALUE_HEADS = 8
HEAD_SIZE = 128
GROUP = HQ // KEY_VALUE_HEADS

ROPE_BASE = 1000000.0
EPSILON = 1e-06
MASKED = -1e30
SCALE = HEAD_SIZE ** (-0.5)
MESH = pl.DeviceIdType.MESH
BF16 = jnp.bfloat16
F32 = jnp.float32


def matrix_product(left, right):
    return jnp.dot(left, right, preferred_element_type=F32)


def outer_sum(left, right):
    return lax.dot_general(left, right, (((0,), (0,)), ((), ())), preferred_element_type=F32)


def back_matmul(left, right):
    return lax.dot_general(left, right, (((1,), (1,)), ((), ())), preferred_element_type=F32)


def inverse_rms(values):
    return lax.rsqrt(jnp.mean(values * values, axis=-1, keepdims=True) + EPSILON)


def rms_backward(values, gain, grad):
    c = inverse_rms(values)
    scaled = grad * gain
    inner = jnp.mean(values * scaled, axis=-1, keepdims=True)
    return c * scaled - values * (c * c * c) * inner, grad * values * c


def greet(*axes):
    barrier = pltpu.get_barrier_semaphore()
    count = 0
    for axis in axes:
        n = lax.axis_size(axis)
        me = lax.axis_index(axis)
        for step in range(1, n):
            pl.semaphore_signal(
                barrier, inc=1, device_id={axis: lax.rem(me + step, n)}, device_id_type=MESH
            )
        count += n - 1
    pl.semaphore_wait(barrier, count)


def block_of(index, size):
    return pl.ds(pl.multiple_of(index * size, size), size)


def start_to_peers(axis, source, target, send_sem, recv_sem):
    n = lax.axis_size(axis)
    me = lax.axis_index(axis)
    copies = []
    for step in range(1, n):
        peer = lax.rem(me + step, n)
        copy = pltpu.make_async_remote_copy(
            src_ref=source(peer),
            dst_ref=target(step),
            send_sem=send_sem.at[step - 1],
            recv_sem=recv_sem.at[step - 1],
            device_id={axis: peer},
            device_id_type=MESH,
        )
        copy.start()
        copies.append(copy)
    return copies


def semaphores(*counts):
    return [pltpu.SemaphoreType.DMA((count,)) for count in counts]


VMEM_SPEC = pl.BlockSpec(memory_space=pltpu.VMEM)
ANY_SPEC = pl.BlockSpec(memory_space=pl.ANY)


def communicating(call_id, **more):
    return pltpu.CompilerParams(collective_id=call_id, has_side_effects=True, **more)


def remote(source, target, send_sem, recv_sem, peer):
    return pltpu.make_async_remote_copy(
        src_ref=source,
        dst_ref=target,
        send_sem=send_sem,
        recv_sem=recv_sem,
        device_id={"seq": peer},
        device_id_type=MESH,
    )


class Plane:
    def __init__(self):
        self.n = lax.axis_size("seq")
        self.ny = self.n // 2
        self.me = lax.axis_index("seq")
        self.x = lax.rem(self.me, 2)
        self.y = self.me // 2

    def at(self, j, across):
        row = lax.rem(self.y + j + self.ny, self.ny)
        return row * 2 + ((1 - self.x) if across else self.x)


class RelayGather(Plane):
    def __init__(self, source, target, sems):
        super().__init__()
        self.source, self.target = source, target
        self.sx, self.rx, self.sy, self.ry, self.sy2, self.ry2, self.sx2, self.rx2 = sems

    @staticmethod
    def semaphores(n):
        ny = n // 2
        dma = pltpu.SemaphoreType.DMA
        return [dma((2,))] * 2 + [dma((ny - 1, 2))] * 2 + [dma((ny - 1,))] * 4

    def x1(self, half):
        return remote(
            self.source(half), self.target(self.me, half), self.sx.at[half], self.rx.at[half],
            self.at(0, True),
        )

    def y1(self, j, half):
        return remote(
            self.source(half), self.target(self.me, half), self.sy.at[j - 1, half],
            self.ry.at[j - 1, half], self.at(j, False),
        )

    def y2(self, j):
        block = self.target(self.at(0, True), 0)
        return remote(block, block, self.sy2.at[j - 1], self.ry2.at[j - 1], self.at(j, False))

    def x2(self, j):
        block = self.target(self.at(-j, False), 1)
        return remote(block, block, self.sx2.at[j - 1], self.rx2.at[j - 1], self.at(0, True))

    def start(self):
        others = range(1, self.ny)
        self.x1(0).start()
        for j in others:
            self.y1(j, 1).start()
        self.x1(1).start()
        for j in others:
            self.y1(j, 0).start()

    def forward(self):
        others = range(1, self.ny)
        self.x1(0).wait_recv()
        for j in others:
            self.y2(j).start()
        for j in others:
            self.y1(j, 1).wait_recv()
            self.x2(j).start()

    def finish(self):
        self.x1(0).wait_send()
        self.x1(1).wait()
        for j in range(1, self.ny):
            self.y1(j, 1).wait_send()
            self.y1(j, 0).wait()
            self.y2(j).wait()
            self.x2(j).wait()


def row_halves(ref, rows, owner, half):
    size = rows // 2
    return ref.at[pl.ds(pl.multiple_of(owner * rows + half * size, size), size)]


def column_halves(ref, half):
    size = ref.shape[-1] // 2
    return ref.at[:, half * size : (half + 1) * size]


def gather_by_rows(x_ref, o_ref, sems):
    rows = x_ref.shape[0]
    return RelayGather(
        lambda half: row_halves(x_ref, rows, 0, half),
        lambda owner, half: row_halves(o_ref, rows, owner, half),
        sems,
    )


def gather_by_columns(x_ref, o_ref, sems):
    return RelayGather(
        lambda half: column_halves(x_ref, half),
        lambda owner, half: column_halves(o_ref.at[owner], half),
        sems,
    )


class RelayScatter(Plane):
    def __init__(self, partial, buffers, sems):
        super().__init__()
        self.partial = partial
        self.rows = partial.shape[0] // self.n
        self.from_x, self.from_y, self.sent_y, self.late_y, self.sent_x, self.late_x = buffers
        self.sx, self.rx, self.sy, self.ry, self.sy2, self.ry2, self.sx2, self.rx2 = sems

    @staticmethod
    def scratch(n, rows, width):
        ny, half = n // 2, rows // 2
        dma = pltpu.SemaphoreType.DMA
        return [
            pltpu.VMEM((ny, half, width), BF16),
            pltpu.VMEM((ny - 1, 2, half, width), BF16),
            pltpu.VMEM((ny - 1, half, width), BF16),
            pltpu.VMEM((ny - 1, half, width), BF16),
            pltpu.VMEM((half, width), BF16),
            pltpu.VMEM((half, width), BF16),
        ] + [dma((ny,))] * 2 + [dma((ny - 1, 2))] * 2 + [dma((ny - 1,))] * 2 + [dma((1,))] * 2

    def piece(self, owner, half):
        return row_halves(self.partial, self.rows, owner, half)

    def x1(self, j):
        return remote(
            self.piece(self.at(j, True), 0), self.from_x.at[j], self.sx.at[j], self.rx.at[j],
            self.at(0, True),
        )

    def y1(self, j, final):
        return remote(
            self.piece(self.at(j, not final), 1), self.from_y.at[j - 1, int(final)],
            self.sy.at[j - 1, int(final)], self.ry.at[j - 1, int(final)], self.at(j, False),
        )

    def y2(self, j):
        return remote(
            self.sent_y.at[j - 1], self.late_y.at[j - 1], self.sy2.at[j - 1], self.ry2.at[j - 1],
            self.at(j, False),
        )

    def x2(self):
        return remote(self.sent_x, self.late_x, self.sx2.at[0], self.rx2.at[0], self.at(0, True))

    def start(self):
        others = range(1, self.ny)
        for j in others:
            self.x1(j).start()
            self.y1(j, False).start()
        self.x1(0).start()
        for j in others:
            self.y1(j, True).start()

    def forward(self, o_ref):
        others = range(1, self.ny)
        half = self.rows // 2
        for j in others:
            self.x1(j).wait_recv()
            own = self.piece(self.at(j, False), 0)[...].astype(F32)
            self.sent_y[j - 1] = (own + self.from_x[j].astype(F32)).astype(BF16)
        total = self.piece(self.at(0, True), 1)[...].astype(F32)
        for j in others:
            self.y1(j, False).wait_recv()
            total = total + self.from_y[j - 1, 0].astype(F32)
        self.sent_x[...] = total.astype(BF16)
        for j in others:
            self.y2(j).start()
        o_ref[:half, :] = self.piece(self.me, 0)[...].astype(F32)
        self.x2().start()
        o_ref[half:, :] = self.piece(self.me, 1)[...].astype(F32)

    def finish(self, o_ref):
        others = range(1, self.ny)
        half = self.rows // 2
        self.x1(0).wait()
        first = o_ref[:half, :] + self.from_x[0].astype(F32)
        second = o_ref[half:, :]
        for j in others:
            self.x1(j).wait_send()
            self.y1(j, False).wait_send()
            self.y1(j, True).wait()
            second = second + self.from_y[j - 1, 1].astype(F32)
        for j in others:
            self.y2(j).wait()
            first = first + self.late_y[j - 1].astype(F32)
        o_ref[:half, :] = first
        self.x2().wait()
        o_ref[half:, :] = second + self.late_x[...].astype(F32)


def gather_kernel(x_ref, o_ref, *sems):
    greet("seq")
    relay = gather_by_rows(x_ref, o_ref, sems)
    relay.start()
    o_ref[block_of(lax.axis_index("seq"), x_ref.shape[0]), :] = x_ref[...]
    relay.forward()
    relay.finish()


def gather_rows(x, n, call_id):
    rows, width = x.shape
    return pl.pallas_call(
        gather_kernel,
        out_shape=jax.ShapeDtypeStruct((n * rows, width), x.dtype),
        in_specs=[VMEM_SPEC],
        out_specs=VMEM_SPEC,
        scratch_shapes=RelayGather.semaphores(n),
        compiler_params=communicating(call_id),
    )(x)


def gather_first_kernel(x_ref, gains_ref, o_ref, all_gains, gain_send, gain_recv, *sems):
    greet("seq", "fsdp")
    place = lax.axis_index("fsdp")
    gain_copies = start_to_peers(
        "fsdp", lambda peer: gains_ref, lambda step: all_gains.at[place], gain_send, gain_recv
    )
    relay = gather_by_rows(x_ref, o_ref, sems)
    relay.start()
    o_ref[block_of(lax.axis_index("seq"), x_ref.shape[0]), :] = x_ref[...]
    all_gains[place] = gains_ref[...]
    relay.forward()
    relay.finish()
    for copy in gain_copies:
        copy.wait()


def gather_first(x, gains, n, shards, call_id):
    rows, width = x.shape
    return pl.pallas_call(
        gather_first_kernel,
        out_shape=(
            jax.ShapeDtypeStruct((n * rows, width), x.dtype),
            jax.ShapeDtypeStruct((shards,) + gains.shape, gains.dtype),
        ),
        in_specs=[VMEM_SPEC, VMEM_SPEC],
        out_specs=(VMEM_SPEC, VMEM_SPEC),
        scratch_shapes=semaphores(shards - 1, shards - 1) + RelayGather.semaphores(n),
        compiler_params=communicating(call_id),
        name="gather_first",
    )(x, gains)


def scatter_kernel(p_ref, o_ref, *scratch):
    greet("seq")
    relay = RelayScatter(p_ref, scratch[:6], scratch[6:])
    relay.start()
    relay.forward(o_ref)
    relay.finish(o_ref)


def scatter_sum(partial, n, call_id):
    total, width = partial.shape
    rows = total // n
    return pl.pallas_call(
        scatter_kernel,
        out_shape=jax.ShapeDtypeStruct((rows, width), F32),
        in_specs=[VMEM_SPEC],
        out_specs=VMEM_SPEC,
        scratch_shapes=RelayScatter.scratch(n, rows, width),
        compiler_params=communicating(call_id),
    )(partial)


def scatter_last_kernel(
    p_ref, small_ref, down_ref, gate_up_ref, out_ref,
    o_ref, small_out, down_all, gate_up_all, out_final,
    part_landed, part_sum, row_landed, out_landed, out_mine, out_back,
    part_send, part_recv, row_send, row_recv, first_send, first_recv, second_send, second_recv,
    *scratch,
):
    greet("seq", "fsdp")
    me = lax.axis_index("seq")
    part_copies = start_to_peers(
        "fsdp",
        lambda peer: small_ref.at[peer],
        lambda step: part_landed.at[step - 1],
        part_send,
        part_recv,
    )
    relay = RelayScatter(p_ref, scratch[:6], scratch[6:14])
    down = gather_by_columns(down_ref, down_all, scratch[14:22])
    gate_up = gather_by_columns(gate_up_ref, gate_up_all, scratch[22:30])
    relay.start()
    piece = out_mine.shape[0]
    first = start_to_peers(
        "seq",
        lambda peer: out_ref.at[block_of(peer, piece)],
        lambda step: out_landed.at[step - 1],
        first_send,
        first_recv,
    )
    down.start()
    gate_up.start()
    total = small_ref[lax.axis_index("fsdp")]
    for step, copy in enumerate(part_copies):
        copy.wait()
        total = total + part_landed[step]
    part_sum[...] = total
    down_all[me] = down_ref[...]
    gate_up_all[me] = gate_up_ref[...]
    row_copies = start_to_peers(
        "seq", lambda peer: part_sum, lambda step: row_landed.at[step - 1], row_send, row_recv
    )
    relay.forward(o_ref)
    out_total = out_ref[block_of(me, piece), :].astype(F32)
    for step, copy in enumerate(first):
        copy.wait()
        out_total = out_total + out_landed[step].astype(F32)
    out_mine[...] = out_total.astype(BF16)
    down.forward()
    out_final[block_of(me, piece), :] = out_mine[...].astype(F32)
    second = start_to_peers(
        "seq", lambda peer: out_mine, lambda step: out_back.at[step - 1], second_send, second_recv
    )
    gate_up.forward()
    relay.finish(o_ref)
    for step, copy in enumerate(row_copies):
        copy.wait()
        total = total + row_landed[step]
    small_out[...] = total
    down.finish()
    n = lax.axis_size("seq")
    for step, copy in enumerate(second):
        copy.wait()
        out_final[block_of(lax.rem(me + n - 1 - step, n), piece), :] = out_back[step].astype(F32)
    gate_up.finish()


def scatter_last(partial, small, down, gate_up, out, n, shards, call_id):
    total, width = partial.shape
    rows = total // n
    piece = small.shape[1:]
    return pl.pallas_call(
        scatter_last_kernel,
        out_shape=(
            jax.ShapeDtypeStruct((rows, width), F32),
            jax.ShapeDtypeStruct(piece, F32),
            jax.ShapeDtypeStruct((n,) + down.shape, BF16),
            jax.ShapeDtypeStruct((n,) + gate_up.shape, BF16),
            jax.ShapeDtypeStruct(out.shape, F32),
        ),
        in_specs=[VMEM_SPEC] * 5,
        out_specs=(VMEM_SPEC,) * 5,
        scratch_shapes=[
            pltpu.VMEM((shards - 1,) + piece, F32),
            pltpu.VMEM(piece, F32),
            pltpu.VMEM((n - 1,) + piece, F32),
            pltpu.VMEM((n - 1, out.shape[0] // n, width), BF16),
            pltpu.VMEM((out.shape[0] // n, width), BF16),
            pltpu.VMEM((n - 1, out.shape[0] // n, width), BF16),
        ]
        + semaphores(shards - 1, shards - 1, *([n - 1] * 6))
        + RelayScatter.scratch(n, rows, width)
        + RelayGather.semaphores(n) * 2,
        compiler_params=communicating(call_id),
        name="scatter_last",
    )(partial, small, down, gate_up, out)


def finish_kernel(qkv_ref, q_final, k_final, v_final, qkv_landed, *sems):
    greet("seq")
    n = lax.axis_size("seq")
    me = lax.axis_index("seq")
    split = q_final.shape[1] // n
    narrow = k_final.shape[1] // n

    def place(values, owner):
        values = values.astype(F32)
        q_final[:, block_of(owner, split)] = values[:, :split]
        k_final[:, block_of(owner, narrow)] = values[:, split : split + narrow]
        v_final[:, block_of(owner, narrow)] = values[:, split + narrow :]

    relay = gather_by_columns(qkv_ref, qkv_landed, sems)
    relay.start()
    place(qkv_ref[...], me)
    relay.forward()
    relay.finish()
    for step in range(1, n):
        owner = lax.rem(me + step, n)
        place(qkv_landed[owner], owner)


def finish(qkv, widths, n, call_id):
    return pl.pallas_call(
        finish_kernel,
        out_shape=tuple(jax.ShapeDtypeStruct((qkv.shape[0], size), F32) for size in widths),
        in_specs=[VMEM_SPEC],
        out_specs=(VMEM_SPEC,) * 3,
        scratch_shapes=[pltpu.VMEM((n,) + qkv.shape, BF16)] + RelayGather.semaphores(n),
        compiler_params=communicating(call_id),
        name="finish",
    )(qkv)


def spread_kernel(hidden_piece, pieces_ref, gate_ref, up_ref):
    n, _, width = pieces_ref.shape
    units = width // 2
    span = n * hidden_piece
    for target, base in ((gate_ref, 0), (up_ref, units)):
        for shard in range(units // hidden_piece):
            at = base + shard * hidden_piece
            target[:, shard * span : (shard + 1) * span] = jnp.concatenate(
                [pieces_ref[s, :, at : at + hidden_piece].astype(F32) for s in range(n)], axis=1
            )


def spread_back(pieces, hidden_piece):
    n, rows, width = pieces.shape
    shape = jax.ShapeDtypeStruct((rows, n * width // 2), F32)
    return pl.pallas_call(
        functools.partial(spread_kernel, hidden_piece),
        out_shape=(shape, shape),
        in_specs=[VMEM_SPEC],
        out_specs=(VMEM_SPEC, VMEM_SPEC),
        name="spread_back",
    )(pieces)


def rope(values, cosine, sine):
    return values * cosine + pltpu.roll(values, HEAD_SIZE // 2, 1) * sine


def rope_back(grad, cosine, sine):
    return grad * cosine - pltpu.roll(grad, HEAD_SIZE // 2, 1) * sine


def head_columns(index):
    return pl.ds(pl.multiple_of(index * HEAD_SIZE, HEAD_SIZE), HEAD_SIZE)


def turned_block(shift):
    def block(i):
        return lax.rem(lax.axis_index("seq") + shift + i, lax.axis_size("seq"))

    return block


def forward_kernel(
    q_pre, k_pre, v_ref, gain_q, gain_k, cos_q, sin_q, cos_k, sin_k, place_k, place_q, start_q, cot,
    out_ref, p_ref, q_ref, k_ref, cot_all,
    v_turned, outs, cot_local, send, recv, local, *cot_sems,
):
    i, head = pl.program_id(0), pl.program_id(1)
    n, heads = pl.num_programs(0), pl.num_programs(1)
    seq = lax.axis_size("seq")
    me = lax.axis_index("seq")
    kv = outs.shape[1] // GROUP
    rows = cot.shape[0]
    mine = block_of(me, rows)

    cot_relay = gather_by_rows(cot, cot_all, cot_sems)
    cot_own = pltpu.make_async_copy(cot, cot_all.at[mine], cot_local)

    def out_copy(step, which):
        return pltpu.make_async_remote_copy(
            src_ref=outs.at[step, which],
            dst_ref=out_ref.at[:, head_columns(me * heads + which)],
            send_sem=send.at[step, which],
            recv_sem=recv.at[step, which],
            device_id={"seq": lax.rem(me + 1 + step, seq)},
            device_id_type=MESH,
        )

    def own_copy(which):
        return pltpu.make_async_copy(
            outs.at[seq - 1, which], out_ref.at[:, head_columns(me * heads + which)], local.at[which]
        )

    @pl.when((i == 0) & (head == 0))
    def _():
        greet("seq")
        cot_relay.start()
        cot_own.start()
        for which in range(kv):
            own = pl.ds(which * HEAD_SIZE, HEAD_SIZE)
            pre = k_pre[:, own]
            k_ref[:, own] = rope(
                pre * inverse_rms(pre) * gain_k[...], cos_k[...], sin_k[...]
            ).astype(BF16)
            v_turned[which] = v_ref[:, own].astype(F32).T.astype(BF16)

    @pl.when((i == n // 2) & (head == 0))
    def _():
        cot_relay.forward()

    @pl.when((head > 0) & (i < n - 1))
    def _():
        out_copy(i, head - 1).start()

    @pl.when((head == 0) & (i > 0))
    def _():
        out_copy(i - 1, heads - 1).start()

    pre = q_pre[...]
    query = rope(pre * inverse_rms(pre) * gain_q[...], cos_q[...], sin_q[...]).astype(BF16)
    q_ref[...] = query
    pair = head // GROUP
    scores = back_matmul(k_ref[:, head_columns(pair)], query) * SCALE
    keys = place_k[...]
    allowed = (keys <= place_q[...]) & (keys >= start_q[...])
    scores = jnp.where(allowed, scores, MASKED)
    top = jnp.max(scores, axis=0, keepdims=True)
    weights = jnp.exp(scores - top)
    total = jnp.sum(weights, axis=0, keepdims=True)
    weights = (weights * (1.0 / total)).astype(BF16)
    p_ref[0] = weights
    outs[i, head] = matrix_product(v_turned[pair], weights).T.astype(BF16)

    @pl.when((i == n - 1) & (head == heads - 1))
    def _():
        for which in range(outs.shape[1]):
            own_copy(which).start()
        cot_relay.finish()
        cot_own.wait()
        for step in range(seq - 1):
            for which in range(outs.shape[1]):
                out_copy(step, which).wait()
        for which in range(outs.shape[1]):
            own_copy(which).wait()


def attend_forward(
    q_pre, k_pre, value, gain_q, gain_k, cosine, sine, place, start, cotangent, n, call_id
):
    rows = q_pre.shape[0]
    heads = q_pre.shape[1] // HEAD_SIZE
    kv = heads // GROUP
    block = rows // n
    width = cotangent.shape[1]
    turn = turned_block(1)
    q_spec = pl.BlockSpec((block, HEAD_SIZE), lambda i, h: (turn(i), h))
    k_spec = pl.BlockSpec((rows, kv * HEAD_SIZE), lambda i, h: (0, 0))
    gain_spec = pl.BlockSpec((1, HEAD_SIZE), lambda i, h: (0, 0))
    trig_q = pl.BlockSpec((block, HEAD_SIZE), lambda i, h: (turn(i), 0))
    trig_k = pl.BlockSpec((rows, HEAD_SIZE), lambda i, h: (0, 0))
    column = pl.BlockSpec((rows, 1), lambda i, h: (0, 0))
    row = pl.BlockSpec((1, block), lambda i, h: (0, turn(i)))
    return pl.pallas_call(
        forward_kernel,
        grid=(n, heads),
        out_shape=(
            jax.ShapeDtypeStruct((block, n * heads * HEAD_SIZE), BF16),
            jax.ShapeDtypeStruct((heads, rows, rows), BF16),
            jax.ShapeDtypeStruct((rows, heads * HEAD_SIZE), BF16),
            jax.ShapeDtypeStruct((rows, kv * HEAD_SIZE), BF16),
            jax.ShapeDtypeStruct((rows, width), BF16),
        ),
        in_specs=[
            q_spec, k_spec, k_spec, gain_spec, gain_spec, trig_q, trig_q, trig_k, trig_k,
            column, row, row, ANY_SPEC,
        ],
        out_specs=(
            ANY_SPEC,
            pl.BlockSpec((1, rows, block), lambda i, h: (h, 0, turn(i))),
            q_spec,
            k_spec,
            ANY_SPEC,
        ),
        scratch_shapes=[
            pltpu.VMEM((kv, HEAD_SIZE, rows), BF16),
            pltpu.VMEM((n, heads, block, HEAD_SIZE), BF16),
            pltpu.SemaphoreType.DMA,
            pltpu.SemaphoreType.DMA((n - 1, heads)),
            pltpu.SemaphoreType.DMA((n - 1, heads)),
            pltpu.SemaphoreType.DMA((heads,)),
        ]
        + RelayGather.semaphores(n),
        compiler_params=communicating(call_id),
        name="attend_forward",
    )(
        q_pre, k_pre, value, gain_q, gain_k, cosine, sine, cosine, sine,
        place[:, None], place[None, :], start[None, :], cotangent,
    )


def backward_kernel(
    p_ref, q_ref, k_ref, v_ref, q_pre, k_pre, gain_q, gain_k, cos_q, sin_q, cos_k, sin_k,
    grad_own, bulk,
    dq_ref, dk_ref, dv_ref, dgain_q, dgain_k, bulk_sum,
    k_turned, dk_sum, dv_sum, grads, send, recv, local, *scratch,
):
    i, head = pl.program_id(0), pl.program_id(1)
    n, heads = pl.num_programs(0), pl.num_programs(1)
    seq = lax.axis_size("seq")
    me = lax.axis_index("seq")
    kv = k_turned.shape[0]
    span = grads.shape[2]
    first = (i == 0) & (head == 0)
    last = (i == n - 1) & (head == heads - 1)

    def grad_copy(step):
        peer = lax.rem(me + step, seq)
        return pltpu.make_async_remote_copy(
            src_ref=grad_own.at[:, block_of(peer, span)],
            dst_ref=grads.at[step],
            send_sem=send.at[step - 1],
            recv_sem=recv.at[step - 1],
            device_id={"seq": peer},
            device_id_type=MESH,
        )

    bulk_relay = RelayScatter(bulk, scratch[:6], scratch[6:])
    own_copy = pltpu.make_async_copy(grad_own.at[:, block_of(me, span)], grads.at[0], local)

    @pl.when(first)
    def _():
        greet("seq")
        own_copy.start()
        for step in range(1, seq):
            grad_copy(step).start()
        bulk_relay.start()
        dgain_q[...] = jnp.zeros_like(dgain_q)
        dgain_k[...] = jnp.zeros_like(dgain_k)
        dk_sum[...] = jnp.zeros_like(dk_sum)
        dv_sum[...] = jnp.zeros_like(dv_sum)
        for which in range(kv):
            own = pl.ds(which * HEAD_SIZE, HEAD_SIZE)
            k_turned[which] = k_ref[:, own].astype(F32).T.astype(BF16)
        own_copy.wait()

    for step in range(1, seq):
        @pl.when((head == 0) & (i == seq - step))
        def _():
            grad_copy(step).wait_recv()

    @pl.when((i == n - 1) & (head == 0))
    def _():
        bulk_relay.forward(bulk_sum)

    slot = lax.rem(seq - i, seq)
    pair = head // GROUP
    rounded = p_ref[0]
    weights = rounded.astype(F32)
    grad = grads[slot, :, head_columns(head)]
    grad_weights = back_matmul(v_ref[:, head_columns(pair)], grad)
    delta = jnp.sum(weights * grad_weights, axis=0, keepdims=True)
    grad_scores = (weights * (grad_weights - delta)).astype(BF16)
    dk_sum[pair] += matrix_product(grad_scores, q_ref[...])
    dv_sum[pair] += matrix_product(rounded, grad)
    dq = (matrix_product(k_turned[pair], grad_scores).T * SCALE).astype(BF16).astype(F32)
    dq, gain_rows = rms_backward(q_pre[...], gain_q[...], rope_back(dq, cos_q[...], sin_q[...]))
    dq_ref[...] = dq.astype(BF16)
    dgain_q[...] += jnp.sum(gain_rows, axis=0, keepdims=True)

    @pl.when(last)
    def _():
        for which in range(kv):
            own = pl.ds(which * HEAD_SIZE, HEAD_SIZE)
            dk = (dk_sum[which] * SCALE).astype(BF16).astype(F32)
            dk, gain_rows = rms_backward(
                k_pre[:, own], gain_k[...], rope_back(dk, cos_k[...], sin_k[...])
            )
            dk_ref[:, own] = dk.astype(BF16)
            dgain_k[...] += jnp.sum(gain_rows, axis=0, keepdims=True)
            dv_ref[:, own] = dv_sum[which].astype(BF16)
        for step in range(1, seq):
            grad_copy(step).wait_send()
        bulk_relay.finish(bulk_sum)


def attend_backward(
    weights, query, key, value, grad_own, bulk, q_pre, k_pre, gain_q, gain_k, cosine, sine, n, call_id
):
    rows = q_pre.shape[0]
    heads = q_pre.shape[1] // HEAD_SIZE
    kv = heads // GROUP
    block = rows // n
    turn = turned_block(0)
    q_spec = pl.BlockSpec((block, HEAD_SIZE), lambda i, h: (turn(i), h))
    k_spec = pl.BlockSpec((rows, kv * HEAD_SIZE), lambda i, h: (0, 0))
    gain_spec = pl.BlockSpec((1, HEAD_SIZE), lambda i, h: (0, 0))
    trig_q = pl.BlockSpec((block, HEAD_SIZE), lambda i, h: (turn(i), 0))
    trig_k = pl.BlockSpec((rows, HEAD_SIZE), lambda i, h: (0, 0))
    return pl.pallas_call(
        backward_kernel,
        grid=(n, heads),
        out_shape=(
            jax.ShapeDtypeStruct((rows, heads * HEAD_SIZE), BF16),
            jax.ShapeDtypeStruct((rows, kv * HEAD_SIZE), BF16),
            jax.ShapeDtypeStruct((rows, kv * HEAD_SIZE), BF16),
            jax.ShapeDtypeStruct((1, HEAD_SIZE), F32),
            jax.ShapeDtypeStruct((1, HEAD_SIZE), F32),
            jax.ShapeDtypeStruct((block, bulk.shape[1]), F32),
        ),
        in_specs=[
            pl.BlockSpec((1, rows, block), lambda i, h: (h, 0, turn(i))),
            q_spec, k_spec, k_spec, q_spec, k_spec, gain_spec, gain_spec,
            trig_q, trig_q, trig_k, trig_k, ANY_SPEC,
            pl.BlockSpec(bulk.shape, lambda i, h: (0, 0)),
        ],
        out_specs=(
            q_spec, k_spec, k_spec, gain_spec, gain_spec,
            pl.BlockSpec((block, bulk.shape[1]), lambda i, h: (0, 0)),
        ),
        scratch_shapes=[
            pltpu.VMEM((kv, HEAD_SIZE, rows), BF16),
            pltpu.VMEM((kv, rows, HEAD_SIZE), F32),
            pltpu.VMEM((kv, rows, HEAD_SIZE), F32),
            pltpu.VMEM((n, block, heads * HEAD_SIZE), BF16),
            pltpu.SemaphoreType.DMA((n - 1,)),
            pltpu.SemaphoreType.DMA((n - 1,)),
            pltpu.SemaphoreType.DMA,
        ]
        + RelayScatter.scratch(n, block, bulk.shape[1]),
        compiler_params=communicating(call_id),
        name="attend_backward",
    )(
        weights, query, key, value, q_pre, k_pre, gain_q, gain_k, cosine, sine, cosine, sine,
        grad_own, bulk,
    )


def on_device(
    tokens, lengths, packing, norm_in, w_query, key_projection, value_projection, norm_query,
    norm_key, w_out, norm_post, w_gate, w_up, w_down, cotangent,
):
    n = lax.axis_size("seq")
    shards = lax.axis_size("fsdp")
    me = lax.axis_index("seq")
    resident = tokens.shape[1]
    width = tokens.shape[2]
    rows = resident * n
    heads = HQ // n
    kv = KEY_VALUE_HEADS // n
    hidden_piece = w_down.shape[0] // n

    def columns(weight, pieces):
        size = weight.shape[1] // pieces
        return lax.dynamic_slice_in_dim(weight, me * size, size, axis=1)

    def spread_columns(weight):
        pieces = weight.reshape(weight.shape[0], shards, n, hidden_piece)
        return lax.dynamic_index_in_dim(pieces, me, axis=2, keepdims=False).reshape(
            weight.shape[0], shards * hidden_piece
        )

    def tile_of(values):
        pad = 1024 - values.shape[-1]
        values = jnp.concatenate([values, jnp.zeros(values.shape[:-1] + (pad,), F32)], axis=-1)
        return values.reshape(values.shape[:-1] + (8, 128))

    part, small = norm_in.shape[0], norm_query.shape[0]
    whole, gains = gather_first(
        tokens[0],
        tile_of(jnp.concatenate([norm_in, norm_post, norm_query, norm_key]).astype(F32)),
        n, shards, 0,
    )
    gains = gains.reshape(shards, -1)
    gain_in = gains[:, :part].reshape(1, -1)
    gain_post = gains[:, part : 2 * part].reshape(1, -1)
    gain_query = gains[:, 2 * part : 2 * part + small].reshape(1, -1)
    gain_key = gains[:, 2 * part + small : 2 * part + 2 * small].reshape(1, -1)

    def gathered(*weights):
        sizes = [weight.shape[0] for weight in weights]
        if len({weight.shape[1] for weight in weights}) > 1:
            return [lax.all_gather(weight, "fsdp", axis=0, tiled=True) for weight in weights]
        joined = lax.all_gather(jnp.concatenate(weights, axis=0), "fsdp", axis=0)
        starts = [sum(sizes[:i]) for i in range(len(sizes))]
        return [
            joined[:, start : start + size].reshape(-1, joined.shape[2])
            for start, size in zip(starts, sizes)
        ]

    qkv_weight, down_weight = gathered(
        jnp.concatenate(
            [columns(w_query, n), columns(key_projection, n), columns(value_projection, n)], axis=1
        ),
        lax.dynamic_slice_in_dim(w_down, me * hidden_piece, hidden_piece, axis=0),
    )
    out_weight = lax.all_gather(w_out, "fsdp", axis=0, tiled=True)
    gate_up_weight = lax.all_gather(
        jnp.concatenate([spread_columns(w_gate), spread_columns(w_up)], axis=1), "fsdp", axis=0, tiled=True
    )

    order = packing[0]
    places = jnp.arange(rows, dtype=jnp.int32)
    place = jnp.sum(jnp.where(order[None, :] == places[:, None], places[None, :], 0), axis=1)
    ends = jnp.cumsum(lengths[0])
    start = jnp.sum(jnp.where(place[:, None] >= ends[None, :], lengths[0][None, :], 0), axis=1)
    half = HEAD_SIZE // 2
    inv_freq = ROPE_BASE ** (-jnp.arange(half, dtype=F32) / half)
    angles = (place - start).astype(F32)[:, None] * inv_freq[None, :]
    cosine, sine = jnp.cos(angles), jnp.sin(angles)
    cosine = jnp.concatenate([cosine, cosine], axis=1)
    sine = jnp.concatenate([-sine, sine], axis=1)

    inputs = tokens[0].astype(F32)
    whole_f32 = whole.astype(F32)
    unit = whole_f32 * inverse_rms(whole_f32)
    normalized = (unit * gain_in).astype(BF16)
    qkv = matrix_product(normalized, qkv_weight)
    split = heads * HEAD_SIZE
    q_pre = qkv[:, :split]
    k_pre = qkv[:, split : split + kv * HEAD_SIZE]
    value = qkv[:, split + kv * HEAD_SIZE :].astype(BF16)
    attended, weights, query, key, grad_mlp = attend_forward(
        q_pre, k_pre, value, gain_query, gain_key, cosine, sine, place, start, cotangent[0], n, 1
    )
    middle = inputs + matrix_product(attended, out_weight)
    normed_post_mine = (middle * inverse_rms(middle) * gain_post).astype(BF16)
    normed_post = gather_rows(normed_post_mine, n, 2)

    grad_hidden = lax.optimization_barrier(back_matmul(grad_mlp, down_weight))
    gate_up = matrix_product(normed_post, gate_up_weight)
    units = shards * hidden_piece
    gate, up = gate_up[:, :units], gate_up[:, units:]
    logistic = 1.0 / (1.0 + jnp.exp(-gate))
    hidden = (gate / (1.0 + jnp.exp(-gate)) * up).astype(BF16)
    mlp_partial = matrix_product(hidden, down_weight).astype(BF16)

    grad_down = outer_sum(hidden, grad_mlp).astype(BF16)
    grad_gate = (grad_hidden * up * (logistic + gate * logistic * (1.0 - logistic))).astype(BF16)
    grad_up = (grad_hidden * gate * logistic).astype(BF16)
    grad_gate_up = jnp.concatenate([grad_gate, grad_up], axis=1)
    grad_gate_up_weight = outer_sum(normed_post, grad_gate_up).astype(BF16)
    grad_partial, grad_down, grad_gate_up_weight = lax.optimization_barrier(
        (back_matmul(grad_gate_up, gate_up_weight).astype(BF16), grad_down, grad_gate_up_weight)
    )
    gate_up_share = lax.psum_scatter(grad_gate_up_weight, "fsdp", scatter_dimension=0, tiled=True)
    grad_normed_post = scatter_sum(grad_partial, n, 3)
    grad_middle, gain_rows = rms_backward(middle, gain_post, grad_normed_post)
    grad_middle = cotangent[0].astype(F32) + grad_middle
    grad_gain_post = jnp.sum(gain_rows, axis=0)
    grad_branch = grad_middle.astype(BF16)
    grad_out = outer_sum(attended, grad_branch).astype(BF16)
    out_down_share = lax.psum_scatter(
        jnp.concatenate(
            [grad_out.reshape(shards, -1, width), grad_down.reshape(shards, -1, width)], axis=1
        ).reshape(-1, width),
        "fsdp", scatter_dimension=0, tiled=True,
    )
    out_share, down_share = out_down_share[: w_out.shape[0]], out_down_share[w_out.shape[0] :]
    grad_attended = back_matmul(grad_branch, out_weight).astype(BF16)
    grad_q, grad_k, grad_v, grad_gain_query, grad_gain_key, mlp_sum = attend_backward(
        weights, query, key, value, grad_attended, mlp_partial, q_pre, k_pre, gain_query,
        gain_key, cosine, sine, n, 4,
    )
    output = (middle + mlp_sum).astype(BF16)[None]
    grad_qkv = jnp.concatenate([grad_q, grad_k, grad_v], axis=1)
    grad_qkv_weight = outer_sum(normalized, grad_qkv).astype(BF16)
    qkv_share = lax.psum_scatter(grad_qkv_weight, "fsdp", scatter_dimension=0, tiled=True)
    partial = back_matmul(grad_qkv, qkv_weight)
    grad_gain_in = jnp.sum(partial * unit, axis=0)
    small_grads = [grad_gain_in, grad_gain_post, grad_gain_query, grad_gain_key]
    small_grads = tile_of(jnp.concatenate([g.reshape(shards, -1) for g in small_grads], axis=1))
    grad_normed, gain_shares, down_all, gate_up_all, final_out = scatter_last(
        partial.astype(BF16), small_grads, down_share, gate_up_share, out_share, n, shards, 5
    )
    gain_shares = gain_shares.reshape(-1)
    grad_inputs, _ = rms_backward(inputs, gain_in, grad_normed)
    input_grad = (grad_middle + grad_inputs).astype(BF16)[None]

    final_down = down_all.astype(F32).reshape(-1, width)
    final_gate, final_up = spread_back(gate_up_all, hidden_piece)
    final_query, final_key, final_value = finish(
        qkv_share, (HQ * HEAD_SIZE,) + (KEY_VALUE_HEADS * HEAD_SIZE,) * 2, n, 6
    )

    return (
        output,
        input_grad,
        gain_shares[:part],
        final_query,
        final_key,
        final_value,
        gain_shares[2 * part : 2 * part + small],
        gain_shares[2 * part + small : 2 * part + 2 * small],
        final_out,
        gain_shares[part : 2 * part],
        final_gate,
        final_up,
        final_down,
    )


def solution(mesh):
    flat, wide = P("fsdp"), P("fsdp", None)
    whole = P("fsdp", "seq", None)
    in_specs = (
        whole, wide, wide, flat, wide, wide, wide, flat, flat, wide, flat, wide, wide, wide, whole,
    )
    out_specs = (whole, whole, flat, wide, wide, wide, flat, flat, wide, flat, wide, wide, wide)

    return jax.shard_map(
        on_device, mesh=mesh, in_specs=in_specs, out_specs=out_specs, check_vma=False
    )
```

```python
import functools

import jax
import jax.numpy as jnp
from jax import lax
from jax.experimental import pallas as pl
from jax.experimental.pallas import tpu as pltpu
from jax.sharding import PartitionSpec as P


HQ = 16
KEY_VALUE_HEADS = 8
HEAD_SIZE = 128
GROUP = HQ // KEY_VALUE_HEADS

ROPE_BASE = 1000000.0
EPSILON = 1e-06
MASKED = -1e30
SCALE = HEAD_SIZE ** (-0.5)
MESH = pl.DeviceIdType.MESH
BF16 = jnp.bfloat16
F32 = jnp.float32


def matrix_product(left, right):
    return jnp.dot(left, right, preferred_element_type=F32)


def outer_sum(left, right):
    return lax.dot_general(left, right, (((0,), (0,)), ((), ())), preferred_element_type=F32)


def back_matmul(left, right):
    return lax.dot_general(left, right, (((1,), (1,)), ((), ())), preferred_element_type=F32)


def inverse_rms(values):
    return lax.rsqrt(jnp.mean(values * values, axis=-1, keepdims=True) + EPSILON)


def rms_backward(values, gain, grad):
    c = inverse_rms(values)
    scaled = grad * gain
    inner = jnp.mean(values * scaled, axis=-1, keepdims=True)
    return c * scaled - values * (c * c * c) * inner, grad * values * c


def greet(*axes):
    barrier = pltpu.get_barrier_semaphore()
    count = 0
    for axis in axes:
        n = lax.axis_size(axis)
        me = lax.axis_index(axis)
        for step in range(1, n):
            pl.semaphore_signal(
                barrier, inc=1, device_id={axis: lax.rem(me + step, n)}, device_id_type=MESH
            )
        count += n - 1
    pl.semaphore_wait(barrier, count)


def block_of(index, size):
    return pl.ds(pl.multiple_of(index * size, size), size)


def start_to_peers(axis, source, target, send_sem, recv_sem):
    n = lax.axis_size(axis)
    me = lax.axis_index(axis)
    copies = []
    for step in range(1, n):
        peer = lax.rem(me + step, n)
        copy = pltpu.make_async_remote_copy(
            src_ref=source(peer),
            dst_ref=target(step),
            send_sem=send_sem.at[step - 1],
            recv_sem=recv_sem.at[step - 1],
            device_id={axis: peer},
            device_id_type=MESH,
        )
        copy.start()
        copies.append(copy)
    return copies


def semaphores(*counts):
    return [pltpu.SemaphoreType.DMA((count,)) for count in counts]


VMEM_SPEC = pl.BlockSpec(memory_space=pltpu.VMEM)
ANY_SPEC = pl.BlockSpec(memory_space=pl.ANY)


def communicating(call_id, **more):
    return pltpu.CompilerParams(collective_id=call_id, has_side_effects=True, **more)


def remote(source, target, send_sem, recv_sem, peer):
    return pltpu.make_async_remote_copy(
        src_ref=source,
        dst_ref=target,
        send_sem=send_sem,
        recv_sem=recv_sem,
        device_id={"seq": peer},
        device_id_type=MESH,
    )


class Plane:
    def __init__(self):
        self.n = lax.axis_size("seq")
        self.ny = self.n // 2
        self.me = lax.axis_index("seq")
        self.x = lax.rem(self.me, 2)
        self.y = self.me // 2

    def at(self, j, across):
        row = lax.rem(self.y + j + self.ny, self.ny)
        return row * 2 + ((1 - self.x) if across else self.x)


class RelayGather(Plane):
    def __init__(self, source, target, sems):
        super().__init__()
        self.source, self.target = source, target
        self.sx, self.rx, self.sy, self.ry, self.sy2, self.ry2, self.sx2, self.rx2 = sems

    @staticmethod
    def semaphores(n):
        ny = n // 2
        dma = pltpu.SemaphoreType.DMA
        return [dma((2,))] * 2 + [dma((ny - 1, 2))] * 2 + [dma((ny - 1,))] * 4

    def x1(self, half):
        return remote(
            self.source(half), self.target(self.me, half), self.sx.at[half], self.rx.at[half],
            self.at(0, True),
        )

    def y1(self, j, half):
        return remote(
            self.source(half), self.target(self.me, half), self.sy.at[j - 1, half],
            self.ry.at[j - 1, half], self.at(j, False),
        )

    def y2(self, j):
        block = self.target(self.at(0, True), 0)
        return remote(block, block, self.sy2.at[j - 1], self.ry2.at[j - 1], self.at(j, False))

    def x2(self, j):
        block = self.target(self.at(-j, False), 1)
        return remote(block, block, self.sx2.at[j - 1], self.rx2.at[j - 1], self.at(0, True))

    def start(self):
        others = range(1, self.ny)
        self.x1(0).start()
        for j in others:
            self.y1(j, 1).start()
        self.x1(1).start()
        for j in others:
            self.y1(j, 0).start()

    def forward(self):
        others = range(1, self.ny)
        self.x1(0).wait_recv()
        for j in others:
            self.y2(j).start()
        for j in others:
            self.y1(j, 1).wait_recv()
            self.x2(j).start()

    def finish(self):
        self.x1(0).wait_send()
        self.x1(1).wait()
        for j in range(1, self.ny):
            self.y1(j, 1).wait_send()
            self.y1(j, 0).wait()
            self.y2(j).wait()
            self.x2(j).wait()


def row_halves(ref, rows, owner, half):
    size = rows // 2
    return ref.at[pl.ds(pl.multiple_of(owner * rows + half * size, size), size)]


def column_halves(ref, half):
    size = ref.shape[-1] // 2
    return ref.at[:, half * size : (half + 1) * size]


def gather_by_rows(x_ref, o_ref, sems):
    rows = x_ref.shape[0]
    return RelayGather(
        lambda half: row_halves(x_ref, rows, 0, half),
        lambda owner, half: row_halves(o_ref, rows, owner, half),
        sems,
    )


def gather_by_columns(x_ref, o_ref, sems):
    return RelayGather(
        lambda half: column_halves(x_ref, half),
        lambda owner, half: column_halves(o_ref.at[owner], half),
        sems,
    )


class RelayScatter(Plane):
    def __init__(self, partial, buffers, sems):
        super().__init__()
        self.partial = partial
        self.rows = partial.shape[0] // self.n
        self.from_x, self.from_y, self.sent_y, self.late_y, self.sent_x, self.late_x = buffers
        self.sx, self.rx, self.sy, self.ry, self.sy2, self.ry2, self.sx2, self.rx2 = sems

    @staticmethod
    def scratch(n, rows, width):
        ny, half = n // 2, rows // 2
        dma = pltpu.SemaphoreType.DMA
        return [
            pltpu.VMEM((ny, half, width), BF16),
            pltpu.VMEM((ny - 1, 2, half, width), BF16),
            pltpu.VMEM((ny - 1, half, width), BF16),
            pltpu.VMEM((ny - 1, half, width), BF16),
            pltpu.VMEM((half, width), BF16),
            pltpu.VMEM((half, width), BF16),
        ] + [dma((ny,))] * 2 + [dma((ny - 1, 2))] * 2 + [dma((ny - 1,))] * 2 + [dma((1,))] * 2

    def piece(self, owner, half):
        return row_halves(self.partial, self.rows, owner, half)

    def x1(self, j):
        return remote(
            self.piece(self.at(j, True), 0), self.from_x.at[j], self.sx.at[j], self.rx.at[j],
            self.at(0, True),
        )

    def y1(self, j, final):
        return remote(
            self.piece(self.at(j, not final), 1), self.from_y.at[j - 1, int(final)],
            self.sy.at[j - 1, int(final)], self.ry.at[j - 1, int(final)], self.at(j, False),
        )

    def y2(self, j):
        return remote(
            self.sent_y.at[j - 1], self.late_y.at[j - 1], self.sy2.at[j - 1], self.ry2.at[j - 1],
            self.at(j, False),
        )

    def x2(self):
        return remote(self.sent_x, self.late_x, self.sx2.at[0], self.rx2.at[0], self.at(0, True))

    def start(self):
        others = range(1, self.ny)
        for j in others:
            self.x1(j).start()
            self.y1(j, False).start()
        self.x1(0).start()
        for j in others:
            self.y1(j, True).start()

    def forward(self, o_ref):
        others = range(1, self.ny)
        half = self.rows // 2
        for j in others:
            self.x1(j).wait_recv()
            own = self.piece(self.at(j, False), 0)[...].astype(F32)
            self.sent_y[j - 1] = (own + self.from_x[j].astype(F32)).astype(BF16)
        total = self.piece(self.at(0, True), 1)[...].astype(F32)
        for j in others:
            self.y1(j, False).wait_recv()
            total = total + self.from_y[j - 1, 0].astype(F32)
        self.sent_x[...] = total.astype(BF16)
        for j in others:
            self.y2(j).start()
        o_ref[:half, :] = self.piece(self.me, 0)[...].astype(F32)
        self.x2().start()
        o_ref[half:, :] = self.piece(self.me, 1)[...].astype(F32)

    def finish(self, o_ref):
        others = range(1, self.ny)
        half = self.rows // 2
        self.x1(0).wait()
        first = o_ref[:half, :] + self.from_x[0].astype(F32)
        second = o_ref[half:, :]
        for j in others:
            self.x1(j).wait_send()
            self.y1(j, False).wait_send()
            self.y1(j, True).wait()
            second = second + self.from_y[j - 1, 1].astype(F32)
        for j in others:
            self.y2(j).wait()
            first = first + self.late_y[j - 1].astype(F32)
        o_ref[:half, :] = first
        self.x2().wait()
        o_ref[half:, :] = second + self.late_x[...].astype(F32)


def gather_kernel(x_ref, o_ref, *sems):
    greet("seq")
    relay = gather_by_rows(x_ref, o_ref, sems)
    relay.start()
    o_ref[block_of(lax.axis_index("seq"), x_ref.shape[0]), :] = x_ref[...]
    relay.forward()
    relay.finish()


def gather_rows(x, n, call_id):
    rows, width = x.shape
    return pl.pallas_call(
        gather_kernel,
        out_shape=jax.ShapeDtypeStruct((n * rows, width), x.dtype),
        in_specs=[VMEM_SPEC],
        out_specs=VMEM_SPEC,
        scratch_shapes=RelayGather.semaphores(n),
        compiler_params=communicating(call_id),
    )(x)


def gather_first_kernel(x_ref, gains_ref, o_ref, all_gains, gain_send, gain_recv, *sems):
    greet("seq", "fsdp")
    place = lax.axis_index("fsdp")
    gain_copies = start_to_peers(
        "fsdp", lambda peer: gains_ref, lambda step: all_gains.at[place], gain_send, gain_recv
    )
    relay = gather_by_rows(x_ref, o_ref, sems)
    relay.start()
    o_ref[block_of(lax.axis_index("seq"), x_ref.shape[0]), :] = x_ref[...]
    all_gains[place] = gains_ref[...]
    relay.forward()
    relay.finish()
    for copy in gain_copies:
        copy.wait()


def gather_first(x, gains, n, shards, call_id):
    rows, width = x.shape
    return pl.pallas_call(
        gather_first_kernel,
        out_shape=(
            jax.ShapeDtypeStruct((n * rows, width), x.dtype),
            jax.ShapeDtypeStruct((shards,) + gains.shape, gains.dtype),
        ),
        in_specs=[VMEM_SPEC, VMEM_SPEC],
        out_specs=(VMEM_SPEC, VMEM_SPEC),
        scratch_shapes=semaphores(shards - 1, shards - 1) + RelayGather.semaphores(n),
        compiler_params=communicating(call_id),
        name="gather_first",
    )(x, gains)


def scatter_kernel(p_ref, o_ref, *scratch):
    greet("seq")
    relay = RelayScatter(p_ref, scratch[:6], scratch[6:])
    relay.start()
    relay.forward(o_ref)
    relay.finish(o_ref)


def scatter_sum(partial, n, call_id):
    total, width = partial.shape
    rows = total // n
    return pl.pallas_call(
        scatter_kernel,
        out_shape=jax.ShapeDtypeStruct((rows, width), F32),
        in_specs=[VMEM_SPEC],
        out_specs=VMEM_SPEC,
        scratch_shapes=RelayScatter.scratch(n, rows, width),
        compiler_params=communicating(call_id),
    )(partial)


def scatter_last_kernel(
    p_ref, small_ref, o_ref, small_out, part_landed, part_sum, row_landed,
    part_send, part_recv, row_send, row_recv, *scratch,
):
    greet("seq", "fsdp")
    part_copies = start_to_peers(
        "fsdp",
        lambda peer: small_ref.at[peer],
        lambda step: part_landed.at[step - 1],
        part_send,
        part_recv,
    )
    relay = RelayScatter(p_ref, scratch[:6], scratch[6:])
    relay.start()
    total = small_ref[lax.axis_index("fsdp")]
    for step, copy in enumerate(part_copies):
        copy.wait()
        total = total + part_landed[step]
    part_sum[...] = total
    relay.forward(o_ref)
    row_copies = start_to_peers(
        "seq", lambda peer: part_sum, lambda step: row_landed.at[step - 1], row_send, row_recv
    )
    relay.finish(o_ref)
    for step, copy in enumerate(row_copies):
        copy.wait()
        total = total + row_landed[step]
    small_out[...] = total


def scatter_last(partial, small, n, shards, call_id):
    total, width = partial.shape
    rows = total // n
    piece = small.shape[1:]
    return pl.pallas_call(
        scatter_last_kernel,
        out_shape=(jax.ShapeDtypeStruct((rows, width), F32), jax.ShapeDtypeStruct(piece, F32)),
        in_specs=[VMEM_SPEC] * 2,
        out_specs=(VMEM_SPEC,) * 2,
        scratch_shapes=[
            pltpu.VMEM((shards - 1,) + piece, F32),
            pltpu.VMEM(piece, F32),
            pltpu.VMEM((n - 1,) + piece, F32),
        ]
        + semaphores(shards - 1, shards - 1, n - 1, n - 1)
        + RelayScatter.scratch(n, rows, width),
        compiler_params=communicating(call_id),
        name="scatter_last",
    )(partial, small)


def share_kernel(
    down_ref, out_ref, down_all, out_final, out_landed, out_mine, out_back,
    first_send, first_recv, second_send, second_recv, *sems,
):
    greet("seq")
    n = lax.axis_size("seq")
    me = lax.axis_index("seq")
    piece = out_mine.shape[0]
    first = start_to_peers(
        "seq",
        lambda peer: out_ref.at[block_of(peer, piece)],
        lambda step: out_landed.at[step - 1],
        first_send,
        first_recv,
    )
    down = gather_by_columns(down_ref, down_all, sems)
    down.start()
    down_all[me] = down_ref[...]
    total = out_ref[block_of(me, piece), :].astype(F32)
    for step, copy in enumerate(first):
        copy.wait()
        total = total + out_landed[step].astype(F32)
    out_mine[...] = total.astype(BF16)
    down.forward()
    out_final[block_of(me, piece), :] = out_mine[...].astype(F32)
    second = start_to_peers(
        "seq", lambda peer: out_mine, lambda step: out_back.at[step - 1], second_send, second_recv
    )
    for step, copy in enumerate(second):
        copy.wait()
        out_final[block_of(lax.rem(me + n - 1 - step, n), piece), :] = out_back[step].astype(F32)
    down.finish()


def share(down, out, n, call_id):
    rows, width = out.shape
    return pl.pallas_call(
        share_kernel,
        out_shape=(
            jax.ShapeDtypeStruct((n,) + down.shape, BF16),
            jax.ShapeDtypeStruct(out.shape, F32),
        ),
        in_specs=[VMEM_SPEC] * 2,
        out_specs=(VMEM_SPEC,) * 2,
        scratch_shapes=[
            pltpu.VMEM((n - 1, rows // n, width), BF16),
            pltpu.VMEM((rows // n, width), BF16),
            pltpu.VMEM((n - 1, rows // n, width), BF16),
        ]
        + semaphores(*([n - 1] * 4))
        + RelayGather.semaphores(n),
        compiler_params=communicating(call_id),
        name="share",
    )(down, out)


def finish_kernel(qkv_ref, q_final, k_final, v_final, qkv_landed, *sems):
    greet("seq")
    n = lax.axis_size("seq")
    me = lax.axis_index("seq")
    split = q_final.shape[1] // n
    narrow = k_final.shape[1] // n

    def place(values, owner):
        values = values.astype(F32)
        q_final[:, block_of(owner, split)] = values[:, :split]
        k_final[:, block_of(owner, narrow)] = values[:, split : split + narrow]
        v_final[:, block_of(owner, narrow)] = values[:, split + narrow :]

    relay = gather_by_columns(qkv_ref, qkv_landed, sems)
    relay.start()
    place(qkv_ref[...], me)
    relay.forward()
    relay.finish()
    for step in range(1, n):
        owner = lax.rem(me + step, n)
        place(qkv_landed[owner], owner)


def finish(qkv, widths, n, call_id):
    return pl.pallas_call(
        finish_kernel,
        out_shape=tuple(jax.ShapeDtypeStruct((qkv.shape[0], size), F32) for size in widths),
        in_specs=[VMEM_SPEC],
        out_specs=(VMEM_SPEC,) * 3,
        scratch_shapes=[pltpu.VMEM((n,) + qkv.shape, BF16)] + RelayGather.semaphores(n),
        compiler_params=communicating(call_id),
        name="finish",
    )(qkv)


def spread_kernel(hidden_piece, pieces_ref, gate_ref, up_ref):
    n, _, width = pieces_ref.shape
    units = width // 2
    span = n * hidden_piece
    for target, base in ((gate_ref, 0), (up_ref, units)):
        for shard in range(units // hidden_piece):
            at = base + shard * hidden_piece
            target[:, shard * span : (shard + 1) * span] = jnp.concatenate(
                [pieces_ref[s, :, at : at + hidden_piece].astype(F32) for s in range(n)], axis=1
            )


def spread_back(pieces, hidden_piece):
    n, rows, width = pieces.shape
    shape = jax.ShapeDtypeStruct((rows, n * width // 2), F32)
    return pl.pallas_call(
        functools.partial(spread_kernel, hidden_piece),
        out_shape=(shape, shape),
        in_specs=[VMEM_SPEC],
        out_specs=(VMEM_SPEC, VMEM_SPEC),
        name="spread_back",
    )(pieces)


def rope(values, cosine, sine):
    return values * cosine + pltpu.roll(values, HEAD_SIZE // 2, 1) * sine


def rope_back(grad, cosine, sine):
    return grad * cosine - pltpu.roll(grad, HEAD_SIZE // 2, 1) * sine


def head_columns(index):
    return pl.ds(pl.multiple_of(index * HEAD_SIZE, HEAD_SIZE), HEAD_SIZE)


def turned_block(shift):
    def block(i):
        return lax.rem(lax.axis_index("seq") + shift + i, lax.axis_size("seq"))

    return block


def forward_kernel(
    q_pre, k_pre, v_ref, gain_q, gain_k, cos_q, sin_q, cos_k, sin_k, place_k, place_q, start_q, cot,
    out_ref, p_ref, q_ref, k_ref, cot_all,
    v_turned, outs, cot_local, send, recv, local, *cot_sems,
):
    i, head = pl.program_id(0), pl.program_id(1)
    n, heads = pl.num_programs(0), pl.num_programs(1)
    seq = lax.axis_size("seq")
    me = lax.axis_index("seq")
    kv = outs.shape[1] // GROUP
    rows = cot.shape[0]
    mine = block_of(me, rows)

    cot_relay = gather_by_rows(cot, cot_all, cot_sems)
    cot_own = pltpu.make_async_copy(cot, cot_all.at[mine], cot_local)

    def out_copy(step, which):
        return pltpu.make_async_remote_copy(
            src_ref=outs.at[step, which],
            dst_ref=out_ref.at[:, head_columns(me * heads + which)],
            send_sem=send.at[step, which],
            recv_sem=recv.at[step, which],
            device_id={"seq": lax.rem(me + 1 + step, seq)},
            device_id_type=MESH,
        )

    def own_copy(which):
        return pltpu.make_async_copy(
            outs.at[seq - 1, which], out_ref.at[:, head_columns(me * heads + which)], local.at[which]
        )

    @pl.when((i == 0) & (head == 0))
    def _():
        greet("seq")
        cot_relay.start()
        cot_own.start()
        for which in range(kv):
            own = pl.ds(which * HEAD_SIZE, HEAD_SIZE)
            pre = k_pre[:, own]
            k_ref[:, own] = rope(
                pre * inverse_rms(pre) * gain_k[...], cos_k[...], sin_k[...]
            ).astype(BF16)
            v_turned[which] = v_ref[:, own].astype(F32).T.astype(BF16)

    @pl.when((i == n // 2) & (head == 0))
    def _():
        cot_relay.forward()

    @pl.when((head > 0) & (i < n - 1))
    def _():
        out_copy(i, head - 1).start()

    @pl.when((head == 0) & (i > 0))
    def _():
        out_copy(i - 1, heads - 1).start()

    pre = q_pre[...]
    query = rope(pre * inverse_rms(pre) * gain_q[...], cos_q[...], sin_q[...]).astype(BF16)
    q_ref[...] = query
    pair = head // GROUP
    scores = back_matmul(k_ref[:, head_columns(pair)], query) * SCALE
    keys = place_k[...]
    allowed = (keys <= place_q[...]) & (keys >= start_q[...])
    scores = jnp.where(allowed, scores, MASKED)
    top = jnp.max(scores, axis=0, keepdims=True)
    weights = jnp.exp(scores - top)
    total = jnp.sum(weights, axis=0, keepdims=True)
    weights = (weights * (1.0 / total)).astype(BF16)
    p_ref[0] = weights
    outs[i, head] = matrix_product(v_turned[pair], weights).T.astype(BF16)

    @pl.when((i == n - 1) & (head == heads - 1))
    def _():
        for which in range(outs.shape[1]):
            own_copy(which).start()
        cot_relay.finish()
        cot_own.wait()
        for step in range(seq - 1):
            for which in range(outs.shape[1]):
                out_copy(step, which).wait()
        for which in range(outs.shape[1]):
            own_copy(which).wait()


def attend_forward(
    q_pre, k_pre, value, gain_q, gain_k, cosine, sine, place, start, cotangent, n, call_id
):
    rows = q_pre.shape[0]
    heads = q_pre.shape[1] // HEAD_SIZE
    kv = heads // GROUP
    block = rows // n
    width = cotangent.shape[1]
    turn = turned_block(1)
    q_spec = pl.BlockSpec((block, HEAD_SIZE), lambda i, h: (turn(i), h))
    k_spec = pl.BlockSpec((rows, kv * HEAD_SIZE), lambda i, h: (0, 0))
    gain_spec = pl.BlockSpec((1, HEAD_SIZE), lambda i, h: (0, 0))
    trig_q = pl.BlockSpec((block, HEAD_SIZE), lambda i, h: (turn(i), 0))
    trig_k = pl.BlockSpec((rows, HEAD_SIZE), lambda i, h: (0, 0))
    column = pl.BlockSpec((rows, 1), lambda i, h: (0, 0))
    row = pl.BlockSpec((1, block), lambda i, h: (0, turn(i)))
    return pl.pallas_call(
        forward_kernel,
        grid=(n, heads),
        out_shape=(
            jax.ShapeDtypeStruct((block, n * heads * HEAD_SIZE), BF16),
            jax.ShapeDtypeStruct((heads, rows, rows), BF16),
            jax.ShapeDtypeStruct((rows, heads * HEAD_SIZE), BF16),
            jax.ShapeDtypeStruct((rows, kv * HEAD_SIZE), BF16),
            jax.ShapeDtypeStruct((rows, width), BF16),
        ),
        in_specs=[
            q_spec, k_spec, k_spec, gain_spec, gain_spec, trig_q, trig_q, trig_k, trig_k,
            column, row, row, ANY_SPEC,
        ],
        out_specs=(
            ANY_SPEC,
            pl.BlockSpec((1, rows, block), lambda i, h: (h, 0, turn(i))),
            q_spec,
            k_spec,
            ANY_SPEC,
        ),
        scratch_shapes=[
            pltpu.VMEM((kv, HEAD_SIZE, rows), BF16),
            pltpu.VMEM((n, heads, block, HEAD_SIZE), BF16),
            pltpu.SemaphoreType.DMA,
            pltpu.SemaphoreType.DMA((n - 1, heads)),
            pltpu.SemaphoreType.DMA((n - 1, heads)),
            pltpu.SemaphoreType.DMA((heads,)),
        ]
        + RelayGather.semaphores(n),
        compiler_params=communicating(call_id),
        name="attend_forward",
    )(
        q_pre, k_pre, value, gain_q, gain_k, cosine, sine, cosine, sine,
        place[:, None], place[None, :], start[None, :], cotangent,
    )


def backward_kernel(
    p_ref, q_ref, k_ref, v_ref, q_pre, k_pre, gain_q, gain_k, cos_q, sin_q, cos_k, sin_k,
    grad_own, bulk,
    dq_ref, dk_ref, dv_ref, dgain_q, dgain_k, bulk_sum,
    k_turned, dk_sum, dv_sum, grads, send, recv, local, *scratch,
):
    i, head = pl.program_id(0), pl.program_id(1)
    n, heads = pl.num_programs(0), pl.num_programs(1)
    seq = lax.axis_size("seq")
    me = lax.axis_index("seq")
    kv = k_turned.shape[0]
    span = grads.shape[2]
    first = (i == 0) & (head == 0)
    last = (i == n - 1) & (head == heads - 1)

    def grad_copy(step):
        peer = lax.rem(me + step, seq)
        return pltpu.make_async_remote_copy(
            src_ref=grad_own.at[:, block_of(peer, span)],
            dst_ref=grads.at[step],
            send_sem=send.at[step - 1],
            recv_sem=recv.at[step - 1],
            device_id={"seq": peer},
            device_id_type=MESH,
        )

    bulk_relay = RelayScatter(bulk, scratch[:6], scratch[6:])
    own_copy = pltpu.make_async_copy(grad_own.at[:, block_of(me, span)], grads.at[0], local)

    @pl.when(first)
    def _():
        greet("seq")
        own_copy.start()
        for step in range(1, seq):
            grad_copy(step).start()
        bulk_relay.start()
        dgain_q[...] = jnp.zeros_like(dgain_q)
        dgain_k[...] = jnp.zeros_like(dgain_k)
        dk_sum[...] = jnp.zeros_like(dk_sum)
        dv_sum[...] = jnp.zeros_like(dv_sum)
        for which in range(kv):
            own = pl.ds(which * HEAD_SIZE, HEAD_SIZE)
            k_turned[which] = k_ref[:, own].astype(F32).T.astype(BF16)
        own_copy.wait()

    for step in range(1, seq):
        @pl.when((head == 0) & (i == seq - step))
        def _():
            grad_copy(step).wait_recv()

    @pl.when((i == n - 1) & (head == 0))
    def _():
        bulk_relay.forward(bulk_sum)

    slot = lax.rem(seq - i, seq)
    pair = head // GROUP
    rounded = p_ref[0]
    weights = rounded.astype(F32)
    grad = grads[slot, :, head_columns(head)]
    grad_weights = back_matmul(v_ref[:, head_columns(pair)], grad)
    delta = jnp.sum(weights * grad_weights, axis=0, keepdims=True)
    grad_scores = (weights * (grad_weights - delta)).astype(BF16)
    dk_sum[pair] += matrix_product(grad_scores, q_ref[...])
    dv_sum[pair] += matrix_product(rounded, grad)
    dq = (matrix_product(k_turned[pair], grad_scores).T * SCALE).astype(BF16).astype(F32)
    dq, gain_rows = rms_backward(q_pre[...], gain_q[...], rope_back(dq, cos_q[...], sin_q[...]))
    dq_ref[...] = dq.astype(BF16)
    dgain_q[...] += jnp.sum(gain_rows, axis=0, keepdims=True)

    @pl.when(last)
    def _():
        for which in range(kv):
            own = pl.ds(which * HEAD_SIZE, HEAD_SIZE)
            dk = (dk_sum[which] * SCALE).astype(BF16).astype(F32)
            dk, gain_rows = rms_backward(
                k_pre[:, own], gain_k[...], rope_back(dk, cos_k[...], sin_k[...])
            )
            dk_ref[:, own] = dk.astype(BF16)
            dgain_k[...] += jnp.sum(gain_rows, axis=0, keepdims=True)
            dv_ref[:, own] = dv_sum[which].astype(BF16)
        for step in range(1, seq):
            grad_copy(step).wait_send()
        bulk_relay.finish(bulk_sum)


def attend_backward(
    weights, query, key, value, grad_own, bulk, q_pre, k_pre, gain_q, gain_k, cosine, sine, n, call_id
):
    rows = q_pre.shape[0]
    heads = q_pre.shape[1] // HEAD_SIZE
    kv = heads // GROUP
    block = rows // n
    turn = turned_block(0)
    q_spec = pl.BlockSpec((block, HEAD_SIZE), lambda i, h: (turn(i), h))
    k_spec = pl.BlockSpec((rows, kv * HEAD_SIZE), lambda i, h: (0, 0))
    gain_spec = pl.BlockSpec((1, HEAD_SIZE), lambda i, h: (0, 0))
    trig_q = pl.BlockSpec((block, HEAD_SIZE), lambda i, h: (turn(i), 0))
    trig_k = pl.BlockSpec((rows, HEAD_SIZE), lambda i, h: (0, 0))
    return pl.pallas_call(
        backward_kernel,
        grid=(n, heads),
        out_shape=(
            jax.ShapeDtypeStruct((rows, heads * HEAD_SIZE), BF16),
            jax.ShapeDtypeStruct((rows, kv * HEAD_SIZE), BF16),
            jax.ShapeDtypeStruct((rows, kv * HEAD_SIZE), BF16),
            jax.ShapeDtypeStruct((1, HEAD_SIZE), F32),
            jax.ShapeDtypeStruct((1, HEAD_SIZE), F32),
            jax.ShapeDtypeStruct((block, bulk.shape[1]), F32),
        ),
        in_specs=[
            pl.BlockSpec((1, rows, block), lambda i, h: (h, 0, turn(i))),
            q_spec, k_spec, k_spec, q_spec, k_spec, gain_spec, gain_spec,
            trig_q, trig_q, trig_k, trig_k, ANY_SPEC,
            pl.BlockSpec(bulk.shape, lambda i, h: (0, 0)),
        ],
        out_specs=(
            q_spec, k_spec, k_spec, gain_spec, gain_spec,
            pl.BlockSpec((block, bulk.shape[1]), lambda i, h: (0, 0)),
        ),
        scratch_shapes=[
            pltpu.VMEM((kv, HEAD_SIZE, rows), BF16),
            pltpu.VMEM((kv, rows, HEAD_SIZE), F32),
            pltpu.VMEM((kv, rows, HEAD_SIZE), F32),
            pltpu.VMEM((n, block, heads * HEAD_SIZE), BF16),
            pltpu.SemaphoreType.DMA((n - 1,)),
            pltpu.SemaphoreType.DMA((n - 1,)),
            pltpu.SemaphoreType.DMA,
        ]
        + RelayScatter.scratch(n, block, bulk.shape[1]),
        compiler_params=communicating(call_id),
        name="attend_backward",
    )(
        weights, query, key, value, q_pre, k_pre, gain_q, gain_k, cosine, sine, cosine, sine,
        grad_own, bulk,
    )


def on_device(
    tokens, lengths, packing, norm_in, w_query, key_projection, value_projection, norm_query,
    norm_key, w_out, norm_post, w_gate, w_up, w_down, cotangent,
):
    n = lax.axis_size("seq")
    shards = lax.axis_size("fsdp")
    me = lax.axis_index("seq")
    resident = tokens.shape[1]
    width = tokens.shape[2]
    rows = resident * n
    heads = HQ // n
    kv = KEY_VALUE_HEADS // n
    hidden_piece = w_down.shape[0] // n

    def columns(weight, pieces):
        size = weight.shape[1] // pieces
        return lax.dynamic_slice_in_dim(weight, me * size, size, axis=1)

    def spread_columns(weight):
        pieces = weight.reshape(weight.shape[0], shards, n, hidden_piece)
        return lax.dynamic_index_in_dim(pieces, me, axis=2, keepdims=False).reshape(
            weight.shape[0], shards * hidden_piece
        )

    def tile_of(values):
        pad = 1024 - values.shape[-1]
        values = jnp.concatenate([values, jnp.zeros(values.shape[:-1] + (pad,), F32)], axis=-1)
        return values.reshape(values.shape[:-1] + (8, 128))

    part, small = norm_in.shape[0], norm_query.shape[0]
    whole, gains = gather_first(
        tokens[0],
        tile_of(jnp.concatenate([norm_in, norm_post, norm_query, norm_key]).astype(F32)),
        n, shards, 0,
    )
    gains = gains.reshape(shards, -1)
    gain_in = gains[:, :part].reshape(1, -1)
    gain_post = gains[:, part : 2 * part].reshape(1, -1)
    gain_query = gains[:, 2 * part : 2 * part + small].reshape(1, -1)
    gain_key = gains[:, 2 * part + small : 2 * part + 2 * small].reshape(1, -1)

    def gathered(*weights):
        sizes = [weight.shape[0] for weight in weights]
        if len({weight.shape[1] for weight in weights}) > 1:
            return [lax.all_gather(weight, "fsdp", axis=0, tiled=True) for weight in weights]
        joined = lax.all_gather(jnp.concatenate(weights, axis=0), "fsdp", axis=0)
        starts = [sum(sizes[:i]) for i in range(len(sizes))]
        return [
            joined[:, start : start + size].reshape(-1, joined.shape[2])
            for start, size in zip(starts, sizes)
        ]

    qkv_weight, down_weight = gathered(
        jnp.concatenate(
            [columns(w_query, n), columns(key_projection, n), columns(value_projection, n)], axis=1
        ),
        lax.dynamic_slice_in_dim(w_down, me * hidden_piece, hidden_piece, axis=0),
    )
    out_weight = lax.all_gather(w_out, "fsdp", axis=0, tiled=True)
    gate_up_weight = lax.all_gather(
        jnp.concatenate([spread_columns(w_gate), spread_columns(w_up)], axis=1), "fsdp", axis=0, tiled=True
    )

    order = packing[0]
    places = jnp.arange(rows, dtype=jnp.int32)
    place = jnp.sum(jnp.where(order[None, :] == places[:, None], places[None, :], 0), axis=1)
    ends = jnp.cumsum(lengths[0])
    start = jnp.sum(jnp.where(place[:, None] >= ends[None, :], lengths[0][None, :], 0), axis=1)
    half = HEAD_SIZE // 2
    inv_freq = ROPE_BASE ** (-jnp.arange(half, dtype=F32) / half)
    angles = (place - start).astype(F32)[:, None] * inv_freq[None, :]
    cosine, sine = jnp.cos(angles), jnp.sin(angles)
    cosine = jnp.concatenate([cosine, cosine], axis=1)
    sine = jnp.concatenate([-sine, sine], axis=1)

    inputs = tokens[0].astype(F32)
    whole_f32 = whole.astype(F32)
    unit = whole_f32 * inverse_rms(whole_f32)
    normalized = (unit * gain_in).astype(BF16)
    qkv = matrix_product(normalized, qkv_weight)
    split = heads * HEAD_SIZE
    q_pre = qkv[:, :split]
    k_pre = qkv[:, split : split + kv * HEAD_SIZE]
    value = qkv[:, split + kv * HEAD_SIZE :].astype(BF16)
    attended, weights, query, key, grad_mlp = attend_forward(
        q_pre, k_pre, value, gain_query, gain_key, cosine, sine, place, start, cotangent[0], n, 1
    )
    middle = inputs + matrix_product(attended, out_weight)
    normed_post_mine = (middle * inverse_rms(middle) * gain_post).astype(BF16)
    normed_post = gather_rows(normed_post_mine, n, 2)

    grad_hidden = lax.optimization_barrier(back_matmul(grad_mlp, down_weight))
    gate_up = matrix_product(normed_post, gate_up_weight)
    units = shards * hidden_piece
    gate, up = gate_up[:, :units], gate_up[:, units:]
    logistic = 1.0 / (1.0 + jnp.exp(-gate))
    hidden = (gate / (1.0 + jnp.exp(-gate)) * up).astype(BF16)
    grad_gate = (grad_hidden * up * (logistic + gate * logistic * (1.0 - logistic))).astype(BF16)
    grad_up = (grad_hidden * gate * logistic).astype(BF16)
    grad_gate_up = jnp.concatenate([grad_gate, grad_up], axis=1)
    grad_gate_up_weight = outer_sum(normed_post, grad_gate_up).astype(BF16)
    grad_gate_up_weight, grad_gate_up, hidden = lax.optimization_barrier(
        (grad_gate_up_weight, grad_gate_up, hidden)
    )
    mlp_partial = matrix_product(hidden, down_weight).astype(BF16)
    grad_partial, grad_down = lax.optimization_barrier(
        (
            back_matmul(grad_gate_up, gate_up_weight).astype(BF16),
            outer_sum(hidden, grad_mlp).astype(BF16),
        )
    )
    gate_up_share = lax.psum_scatter(grad_gate_up_weight, "fsdp", scatter_dimension=0, tiled=True)
    grad_normed_post = scatter_sum(grad_partial, n, 3)
    grad_middle, gain_rows = rms_backward(middle, gain_post, grad_normed_post)
    grad_middle = cotangent[0].astype(F32) + grad_middle
    grad_gain_post = jnp.sum(gain_rows, axis=0)
    grad_branch = grad_middle.astype(BF16)
    grad_out = outer_sum(attended, grad_branch).astype(BF16)
    out_down_share = lax.psum_scatter(
        jnp.concatenate(
            [grad_out.reshape(shards, -1, width), grad_down.reshape(shards, -1, width)], axis=1
        ).reshape(-1, width),
        "fsdp", scatter_dimension=0, tiled=True,
    )
    out_share, down_share = out_down_share[: w_out.shape[0]], out_down_share[w_out.shape[0] :]
    grad_attended = back_matmul(grad_branch, out_weight).astype(BF16)
    grad_q, grad_k, grad_v, grad_gain_query, grad_gain_key, mlp_sum = attend_backward(
        weights, query, key, value, grad_attended, mlp_partial, q_pre, k_pre, gain_query,
        gain_key, cosine, sine, n, 4,
    )
    output = (middle + mlp_sum).astype(BF16)[None]
    grad_qkv = jnp.concatenate([grad_q, grad_k, grad_v], axis=1)
    grad_qkv_weight = outer_sum(normalized, grad_qkv).astype(BF16)
    qkv_share = lax.psum_scatter(grad_qkv_weight, "fsdp", scatter_dimension=0, tiled=True)
    gate_up_share, _ = lax.optimization_barrier((gate_up_share, grad_qkv))
    gate_up_all = [gate_up_share]
    for step in range(1, n):
        pairs = [(i, (i + step) % n) for i in range(n)]
        gate_up_all.append(lax.ppermute(gate_up_share, "seq", pairs))
    partial = back_matmul(grad_qkv, qkv_weight)
    grad_gain_in = jnp.sum(partial * unit, axis=0)
    small_grads = [grad_gain_in, grad_gain_post, grad_gain_query, grad_gain_key]
    small_grads = tile_of(jnp.concatenate([g.reshape(shards, -1) for g in small_grads], axis=1))
    grad_normed, gain_shares = scatter_last(
        partial.astype(BF16), small_grads, n, shards, 5
    )
    late_down, late_out, _ = lax.optimization_barrier((down_share, out_share, gain_shares))
    down_all, final_out = share(late_down, late_out, n, 7)
    gain_shares = gain_shares.reshape(-1)
    grad_inputs, _ = rms_backward(inputs, gain_in, grad_normed)
    input_grad = (grad_middle + grad_inputs).astype(BF16)[None]

    final_down = down_all.astype(F32).reshape(-1, width)
    by_step = jnp.stack(gate_up_all)
    final_gate, final_up = spread_back(
        jnp.stack(
            [
                lax.dynamic_index_in_dim(by_step, lax.rem(me + n - owner, n), keepdims=False)
                for owner in range(n)
            ]
        ),
        hidden_piece,
    )
    final_query, final_key, final_value = finish(
        qkv_share, (HQ * HEAD_SIZE,) + (KEY_VALUE_HEADS * HEAD_SIZE,) * 2, n, 6
    )

    return (
        output,
        input_grad,
        gain_shares[:part],
        final_query,
        final_key,
        final_value,
        gain_shares[2 * part : 2 * part + small],
        gain_shares[2 * part + small : 2 * part + 2 * small],
        final_out,
        gain_shares[part : 2 * part],
        final_gate,
        final_up,
        final_down,
    )


def solution(mesh):
    flat, wide = P("fsdp"), P("fsdp", None)
    whole = P("fsdp", "seq", None)
    in_specs = (
        whole, wide, wide, flat, wide, wide, wide, flat, flat, wide, flat, wide, wide, wide, whole,
    )
    out_specs = (whole, whole, flat, wide, wide, wide, flat, flat, wide, flat, wide, wide, wide)

    return jax.shard_map(
        on_device, mesh=mesh, in_specs=in_specs, out_specs=out_specs, check_vma=False
    )
```

```python
import functools

import jax
import jax.numpy as jnp
from jax import lax
from jax.experimental import pallas as pl
from jax.experimental.pallas import tpu as pltpu
from jax.sharding import PartitionSpec as P


HQ = 16
KEY_VALUE_HEADS = 8
HEAD_SIZE = 128
GROUP = HQ // KEY_VALUE_HEADS

ROPE_BASE = 1000000.0
EPSILON = 1e-06
MASKED = -1e30
SCALE = HEAD_SIZE ** (-0.5)
MESH = pl.DeviceIdType.MESH
BF16 = jnp.bfloat16
F32 = jnp.float32


def matrix_product(left, right):
    return jnp.dot(left, right, preferred_element_type=F32)


def outer_sum(left, right):
    return lax.dot_general(left, right, (((0,), (0,)), ((), ())), preferred_element_type=F32)


def back_matmul(left, right):
    return lax.dot_general(left, right, (((1,), (1,)), ((), ())), preferred_element_type=F32)


def inverse_rms(values):
    return lax.rsqrt(jnp.mean(values * values, axis=-1, keepdims=True) + EPSILON)


def rms_backward(values, gain, grad):
    c = inverse_rms(values)
    scaled = grad * gain
    inner = jnp.mean(values * scaled, axis=-1, keepdims=True)
    return c * scaled - values * (c * c * c) * inner, grad * values * c


def greet(*axes):
    barrier = pltpu.get_barrier_semaphore()
    count = 0
    for axis in axes:
        n = lax.axis_size(axis)
        me = lax.axis_index(axis)
        for step in range(1, n):
            pl.semaphore_signal(
                barrier, inc=1, device_id={axis: lax.rem(me + step, n)}, device_id_type=MESH
            )
        count += n - 1
    pl.semaphore_wait(barrier, count)


def block_of(index, size):
    return pl.ds(pl.multiple_of(index * size, size), size)


def start_to_peers(axis, source, target, send_sem, recv_sem):
    n = lax.axis_size(axis)
    me = lax.axis_index(axis)
    copies = []
    for step in range(1, n):
        peer = lax.rem(me + step, n)
        copy = pltpu.make_async_remote_copy(
            src_ref=source(peer),
            dst_ref=target(step),
            send_sem=send_sem.at[step - 1],
            recv_sem=recv_sem.at[step - 1],
            device_id={axis: peer},
            device_id_type=MESH,
        )
        copy.start()
        copies.append(copy)
    return copies


def semaphores(*counts):
    return [pltpu.SemaphoreType.DMA((count,)) for count in counts]


VMEM_SPEC = pl.BlockSpec(memory_space=pltpu.VMEM)
ANY_SPEC = pl.BlockSpec(memory_space=pl.ANY)


def communicating(call_id, **more):
    return pltpu.CompilerParams(collective_id=call_id, has_side_effects=True, **more)


def remote(source, target, send_sem, recv_sem, peer):
    return pltpu.make_async_remote_copy(
        src_ref=source,
        dst_ref=target,
        send_sem=send_sem,
        recv_sem=recv_sem,
        device_id={"seq": peer},
        device_id_type=MESH,
    )


class Plane:
    def __init__(self):
        self.n = lax.axis_size("seq")
        self.ny = self.n // 2
        self.me = lax.axis_index("seq")
        self.x = lax.rem(self.me, 2)
        self.y = self.me // 2

    def at(self, j, across):
        row = lax.rem(self.y + j + self.ny, self.ny)
        return row * 2 + ((1 - self.x) if across else self.x)


class RelayGather(Plane):
    def __init__(self, source, target, sems):
        super().__init__()
        self.source, self.target = source, target
        self.sx, self.rx, self.sy, self.ry, self.sy2, self.ry2, self.sx2, self.rx2 = sems

    @staticmethod
    def semaphores(n):
        ny = n // 2
        dma = pltpu.SemaphoreType.DMA
        return [dma((2,))] * 2 + [dma((ny - 1, 2))] * 2 + [dma((ny - 1,))] * 4

    def x1(self, half):
        return remote(
            self.source(half), self.target(self.me, half), self.sx.at[half], self.rx.at[half],
            self.at(0, True),
        )

    def y1(self, j, half):
        return remote(
            self.source(half), self.target(self.me, half), self.sy.at[j - 1, half],
            self.ry.at[j - 1, half], self.at(j, False),
        )

    def y2(self, j):
        block = self.target(self.at(0, True), 0)
        return remote(block, block, self.sy2.at[j - 1], self.ry2.at[j - 1], self.at(j, False))

    def x2(self, j):
        block = self.target(self.at(-j, False), 1)
        return remote(block, block, self.sx2.at[j - 1], self.rx2.at[j - 1], self.at(0, True))

    def start(self):
        others = range(1, self.ny)
        self.x1(0).start()
        for j in others:
            self.y1(j, 1).start()
        self.x1(1).start()
        for j in others:
            self.y1(j, 0).start()

    def forward(self):
        others = range(1, self.ny)
        self.x1(0).wait_recv()
        for j in others:
            self.y2(j).start()
        for j in others:
            self.y1(j, 1).wait_recv()
            self.x2(j).start()

    def finish(self):
        self.x1(0).wait_send()
        self.x1(1).wait()
        for j in range(1, self.ny):
            self.y1(j, 1).wait_send()
            self.y1(j, 0).wait()
            self.y2(j).wait()
            self.x2(j).wait()


def row_halves(ref, rows, owner, half):
    size = rows // 2
    return ref.at[pl.ds(pl.multiple_of(owner * rows + half * size, size), size)]


def column_halves(ref, half):
    size = ref.shape[-1] // 2
    return ref.at[:, half * size : (half + 1) * size]


def gather_by_rows(x_ref, o_ref, sems):
    rows = x_ref.shape[0]
    return RelayGather(
        lambda half: row_halves(x_ref, rows, 0, half),
        lambda owner, half: row_halves(o_ref, rows, owner, half),
        sems,
    )


def gather_by_columns(x_ref, o_ref, sems):
    return RelayGather(
        lambda half: column_halves(x_ref, half),
        lambda owner, half: column_halves(o_ref.at[owner], half),
        sems,
    )


class RelayScatter(Plane):
    def __init__(self, partial, buffers, sems):
        super().__init__()
        self.partial = partial
        self.rows = partial.shape[0] // self.n
        self.from_x, self.from_y, self.sent_y, self.late_y, self.sent_x, self.late_x = buffers
        self.sx, self.rx, self.sy, self.ry, self.sy2, self.ry2, self.sx2, self.rx2 = sems

    @staticmethod
    def scratch(n, rows, width):
        ny, half = n // 2, rows // 2
        dma = pltpu.SemaphoreType.DMA
        return [
            pltpu.VMEM((ny, half, width), BF16),
            pltpu.VMEM((ny - 1, 2, half, width), BF16),
            pltpu.VMEM((ny - 1, half, width), BF16),
            pltpu.VMEM((ny - 1, half, width), BF16),
            pltpu.VMEM((half, width), BF16),
            pltpu.VMEM((half, width), BF16),
        ] + [dma((ny,))] * 2 + [dma((ny - 1, 2))] * 2 + [dma((ny - 1,))] * 2 + [dma((1,))] * 2

    def piece(self, owner, half):
        return row_halves(self.partial, self.rows, owner, half)

    def x1(self, j):
        return remote(
            self.piece(self.at(j, True), 0), self.from_x.at[j], self.sx.at[j], self.rx.at[j],
            self.at(0, True),
        )

    def y1(self, j, final):
        return remote(
            self.piece(self.at(j, not final), 1), self.from_y.at[j - 1, int(final)],
            self.sy.at[j - 1, int(final)], self.ry.at[j - 1, int(final)], self.at(j, False),
        )

    def y2(self, j):
        return remote(
            self.sent_y.at[j - 1], self.late_y.at[j - 1], self.sy2.at[j - 1], self.ry2.at[j - 1],
            self.at(j, False),
        )

    def x2(self):
        return remote(self.sent_x, self.late_x, self.sx2.at[0], self.rx2.at[0], self.at(0, True))

    def start(self):
        others = range(1, self.ny)
        for j in others:
            self.x1(j).start()
            self.y1(j, False).start()
        self.x1(0).start()
        for j in others:
            self.y1(j, True).start()

    def forward(self, o_ref):
        others = range(1, self.ny)
        half = self.rows // 2
        for j in others:
            self.x1(j).wait_recv()
            own = self.piece(self.at(j, False), 0)[...].astype(F32)
            self.sent_y[j - 1] = (own + self.from_x[j].astype(F32)).astype(BF16)
        total = self.piece(self.at(0, True), 1)[...].astype(F32)
        for j in others:
            self.y1(j, False).wait_recv()
            total = total + self.from_y[j - 1, 0].astype(F32)
        self.sent_x[...] = total.astype(BF16)
        for j in others:
            self.y2(j).start()
        o_ref[:half, :] = self.piece(self.me, 0)[...].astype(F32)
        self.x2().start()
        o_ref[half:, :] = self.piece(self.me, 1)[...].astype(F32)

    def finish(self, o_ref):
        others = range(1, self.ny)
        half = self.rows // 2
        self.x1(0).wait()
        first = o_ref[:half, :] + self.from_x[0].astype(F32)
        second = o_ref[half:, :]
        for j in others:
            self.x1(j).wait_send()
            self.y1(j, False).wait_send()
            self.y1(j, True).wait()
            second = second + self.from_y[j - 1, 1].astype(F32)
        for j in others:
            self.y2(j).wait()
            first = first + self.late_y[j - 1].astype(F32)
        o_ref[:half, :] = first
        self.x2().wait()
        o_ref[half:, :] = second + self.late_x[...].astype(F32)


def gather_kernel(x_ref, o_ref, *sems):
    greet("seq")
    relay = gather_by_rows(x_ref, o_ref, sems)
    relay.start()
    o_ref[block_of(lax.axis_index("seq"), x_ref.shape[0]), :] = x_ref[...]
    relay.forward()
    relay.finish()


def gather_rows(x, n, call_id):
    rows, width = x.shape
    return pl.pallas_call(
        gather_kernel,
        out_shape=jax.ShapeDtypeStruct((n * rows, width), x.dtype),
        in_specs=[VMEM_SPEC],
        out_specs=VMEM_SPEC,
        scratch_shapes=RelayGather.semaphores(n),
        compiler_params=communicating(call_id),
    )(x)


def gather_first_kernel(x_ref, gains_ref, o_ref, all_gains, gain_send, gain_recv, *sems):
    greet("seq", "fsdp")
    place = lax.axis_index("fsdp")
    gain_copies = start_to_peers(
        "fsdp", lambda peer: gains_ref, lambda step: all_gains.at[place], gain_send, gain_recv
    )
    relay = gather_by_rows(x_ref, o_ref, sems)
    relay.start()
    o_ref[block_of(lax.axis_index("seq"), x_ref.shape[0]), :] = x_ref[...]
    all_gains[place] = gains_ref[...]
    relay.forward()
    relay.finish()
    for copy in gain_copies:
        copy.wait()


def gather_first(x, gains, n, shards, call_id):
    rows, width = x.shape
    return pl.pallas_call(
        gather_first_kernel,
        out_shape=(
            jax.ShapeDtypeStruct((n * rows, width), x.dtype),
            jax.ShapeDtypeStruct((shards,) + gains.shape, gains.dtype),
        ),
        in_specs=[VMEM_SPEC, VMEM_SPEC],
        out_specs=(VMEM_SPEC, VMEM_SPEC),
        scratch_shapes=semaphores(shards - 1, shards - 1) + RelayGather.semaphores(n),
        compiler_params=communicating(call_id),
        name="gather_first",
    )(x, gains)


def scatter_kernel(p_ref, o_ref, *scratch):
    greet("seq")
    relay = RelayScatter(p_ref, scratch[:6], scratch[6:])
    relay.start()
    relay.forward(o_ref)
    relay.finish(o_ref)


def scatter_sum(partial, n, call_id):
    total, width = partial.shape
    rows = total // n
    return pl.pallas_call(
        scatter_kernel,
        out_shape=jax.ShapeDtypeStruct((rows, width), F32),
        in_specs=[VMEM_SPEC],
        out_specs=VMEM_SPEC,
        scratch_shapes=RelayScatter.scratch(n, rows, width),
        compiler_params=communicating(call_id),
    )(partial)


def scatter_last_kernel(
    p_ref, small_ref, o_ref, small_out, part_landed, part_sum, row_landed,
    part_send, part_recv, row_send, row_recv, *scratch,
):
    greet("seq", "fsdp")
    part_copies = start_to_peers(
        "fsdp",
        lambda peer: small_ref.at[peer],
        lambda step: part_landed.at[step - 1],
        part_send,
        part_recv,
    )
    relay = RelayScatter(p_ref, scratch[:6], scratch[6:])
    relay.start()
    total = small_ref[lax.axis_index("fsdp")]
    for step, copy in enumerate(part_copies):
        copy.wait()
        total = total + part_landed[step]
    part_sum[...] = total
    relay.forward(o_ref)
    row_copies = start_to_peers(
        "seq", lambda peer: part_sum, lambda step: row_landed.at[step - 1], row_send, row_recv
    )
    relay.finish(o_ref)
    for step, copy in enumerate(row_copies):
        copy.wait()
        total = total + row_landed[step]
    small_out[...] = total


def scatter_last(partial, small, n, shards, call_id):
    total, width = partial.shape
    rows = total // n
    piece = small.shape[1:]
    return pl.pallas_call(
        scatter_last_kernel,
        out_shape=(jax.ShapeDtypeStruct((rows, width), F32), jax.ShapeDtypeStruct(piece, F32)),
        in_specs=[VMEM_SPEC] * 2,
        out_specs=(VMEM_SPEC,) * 2,
        scratch_shapes=[
            pltpu.VMEM((shards - 1,) + piece, F32),
            pltpu.VMEM(piece, F32),
            pltpu.VMEM((n - 1,) + piece, F32),
        ]
        + semaphores(shards - 1, shards - 1, n - 1, n - 1)
        + RelayScatter.scratch(n, rows, width),
        compiler_params=communicating(call_id),
        name="scatter_last",
    )(partial, small)


def finish_kernel(
    qkv_ref, joined_ref, qkv_all, down_all, out_all, out_landed, out_mine,
    first_send, first_recv, second_send, second_recv, *sems,
):
    greet("seq")
    me = lax.axis_index("seq")
    piece = out_mine.shape[0]
    below = out_all.shape[0]
    count = down_all.shape[1]
    first = start_to_peers(
        "seq",
        lambda peer: joined_ref.at[block_of(peer, piece)],
        lambda step: out_landed.at[step - 1],
        first_send,
        first_recv,
    )
    qkv = gather_by_columns(qkv_ref, qkv_all, sems[:8])
    down = gather_by_columns(joined_ref.at[pl.ds(below, count)], down_all, sems[8:])
    qkv.start()
    down.start()
    qkv_all[me] = qkv_ref[...]
    down_all[me] = joined_ref[below:, :]
    total = joined_ref[block_of(me, piece), :].astype(F32)
    for step, copy in enumerate(first):
        copy.wait()
        total = total + out_landed[step].astype(F32)
    out_mine[...] = total.astype(BF16)
    qkv.forward()
    mine = block_of(me, piece)
    second = start_to_peers(
        "seq", lambda peer: out_mine, lambda step: out_all.at[mine], second_send, second_recv
    )
    out_all[mine, :] = out_mine[...]
    down.forward()
    qkv.finish()
    down.finish()
    for copy in second:
        copy.wait()


def finish(qkv, joined, out_rows, n, call_id):
    width = joined.shape[1]
    down_rows = joined.shape[0] - out_rows
    return pl.pallas_call(
        finish_kernel,
        out_shape=(
            jax.ShapeDtypeStruct((n,) + qkv.shape, BF16),
            jax.ShapeDtypeStruct((n, down_rows, width), BF16),
            jax.ShapeDtypeStruct((out_rows, width), BF16),
        ),
        in_specs=[VMEM_SPEC] * 2,
        out_specs=(VMEM_SPEC,) * 3,
        scratch_shapes=[
            pltpu.VMEM((n - 1, out_rows // n, width), BF16),
            pltpu.VMEM((out_rows // n, width), BF16),
        ]
        + semaphores(*([n - 1] * 4))
        + RelayGather.semaphores(n) * 2,
        compiler_params=communicating(call_id),
        name="finish",
    )(qkv, joined)


def widen_kernel(qkv_ref, down_ref, out_ref, q_final, k_final, v_final, down_final, out_final):
    n = qkv_ref.shape[0]
    split = q_final.shape[1] // n
    narrow = k_final.shape[1] // n
    for owner in range(n):
        values = qkv_ref[owner].astype(F32)
        q_final[:, owner * split : (owner + 1) * split] = values[:, :split]
        k_final[:, owner * narrow : (owner + 1) * narrow] = values[:, split : split + narrow]
        v_final[:, owner * narrow : (owner + 1) * narrow] = values[:, split + narrow :]
    down_final[...] = down_ref[...].astype(F32)
    out_final[...] = out_ref[...].astype(F32)


def widen(qkv_all, down_all, out_all, widths):
    n, rows, _ = qkv_all.shape
    steps = 4

    def by_rows(shape):
        return pl.BlockSpec((shape[0] // steps, shape[1]), lambda i: (i, 0))

    qkv_spec = pl.BlockSpec((n, rows // steps, qkv_all.shape[2]), lambda i: (0, i, 0))
    down_spec = pl.BlockSpec((n // steps,) + down_all.shape[1:], lambda i: (i, 0, 0))
    shapes = [(rows, size) for size in widths]
    return pl.pallas_call(
        widen_kernel,
        grid=(steps,),
        out_shape=tuple(
            jax.ShapeDtypeStruct(shape, F32) for shape in shapes + [down_all.shape, out_all.shape]
        ),
        in_specs=[qkv_spec, down_spec, by_rows(out_all.shape)],
        out_specs=tuple(by_rows(shape) for shape in shapes) + (down_spec, by_rows(out_all.shape)),
        name="widen",
    )(qkv_all, down_all, out_all)


def spread_kernel(hidden_piece, pieces_ref, gate_ref, up_ref):
    n, _, width = pieces_ref.shape
    units = width // 2
    span = n * hidden_piece
    for target, base in ((gate_ref, 0), (up_ref, units)):
        for shard in range(units // hidden_piece):
            at = base + shard * hidden_piece
            target[:, shard * span : (shard + 1) * span] = jnp.concatenate(
                [pieces_ref[s, :, at : at + hidden_piece].astype(F32) for s in range(n)], axis=1
            )


def spread_back(pieces, hidden_piece):
    n, rows, width = pieces.shape
    shape = jax.ShapeDtypeStruct((rows, n * width // 2), F32)
    return pl.pallas_call(
        functools.partial(spread_kernel, hidden_piece),
        out_shape=(shape, shape),
        in_specs=[VMEM_SPEC],
        out_specs=(VMEM_SPEC, VMEM_SPEC),
        name="spread_back",
    )(pieces)


def rope(values, cosine, sine):
    return values * cosine + pltpu.roll(values, HEAD_SIZE // 2, 1) * sine


def rope_back(grad, cosine, sine):
    return grad * cosine - pltpu.roll(grad, HEAD_SIZE // 2, 1) * sine


def head_columns(index):
    return pl.ds(pl.multiple_of(index * HEAD_SIZE, HEAD_SIZE), HEAD_SIZE)


def turned_block(shift):
    def block(i):
        return lax.rem(lax.axis_index("seq") + shift + i, lax.axis_size("seq"))

    return block


def forward_kernel(
    q_pre, k_pre, v_ref, gain_q, gain_k, cos_q, sin_q, cos_k, sin_k, place_k, place_q, start_q, cot,
    out_ref, p_ref, q_ref, k_ref, cot_all,
    v_turned, outs, cot_local, send, recv, local, *cot_sems,
):
    i, head = pl.program_id(0), pl.program_id(1)
    n, heads = pl.num_programs(0), pl.num_programs(1)
    seq = lax.axis_size("seq")
    me = lax.axis_index("seq")
    kv = outs.shape[1] // GROUP
    rows = cot.shape[0]
    mine = block_of(me, rows)

    cot_relay = gather_by_rows(cot, cot_all, cot_sems)
    cot_own = pltpu.make_async_copy(cot, cot_all.at[mine], cot_local)

    def out_copy(step, which):
        return pltpu.make_async_remote_copy(
            src_ref=outs.at[step, which],
            dst_ref=out_ref.at[:, head_columns(me * heads + which)],
            send_sem=send.at[step, which],
            recv_sem=recv.at[step, which],
            device_id={"seq": lax.rem(me + 1 + step, seq)},
            device_id_type=MESH,
        )

    def own_copy(which):
        return pltpu.make_async_copy(
            outs.at[seq - 1, which], out_ref.at[:, head_columns(me * heads + which)], local.at[which]
        )

    @pl.when((i == 0) & (head == 0))
    def _():
        greet("seq")
        cot_relay.start()
        cot_own.start()
        for which in range(kv):
            own = pl.ds(which * HEAD_SIZE, HEAD_SIZE)
            pre = k_pre[:, own]
            k_ref[:, own] = rope(
                pre * inverse_rms(pre) * gain_k[...], cos_k[...], sin_k[...]
            ).astype(BF16)
            v_turned[which] = v_ref[:, own].astype(F32).T.astype(BF16)

    @pl.when((i == n // 2) & (head == 0))
    def _():
        cot_relay.forward()

    @pl.when((head > 0) & (i < n - 1))
    def _():
        out_copy(i, head - 1).start()

    @pl.when((head == 0) & (i > 0))
    def _():
        out_copy(i - 1, heads - 1).start()

    pre = q_pre[...]
    query = rope(pre * inverse_rms(pre) * gain_q[...], cos_q[...], sin_q[...]).astype(BF16)
    q_ref[...] = query
    pair = head // GROUP
    scores = back_matmul(k_ref[:, head_columns(pair)], query) * SCALE
    keys = place_k[...]
    allowed = (keys <= place_q[...]) & (keys >= start_q[...])
    scores = jnp.where(allowed, scores, MASKED)
    top = jnp.max(scores, axis=0, keepdims=True)
    weights = jnp.exp(scores - top)
    total = jnp.sum(weights, axis=0, keepdims=True)
    weights = (weights * (1.0 / total)).astype(BF16)
    p_ref[0] = weights
    outs[i, head] = matrix_product(v_turned[pair], weights).T.astype(BF16)

    @pl.when((i == n - 1) & (head == heads - 1))
    def _():
        for which in range(outs.shape[1]):
            own_copy(which).start()
        cot_relay.finish()
        cot_own.wait()
        for step in range(seq - 1):
            for which in range(outs.shape[1]):
                out_copy(step, which).wait()
        for which in range(outs.shape[1]):
            own_copy(which).wait()


def attend_forward(
    q_pre, k_pre, value, gain_q, gain_k, cosine, sine, place, start, cotangent, n, call_id
):
    rows = q_pre.shape[0]
    heads = q_pre.shape[1] // HEAD_SIZE
    kv = heads // GROUP
    block = rows // n
    width = cotangent.shape[1]
    turn = turned_block(1)
    q_spec = pl.BlockSpec((block, HEAD_SIZE), lambda i, h: (turn(i), h))
    k_spec = pl.BlockSpec((rows, kv * HEAD_SIZE), lambda i, h: (0, 0))
    gain_spec = pl.BlockSpec((1, HEAD_SIZE), lambda i, h: (0, 0))
    trig_q = pl.BlockSpec((block, HEAD_SIZE), lambda i, h: (turn(i), 0))
    trig_k = pl.BlockSpec((rows, HEAD_SIZE), lambda i, h: (0, 0))
    column = pl.BlockSpec((rows, 1), lambda i, h: (0, 0))
    row = pl.BlockSpec((1, block), lambda i, h: (0, turn(i)))
    return pl.pallas_call(
        forward_kernel,
        grid=(n, heads),
        out_shape=(
            jax.ShapeDtypeStruct((block, n * heads * HEAD_SIZE), BF16),
            jax.ShapeDtypeStruct((heads, rows, rows), BF16),
            jax.ShapeDtypeStruct((rows, heads * HEAD_SIZE), BF16),
            jax.ShapeDtypeStruct((rows, kv * HEAD_SIZE), BF16),
            jax.ShapeDtypeStruct((rows, width), BF16),
        ),
        in_specs=[
            q_spec, k_spec, k_spec, gain_spec, gain_spec, trig_q, trig_q, trig_k, trig_k,
            column, row, row, ANY_SPEC,
        ],
        out_specs=(
            ANY_SPEC,
            pl.BlockSpec((1, rows, block), lambda i, h: (h, 0, turn(i))),
            q_spec,
            k_spec,
            ANY_SPEC,
        ),
        scratch_shapes=[
            pltpu.VMEM((kv, HEAD_SIZE, rows), BF16),
            pltpu.VMEM((n, heads, block, HEAD_SIZE), BF16),
            pltpu.SemaphoreType.DMA,
            pltpu.SemaphoreType.DMA((n - 1, heads)),
            pltpu.SemaphoreType.DMA((n - 1, heads)),
            pltpu.SemaphoreType.DMA((heads,)),
        ]
        + RelayGather.semaphores(n),
        compiler_params=communicating(call_id),
        name="attend_forward",
    )(
        q_pre, k_pre, value, gain_q, gain_k, cosine, sine, cosine, sine,
        place[:, None], place[None, :], start[None, :], cotangent,
    )


def backward_kernel(
    p_ref, q_ref, k_ref, v_ref, q_pre, k_pre, gain_q, gain_k, cos_q, sin_q, cos_k, sin_k,
    grad_own, bulk,
    dqkv_ref, dgain_q, dgain_k, bulk_sum,
    k_turned, dk_sum, dv_sum, grads, send, recv, local, *scratch,
):
    i, head = pl.program_id(0), pl.program_id(1)
    n, heads = pl.num_programs(0), pl.num_programs(1)
    seq = lax.axis_size("seq")
    me = lax.axis_index("seq")
    kv = k_turned.shape[0]
    rows = grads.shape[1]
    span = grads.shape[2]
    first = (i == 0) & (head == 0)
    last = (i == n - 1) & (head == heads - 1)

    def grad_copy(step):
        peer = lax.rem(me + step, seq)
        return pltpu.make_async_remote_copy(
            src_ref=grad_own.at[:, block_of(peer, span)],
            dst_ref=grads.at[step],
            send_sem=send.at[step - 1],
            recv_sem=recv.at[step - 1],
            device_id={"seq": peer},
            device_id_type=MESH,
        )

    bulk_relay = RelayScatter(bulk, scratch[:6], scratch[6:])
    own_copy = pltpu.make_async_copy(grad_own.at[:, block_of(me, span)], grads.at[0], local)

    @pl.when(first)
    def _():
        greet("seq")
        own_copy.start()
        for step in range(1, seq):
            grad_copy(step).start()
        bulk_relay.start()
        dgain_q[...] = jnp.zeros_like(dgain_q)
        dgain_k[...] = jnp.zeros_like(dgain_k)
        dk_sum[...] = jnp.zeros_like(dk_sum)
        dv_sum[...] = jnp.zeros_like(dv_sum)
        for which in range(kv):
            own = pl.ds(which * HEAD_SIZE, HEAD_SIZE)
            k_turned[which] = k_ref[:, own].astype(F32).T.astype(BF16)
        own_copy.wait()

    for step in range(1, seq):
        @pl.when((head == 0) & (i == seq - step))
        def _():
            grad_copy(step).wait_recv()

    @pl.when((i == n - 1) & (head == 0))
    def _():
        bulk_relay.forward(bulk_sum)

    slot = lax.rem(seq - i, seq)
    pair = head // GROUP
    rounded = p_ref[0]
    weights = rounded.astype(F32)
    grad = grads[slot, :, head_columns(head)]
    grad_weights = back_matmul(v_ref[:, head_columns(pair)], grad)
    delta = jnp.sum(weights * grad_weights, axis=0, keepdims=True)
    grad_scores = (weights * (grad_weights - delta)).astype(BF16)
    dk_sum[pair] += matrix_product(grad_scores, q_ref[...])
    dv_sum[pair] += matrix_product(rounded, grad)
    dq = (matrix_product(k_turned[pair], grad_scores).T * SCALE).astype(BF16).astype(F32)
    dq, gain_rows = rms_backward(q_pre[...], gain_q[...], rope_back(dq, cos_q[...], sin_q[...]))
    block = block_of(lax.rem(me + i, seq), rows)
    dqkv_ref[block, head_columns(head)] = dq.astype(BF16)
    dgain_q[...] += jnp.sum(gain_rows, axis=0, keepdims=True)

    @pl.when(last)
    def _():
        for which in range(kv):
            own = pl.ds(which * HEAD_SIZE, HEAD_SIZE)
            dk = (dk_sum[which] * SCALE).astype(BF16).astype(F32)
            dk, gain_rows = rms_backward(
                k_pre[:, own], gain_k[...], rope_back(dk, cos_k[...], sin_k[...])
            )
            dqkv_ref[:, head_columns(heads + which)] = dk.astype(BF16)
            dgain_k[...] += jnp.sum(gain_rows, axis=0, keepdims=True)
            dqkv_ref[:, head_columns(heads + kv + which)] = dv_sum[which].astype(BF16)
        for step in range(1, seq):
            grad_copy(step).wait_send()
        bulk_relay.finish(bulk_sum)


def attend_backward(
    weights, query, key, value, grad_own, bulk, q_pre, k_pre, gain_q, gain_k, cosine, sine, n, call_id
):
    rows = q_pre.shape[0]
    heads = q_pre.shape[1] // HEAD_SIZE
    kv = heads // GROUP
    block = rows // n
    turn = turned_block(0)
    q_spec = pl.BlockSpec((block, HEAD_SIZE), lambda i, h: (turn(i), h))
    k_spec = pl.BlockSpec((rows, kv * HEAD_SIZE), lambda i, h: (0, 0))
    gain_spec = pl.BlockSpec((1, HEAD_SIZE), lambda i, h: (0, 0))
    trig_q = pl.BlockSpec((block, HEAD_SIZE), lambda i, h: (turn(i), 0))
    trig_k = pl.BlockSpec((rows, HEAD_SIZE), lambda i, h: (0, 0))
    return pl.pallas_call(
        backward_kernel,
        grid=(n, heads),
        out_shape=(
            jax.ShapeDtypeStruct((rows, (heads + 2 * kv) * HEAD_SIZE), BF16),
            jax.ShapeDtypeStruct((1, HEAD_SIZE), F32),
            jax.ShapeDtypeStruct((1, HEAD_SIZE), F32),
            jax.ShapeDtypeStruct((block, bulk.shape[1]), F32),
        ),
        in_specs=[
            pl.BlockSpec((1, rows, block), lambda i, h: (h, 0, turn(i))),
            q_spec, k_spec, k_spec, q_spec, k_spec, gain_spec, gain_spec,
            trig_q, trig_q, trig_k, trig_k, ANY_SPEC,
            pl.BlockSpec(bulk.shape, lambda i, h: (0, 0)),
        ],
        out_specs=(
            pl.BlockSpec((rows, (heads + 2 * kv) * HEAD_SIZE), lambda i, h: (0, 0)),
            gain_spec, gain_spec,
            pl.BlockSpec((block, bulk.shape[1]), lambda i, h: (0, 0)),
        ),
        scratch_shapes=[
            pltpu.VMEM((kv, HEAD_SIZE, rows), BF16),
            pltpu.VMEM((kv, rows, HEAD_SIZE), F32),
            pltpu.VMEM((kv, rows, HEAD_SIZE), F32),
            pltpu.VMEM((n, block, heads * HEAD_SIZE), BF16),
            pltpu.SemaphoreType.DMA((n - 1,)),
            pltpu.SemaphoreType.DMA((n - 1,)),
            pltpu.SemaphoreType.DMA,
        ]
        + RelayScatter.scratch(n, block, bulk.shape[1]),
        compiler_params=communicating(call_id),
        name="attend_backward",
    )(
        weights, query, key, value, q_pre, k_pre, gain_q, gain_k, cosine, sine, cosine, sine,
        grad_own, bulk,
    )


def on_device(
    tokens, lengths, packing, norm_in, w_query, key_projection, value_projection, norm_query,
    norm_key, w_out, norm_post, w_gate, w_up, w_down, cotangent,
):
    n = lax.axis_size("seq")
    shards = lax.axis_size("fsdp")
    me = lax.axis_index("seq")
    resident = tokens.shape[1]
    width = tokens.shape[2]
    rows = resident * n
    heads = HQ // n
    kv = KEY_VALUE_HEADS // n
    hidden_piece = w_down.shape[0] // n

    def columns(weight, pieces):
        size = weight.shape[1] // pieces
        return lax.dynamic_slice_in_dim(weight, me * size, size, axis=1)

    def spread_columns(weight):
        pieces = weight.reshape(weight.shape[0], shards, n, hidden_piece)
        return lax.dynamic_index_in_dim(pieces, me, axis=2, keepdims=False).reshape(
            weight.shape[0], shards * hidden_piece
        )

    def tile_of(values):
        pad = 1024 - values.shape[-1]
        values = jnp.concatenate([values, jnp.zeros(values.shape[:-1] + (pad,), F32)], axis=-1)
        return values.reshape(values.shape[:-1] + (8, 128))

    part, small = norm_in.shape[0], norm_query.shape[0]
    whole, gains = gather_first(
        tokens[0],
        tile_of(jnp.concatenate([norm_in, norm_post, norm_query, norm_key]).astype(F32)),
        n, shards, 0,
    )
    gains = gains.reshape(shards, -1)
    gain_in = gains[:, :part].reshape(1, -1)
    gain_post = gains[:, part : 2 * part].reshape(1, -1)
    gain_query = gains[:, 2 * part : 2 * part + small].reshape(1, -1)
    gain_key = gains[:, 2 * part + small : 2 * part + 2 * small].reshape(1, -1)

    def gathered(*weights):
        sizes = [weight.shape[0] for weight in weights]
        if len({weight.shape[1] for weight in weights}) > 1:
            return [lax.all_gather(weight, "fsdp", axis=0, tiled=True) for weight in weights]
        joined = lax.all_gather(jnp.concatenate(weights, axis=0), "fsdp", axis=0)
        starts = [sum(sizes[:i]) for i in range(len(sizes))]
        return [
            joined[:, start : start + size].reshape(-1, joined.shape[2])
            for start, size in zip(starts, sizes)
        ]

    qkv_weight, down_weight = gathered(
        jnp.concatenate(
            [columns(w_query, n), columns(key_projection, n), columns(value_projection, n)], axis=1
        ),
        lax.dynamic_slice_in_dim(w_down, me * hidden_piece, hidden_piece, axis=0),
    )
    out_weight = lax.all_gather(w_out, "fsdp", axis=0, tiled=True)
    gate_up_weight = lax.all_gather(
        jnp.concatenate([spread_columns(w_gate), spread_columns(w_up)], axis=1), "fsdp", axis=0, tiled=True
    )

    order = packing[0]
    places = jnp.arange(rows, dtype=jnp.int32)
    place = jnp.sum(jnp.where(order[None, :] == places[:, None], places[None, :], 0), axis=1)
    ends = jnp.cumsum(lengths[0])
    start = jnp.sum(jnp.where(place[:, None] >= ends[None, :], lengths[0][None, :], 0), axis=1)
    half = HEAD_SIZE // 2
    inv_freq = ROPE_BASE ** (-jnp.arange(half, dtype=F32) / half)
    angles = (place - start).astype(F32)[:, None] * inv_freq[None, :]
    cosine, sine = jnp.cos(angles), jnp.sin(angles)
    cosine = jnp.concatenate([cosine, cosine], axis=1)
    sine = jnp.concatenate([-sine, sine], axis=1)

    inputs = tokens[0].astype(F32)
    whole_f32 = whole.astype(F32)
    unit = whole_f32 * inverse_rms(whole_f32)
    normalized = (unit * gain_in).astype(BF16)
    qkv = matrix_product(normalized, qkv_weight)
    split = heads * HEAD_SIZE
    q_pre = qkv[:, :split]
    k_pre = qkv[:, split : split + kv * HEAD_SIZE]
    value = qkv[:, split + kv * HEAD_SIZE :].astype(BF16)
    attended, weights, query, key, grad_mlp = attend_forward(
        q_pre, k_pre, value, gain_query, gain_key, cosine, sine, place, start, cotangent[0], n, 1
    )
    middle = inputs + matrix_product(attended, out_weight)
    normed_post_mine = (middle * inverse_rms(middle) * gain_post).astype(BF16)
    normed_post = gather_rows(normed_post_mine, n, 2)

    grad_hidden = lax.optimization_barrier(back_matmul(grad_mlp, down_weight))
    gate_up = matrix_product(normed_post, gate_up_weight)
    units = shards * hidden_piece
    gate, up = gate_up[:, :units], gate_up[:, units:]
    logistic = 1.0 / (1.0 + jnp.exp(-gate))
    hidden = (gate / (1.0 + jnp.exp(-gate)) * up).astype(BF16)
    grad_gate = (grad_hidden * up * (logistic + gate * logistic * (1.0 - logistic))).astype(BF16)
    grad_up = (grad_hidden * gate * logistic).astype(BF16)
    grad_gate_up = jnp.concatenate([grad_gate, grad_up], axis=1)
    grad_gate_up_weight = outer_sum(normed_post, grad_gate_up).astype(BF16)
    grad_gate_up_weight, grad_gate_up, hidden = lax.optimization_barrier(
        (grad_gate_up_weight, grad_gate_up, hidden)
    )
    mlp_partial = matrix_product(hidden, down_weight).astype(BF16)
    grad_partial, grad_down = lax.optimization_barrier(
        (
            back_matmul(grad_gate_up, gate_up_weight).astype(BF16),
            outer_sum(hidden, grad_mlp).astype(BF16),
        )
    )
    gate_up_share = lax.psum_scatter(grad_gate_up_weight, "fsdp", scatter_dimension=0, tiled=True)
    grad_normed_post = scatter_sum(grad_partial, n, 3)
    grad_middle, gain_rows = rms_backward(middle, gain_post, grad_normed_post)
    grad_middle = cotangent[0].astype(F32) + grad_middle
    grad_gain_post = jnp.sum(gain_rows, axis=0)
    grad_branch = grad_middle.astype(BF16)
    grad_out = outer_sum(attended, grad_branch).astype(BF16)
    out_down_share = lax.psum_scatter(
        jnp.concatenate(
            [grad_out.reshape(shards, -1, width), grad_down.reshape(shards, -1, width)], axis=1
        ).reshape(-1, width),
        "fsdp", scatter_dimension=0, tiled=True,
    )
    grad_attended = back_matmul(grad_branch, out_weight).astype(BF16)
    grad_qkv, grad_gain_query, grad_gain_key, mlp_sum = attend_backward(
        weights, query, key, value, grad_attended, mlp_partial, q_pre, k_pre, gain_query,
        gain_key, cosine, sine, n, 4,
    )
    output = (middle + mlp_sum).astype(BF16)[None]
    grad_qkv_weight = outer_sum(normalized, grad_qkv).astype(BF16)
    qkv_share = lax.psum_scatter(grad_qkv_weight, "fsdp", scatter_dimension=0, tiled=True)
    gate_up_share, _ = lax.optimization_barrier((gate_up_share, grad_qkv))
    gate_up_all = [gate_up_share]
    for step in range(1, n):
        pairs = [(i, (i + step) % n) for i in range(n)]
        gate_up_all.append(lax.ppermute(gate_up_share, "seq", pairs))
    partial = back_matmul(grad_qkv, qkv_weight)
    grad_gain_in = jnp.sum(partial * unit, axis=0)
    small_grads = [grad_gain_in, grad_gain_post, grad_gain_query, grad_gain_key]
    small_grads = tile_of(jnp.concatenate([g.reshape(shards, -1) for g in small_grads], axis=1))
    grad_normed, gain_shares = scatter_last(
        partial.astype(BF16), small_grads, n, shards, 5
    )
    gain_shares = gain_shares.reshape(-1)
    grad_inputs, _ = rms_backward(inputs, gain_in, grad_normed)
    input_grad = (grad_middle + grad_inputs).astype(BF16)[None]

    by_step = jnp.stack(gate_up_all)
    final_gate, final_up = spread_back(
        jnp.stack(
            [
                lax.dynamic_index_in_dim(by_step, lax.rem(me + n - owner, n), keepdims=False)
                for owner in range(n)
            ]
        ),
        hidden_piece,
    )
    qkv_all, down_all, out_all = finish(qkv_share, out_down_share, w_out.shape[0], n, 6)
    final_query, final_key, final_value, final_down, final_out = widen(
        qkv_all, down_all, out_all, (HQ * HEAD_SIZE,) + (KEY_VALUE_HEADS * HEAD_SIZE,) * 2
    )
    final_down = final_down.reshape(-1, width)

    return (
        output,
        input_grad,
        gain_shares[:part],
        final_query,
        final_key,
        final_value,
        gain_shares[2 * part : 2 * part + small],
        gain_shares[2 * part + small : 2 * part + 2 * small],
        final_out,
        gain_shares[part : 2 * part],
        final_gate,
        final_up,
        final_down,
    )


def solution(mesh):
    flat, wide = P("fsdp"), P("fsdp", None)
    whole = P("fsdp", "seq", None)
    in_specs = (
        whole, wide, wide, flat, wide, wide, wide, flat, flat, wide, flat, wide, wide, wide, whole,
    )
    out_specs = (whole, whole, flat, wide, wide, wide, flat, flat, wide, flat, wide, wide, wide)

    return jax.shard_map(
        on_device, mesh=mesh, in_specs=in_specs, out_specs=out_specs, check_vma=False
    )
```

```python
import functools

import jax
import jax.numpy as jnp
from jax import lax
from jax.experimental import pallas as pl
from jax.experimental.pallas import tpu as pltpu
from jax.sharding import PartitionSpec as P


HQ = 16
KEY_VALUE_HEADS = 8
HEAD_SIZE = 128
GROUP = HQ // KEY_VALUE_HEADS

ROPE_BASE = 1000000.0
EPSILON = 1e-06
MASKED = -1e30
SCALE = HEAD_SIZE ** (-0.5)
MESH = pl.DeviceIdType.MESH
BF16 = jnp.bfloat16
F32 = jnp.float32


def matrix_product(left, right):
    return jnp.dot(left, right, preferred_element_type=F32)


def outer_sum(left, right):
    return lax.dot_general(left, right, (((0,), (0,)), ((), ())), preferred_element_type=F32)


def back_matmul(left, right):
    return lax.dot_general(left, right, (((1,), (1,)), ((), ())), preferred_element_type=F32)


def inverse_rms(values):
    return lax.rsqrt(jnp.mean(values * values, axis=-1, keepdims=True) + EPSILON)


def rms_backward(values, gain, grad):
    c = inverse_rms(values)
    scaled = grad * gain
    inner = jnp.mean(values * scaled, axis=-1, keepdims=True)
    return c * scaled - values * (c * c * c) * inner, grad * values * c


def greet(*axes):
    barrier = pltpu.get_barrier_semaphore()
    count = 0
    for axis in axes:
        n = lax.axis_size(axis)
        me = lax.axis_index(axis)
        for step in range(1, n):
            pl.semaphore_signal(
                barrier, inc=1, device_id={axis: lax.rem(me + step, n)}, device_id_type=MESH
            )
        count += n - 1
    pl.semaphore_wait(barrier, count)


def block_of(index, size):
    return pl.ds(pl.multiple_of(index * size, size), size)


def start_to_peers(axis, source, target, send_sem, recv_sem):
    n = lax.axis_size(axis)
    me = lax.axis_index(axis)
    copies = []
    for step in range(1, n):
        peer = lax.rem(me + step, n)
        copy = pltpu.make_async_remote_copy(
            src_ref=source(peer),
            dst_ref=target(step),
            send_sem=send_sem.at[step - 1],
            recv_sem=recv_sem.at[step - 1],
            device_id={axis: peer},
            device_id_type=MESH,
        )
        copy.start()
        copies.append(copy)
    return copies


def semaphores(*counts):
    return [pltpu.SemaphoreType.DMA((count,)) for count in counts]


VMEM_SPEC = pl.BlockSpec(memory_space=pltpu.VMEM)
ANY_SPEC = pl.BlockSpec(memory_space=pl.ANY)


def communicating(call_id, **more):
    return pltpu.CompilerParams(collective_id=call_id, has_side_effects=True, **more)


def remote(source, target, send_sem, recv_sem, peer):
    return pltpu.make_async_remote_copy(
        src_ref=source,
        dst_ref=target,
        send_sem=send_sem,
        recv_sem=recv_sem,
        device_id={"seq": peer},
        device_id_type=MESH,
    )


class Plane:
    def __init__(self):
        self.n = lax.axis_size("seq")
        self.ny = self.n // 2
        self.me = lax.axis_index("seq")
        self.x = lax.rem(self.me, 2)
        self.y = self.me // 2

    def at(self, j, across):
        row = lax.rem(self.y + j + self.ny, self.ny)
        return row * 2 + ((1 - self.x) if across else self.x)


class RelayGather(Plane):
    def __init__(self, source, target, sems):
        super().__init__()
        self.source, self.target = source, target
        self.sx, self.rx, self.sy, self.ry, self.sy2, self.ry2, self.sx2, self.rx2 = sems

    @staticmethod
    def semaphores(n):
        ny = n // 2
        dma = pltpu.SemaphoreType.DMA
        return [dma((2,))] * 2 + [dma((ny - 1, 2))] * 2 + [dma((ny - 1,))] * 4

    def x1(self, half):
        return remote(
            self.source(half), self.target(self.me, half), self.sx.at[half], self.rx.at[half],
            self.at(0, True),
        )

    def y1(self, j, half):
        return remote(
            self.source(half), self.target(self.me, half), self.sy.at[j - 1, half],
            self.ry.at[j - 1, half], self.at(j, False),
        )

    def y2(self, j):
        block = self.target(self.at(0, True), 0)
        return remote(block, block, self.sy2.at[j - 1], self.ry2.at[j - 1], self.at(j, False))

    def x2(self, j):
        block = self.target(self.at(-j, False), 1)
        return remote(block, block, self.sx2.at[j - 1], self.rx2.at[j - 1], self.at(0, True))

    def start(self):
        others = range(1, self.ny)
        self.x1(0).start()
        for j in others:
            self.y1(j, 1).start()
        self.x1(1).start()
        for j in others:
            self.y1(j, 0).start()

    def forward(self):
        others = range(1, self.ny)
        self.x1(0).wait_recv()
        for j in others:
            self.y2(j).start()
        for j in others:
            self.y1(j, 1).wait_recv()
            self.x2(j).start()

    def finish(self):
        self.x1(0).wait_send()
        self.x1(1).wait()
        for j in range(1, self.ny):
            self.y1(j, 1).wait_send()
            self.y1(j, 0).wait()
            self.y2(j).wait()
            self.x2(j).wait()


def row_halves(ref, rows, owner, half):
    size = rows // 2
    return ref.at[pl.ds(pl.multiple_of(owner * rows + half * size, size), size)]


def column_halves(ref, half):
    size = ref.shape[-1] // 2
    return ref.at[:, half * size : (half + 1) * size]


def gather_by_rows(x_ref, o_ref, sems):
    rows = x_ref.shape[0]
    return RelayGather(
        lambda half: row_halves(x_ref, rows, 0, half),
        lambda owner, half: row_halves(o_ref, rows, owner, half),
        sems,
    )


def gather_by_columns(x_ref, o_ref, sems):
    return RelayGather(
        lambda half: column_halves(x_ref, half),
        lambda owner, half: column_halves(o_ref.at[owner], half),
        sems,
    )


class RelayScatter(Plane):
    def __init__(self, partial, buffers, sems):
        super().__init__()
        self.partial = partial
        self.rows = partial.shape[0] // self.n
        self.from_x, self.from_y, self.sent_y, self.late_y, self.sent_x, self.late_x = buffers
        self.sx, self.rx, self.sy, self.ry, self.sy2, self.ry2, self.sx2, self.rx2 = sems

    @staticmethod
    def scratch(n, rows, width):
        ny, half = n // 2, rows // 2
        dma = pltpu.SemaphoreType.DMA
        return [
            pltpu.VMEM((ny, half, width), BF16),
            pltpu.VMEM((ny - 1, 2, half, width), BF16),
            pltpu.VMEM((ny - 1, half, width), BF16),
            pltpu.VMEM((ny - 1, half, width), BF16),
            pltpu.VMEM((half, width), BF16),
            pltpu.VMEM((half, width), BF16),
        ] + [dma((ny,))] * 2 + [dma((ny - 1, 2))] * 2 + [dma((ny - 1,))] * 2 + [dma((1,))] * 2

    def piece(self, owner, half):
        return row_halves(self.partial, self.rows, owner, half)

    def x1(self, j):
        return remote(
            self.piece(self.at(j, True), 0), self.from_x.at[j], self.sx.at[j], self.rx.at[j],
            self.at(0, True),
        )

    def y1(self, j, final):
        return remote(
            self.piece(self.at(j, not final), 1), self.from_y.at[j - 1, int(final)],
            self.sy.at[j - 1, int(final)], self.ry.at[j - 1, int(final)], self.at(j, False),
        )

    def y2(self, j):
        return remote(
            self.sent_y.at[j - 1], self.late_y.at[j - 1], self.sy2.at[j - 1], self.ry2.at[j - 1],
            self.at(j, False),
        )

    def x2(self):
        return remote(self.sent_x, self.late_x, self.sx2.at[0], self.rx2.at[0], self.at(0, True))

    def start(self):
        others = range(1, self.ny)
        for j in others:
            self.x1(j).start()
            self.y1(j, False).start()
        self.x1(0).start()
        for j in others:
            self.y1(j, True).start()

    def forward(self, o_ref):
        others = range(1, self.ny)
        half = self.rows // 2
        for j in others:
            self.x1(j).wait_recv()
            own = self.piece(self.at(j, False), 0)[...].astype(F32)
            self.sent_y[j - 1] = (own + self.from_x[j].astype(F32)).astype(BF16)
        total = self.piece(self.at(0, True), 1)[...].astype(F32)
        for j in others:
            self.y1(j, False).wait_recv()
            total = total + self.from_y[j - 1, 0].astype(F32)
        self.sent_x[...] = total.astype(BF16)
        for j in others:
            self.y2(j).start()
        o_ref[:half, :] = self.piece(self.me, 0)[...].astype(F32)
        self.x2().start()
        o_ref[half:, :] = self.piece(self.me, 1)[...].astype(F32)

    def finish(self, o_ref):
        others = range(1, self.ny)
        half = self.rows // 2
        self.x1(0).wait()
        first = o_ref[:half, :] + self.from_x[0].astype(F32)
        second = o_ref[half:, :]
        for j in others:
            self.x1(j).wait_send()
            self.y1(j, False).wait_send()
            self.y1(j, True).wait()
            second = second + self.from_y[j - 1, 1].astype(F32)
        for j in others:
            self.y2(j).wait()
            first = first + self.late_y[j - 1].astype(F32)
        o_ref[:half, :] = first
        self.x2().wait()
        o_ref[half:, :] = second + self.late_x[...].astype(F32)


def gather_kernel(x_ref, o_ref, *sems):
    greet("seq")
    relay = gather_by_rows(x_ref, o_ref, sems)
    relay.start()
    o_ref[block_of(lax.axis_index("seq"), x_ref.shape[0]), :] = x_ref[...]
    relay.forward()
    relay.finish()


def gather_rows(x, n, call_id):
    rows, width = x.shape
    return pl.pallas_call(
        gather_kernel,
        out_shape=jax.ShapeDtypeStruct((n * rows, width), x.dtype),
        in_specs=[VMEM_SPEC],
        out_specs=VMEM_SPEC,
        scratch_shapes=RelayGather.semaphores(n),
        compiler_params=communicating(call_id),
    )(x)


def gather_first_kernel(x_ref, gains_ref, o_ref, all_gains, gain_send, gain_recv, *sems):
    greet("seq", "fsdp")
    place = lax.axis_index("fsdp")
    gain_copies = start_to_peers(
        "fsdp", lambda peer: gains_ref, lambda step: all_gains.at[place], gain_send, gain_recv
    )
    relay = gather_by_rows(x_ref, o_ref, sems)
    relay.start()
    o_ref[block_of(lax.axis_index("seq"), x_ref.shape[0]), :] = x_ref[...]
    all_gains[place] = gains_ref[...]
    relay.forward()
    relay.finish()
    for copy in gain_copies:
        copy.wait()


def gather_first(x, gains, n, shards, call_id):
    rows, width = x.shape
    return pl.pallas_call(
        gather_first_kernel,
        out_shape=(
            jax.ShapeDtypeStruct((n * rows, width), x.dtype),
            jax.ShapeDtypeStruct((shards,) + gains.shape, gains.dtype),
        ),
        in_specs=[VMEM_SPEC, VMEM_SPEC],
        out_specs=(VMEM_SPEC, VMEM_SPEC),
        scratch_shapes=semaphores(shards - 1, shards - 1) + RelayGather.semaphores(n),
        compiler_params=communicating(call_id),
        name="gather_first",
    )(x, gains)


def scatter_kernel(p_ref, o_ref, *scratch):
    greet("seq")
    relay = RelayScatter(p_ref, scratch[:6], scratch[6:])
    relay.start()
    relay.forward(o_ref)
    relay.finish(o_ref)


def scatter_sum(partial, n, call_id):
    total, width = partial.shape
    rows = total // n
    return pl.pallas_call(
        scatter_kernel,
        out_shape=jax.ShapeDtypeStruct((rows, width), F32),
        in_specs=[VMEM_SPEC],
        out_specs=VMEM_SPEC,
        scratch_shapes=RelayScatter.scratch(n, rows, width),
        compiler_params=communicating(call_id),
    )(partial)


def scatter_last_kernel(
    p_ref, small_ref, o_ref, small_out, part_landed, part_sum, row_landed,
    part_send, part_recv, row_send, row_recv, *scratch,
):
    greet("seq", "fsdp")
    part_copies = start_to_peers(
        "fsdp",
        lambda peer: small_ref.at[peer],
        lambda step: part_landed.at[step - 1],
        part_send,
        part_recv,
    )
    relay = RelayScatter(p_ref, scratch[:6], scratch[6:])
    relay.start()
    total = small_ref[lax.axis_index("fsdp")]
    for step, copy in enumerate(part_copies):
        copy.wait()
        total = total + part_landed[step]
    part_sum[...] = total
    relay.forward(o_ref)
    row_copies = start_to_peers(
        "seq", lambda peer: part_sum, lambda step: row_landed.at[step - 1], row_send, row_recv
    )
    relay.finish(o_ref)
    for step, copy in enumerate(row_copies):
        copy.wait()
        total = total + row_landed[step]
    small_out[...] = total


def scatter_last(partial, small, n, shards, call_id):
    total, width = partial.shape
    rows = total // n
    piece = small.shape[1:]
    return pl.pallas_call(
        scatter_last_kernel,
        out_shape=(jax.ShapeDtypeStruct((rows, width), F32), jax.ShapeDtypeStruct(piece, F32)),
        in_specs=[VMEM_SPEC] * 2,
        out_specs=(VMEM_SPEC,) * 2,
        scratch_shapes=[
            pltpu.VMEM((shards - 1,) + piece, F32),
            pltpu.VMEM(piece, F32),
            pltpu.VMEM((n - 1,) + piece, F32),
        ]
        + semaphores(shards - 1, shards - 1, n - 1, n - 1)
        + RelayScatter.scratch(n, rows, width),
        compiler_params=communicating(call_id),
        name="scatter_last",
    )(partial, small)


def finish_kernel(
    qkv_ref, joined_ref, qkv_all, out_all, out_landed, out_mine,
    first_send, first_recv, second_send, second_recv, *sems,
):
    greet("seq")
    me = lax.axis_index("seq")
    piece = out_mine.shape[0]
    first = start_to_peers(
        "seq",
        lambda peer: joined_ref.at[block_of(peer, piece)],
        lambda step: out_landed.at[step - 1],
        first_send,
        first_recv,
    )
    qkv = gather_by_columns(qkv_ref, qkv_all, sems)
    qkv.start()
    qkv_all[me] = qkv_ref[...]
    total = joined_ref[block_of(me, piece), :].astype(F32)
    for step, copy in enumerate(first):
        copy.wait()
        total = total + out_landed[step].astype(F32)
    out_mine[...] = total.astype(BF16)
    qkv.forward()
    mine = block_of(me, piece)
    second = start_to_peers(
        "seq", lambda peer: out_mine, lambda step: out_all.at[mine], second_send, second_recv
    )
    out_all[mine, :] = out_mine[...]
    qkv.finish()
    for copy in second:
        copy.wait()


def finish(qkv, joined, out_rows, n, call_id):
    width = joined.shape[1]
    return pl.pallas_call(
        finish_kernel,
        out_shape=(
            jax.ShapeDtypeStruct((n,) + qkv.shape, BF16),
            jax.ShapeDtypeStruct((out_rows, width), BF16),
        ),
        in_specs=[VMEM_SPEC] * 2,
        out_specs=(VMEM_SPEC,) * 2,
        scratch_shapes=[
            pltpu.VMEM((n - 1, out_rows // n, width), BF16),
            pltpu.VMEM((out_rows // n, width), BF16),
        ]
        + semaphores(*([n - 1] * 4))
        + RelayGather.semaphores(n),
        compiler_params=communicating(call_id),
        name="finish",
    )(qkv, joined)


def widen_kernel(qkv_ref, out_ref, q_final, k_final, v_final, out_final):
    n = qkv_ref.shape[0]
    split = q_final.shape[1] // n
    narrow = k_final.shape[1] // n
    for owner in range(n):
        values = qkv_ref[owner].astype(F32)
        q_final[:, owner * split : (owner + 1) * split] = values[:, :split]
        k_final[:, owner * narrow : (owner + 1) * narrow] = values[:, split : split + narrow]
        v_final[:, owner * narrow : (owner + 1) * narrow] = values[:, split + narrow :]
    out_final[...] = out_ref[...].astype(F32)


def widen(qkv_all, out_all, widths):
    n, rows, _ = qkv_all.shape
    steps = 4

    def by_rows(shape):
        return pl.BlockSpec((shape[0] // steps, shape[1]), lambda i: (i, 0))

    qkv_spec = pl.BlockSpec((n, rows // steps, qkv_all.shape[2]), lambda i: (0, i, 0))
    shapes = [(rows, size) for size in widths]
    return pl.pallas_call(
        widen_kernel,
        grid=(steps,),
        out_shape=tuple(
            jax.ShapeDtypeStruct(shape, F32) for shape in shapes + [out_all.shape]
        ),
        in_specs=[qkv_spec, by_rows(out_all.shape)],
        out_specs=tuple(by_rows(shape) for shape in shapes) + (by_rows(out_all.shape),),
        name="widen",
    )(qkv_all, out_all)


def owner_of(me_ref, step, n):
    return lax.rem(me_ref[0] + n - step, n)


def spread_kernel(n, hidden_piece, me_ref, *refs):
    steps, (gate_ref, up_ref, pieces) = refs[:n], refs[n:]
    for step, piece in enumerate(steps):
        pieces[owner_of(me_ref, step, n)] = piece[...]
    units = pieces.shape[2] // 2
    span = n * hidden_piece
    for target, base in ((gate_ref, 0), (up_ref, units)):
        for shard in range(units // hidden_piece):
            at = base + shard * hidden_piece
            target[:, shard * span : (shard + 1) * span] = jnp.concatenate(
                [pieces[s, :, at : at + hidden_piece].astype(F32) for s in range(n)], axis=1
            )


SMEM_SPEC = pl.BlockSpec(memory_space=pltpu.SMEM)


def spread_back(steps, me, hidden_piece):
    n = len(steps)
    rows, width = steps[0].shape
    shape = jax.ShapeDtypeStruct((rows, n * width // 2), F32)
    return pl.pallas_call(
        functools.partial(spread_kernel, n, hidden_piece),
        out_shape=(shape, shape),
        in_specs=[SMEM_SPEC] + [VMEM_SPEC] * n,
        out_specs=(VMEM_SPEC, VMEM_SPEC),
        scratch_shapes=[pltpu.VMEM((n, rows, width), BF16)],
        name="spread_back",
    )(me.reshape(1), *steps)


def below_kernel(n, me_ref, *refs):
    steps, target = refs[:n], refs[n]
    for step, piece in enumerate(steps):
        target[owner_of(me_ref, step, n)] = piece[...].astype(F32)


def below_each_other(steps, me):
    n = len(steps)
    rows, width = steps[0].shape
    return pl.pallas_call(
        functools.partial(below_kernel, n),
        out_shape=jax.ShapeDtypeStruct((n, rows, width), F32),
        in_specs=[SMEM_SPEC] + [VMEM_SPEC] * n,
        out_specs=VMEM_SPEC,
        name="below_each_other",
    )(me.reshape(1), *steps).reshape(n * rows, width)


def rope(values, cosine, sine):
    return values * cosine + pltpu.roll(values, HEAD_SIZE // 2, 1) * sine


def rope_back(grad, cosine, sine):
    return grad * cosine - pltpu.roll(grad, HEAD_SIZE // 2, 1) * sine


def head_columns(index):
    return pl.ds(pl.multiple_of(index * HEAD_SIZE, HEAD_SIZE), HEAD_SIZE)


def turned_block(shift):
    def block(i):
        return lax.rem(lax.axis_index("seq") + shift + i, lax.axis_size("seq"))

    return block


def forward_kernel(
    q_pre, k_pre, v_ref, gain_q, gain_k, cos_q, sin_q, cos_k, sin_k, place_k, place_q, start_q, cot,
    out_ref, p_ref, q_ref, k_ref, cot_all,
    v_turned, outs, cot_local, send, recv, local, *cot_sems,
):
    i, head = pl.program_id(0), pl.program_id(1)
    n, heads = pl.num_programs(0), pl.num_programs(1)
    seq = lax.axis_size("seq")
    me = lax.axis_index("seq")
    kv = outs.shape[1] // GROUP
    rows = cot.shape[0]
    mine = block_of(me, rows)

    cot_relay = gather_by_rows(cot, cot_all, cot_sems)
    cot_own = pltpu.make_async_copy(cot, cot_all.at[mine], cot_local)

    def out_copy(step, which):
        return pltpu.make_async_remote_copy(
            src_ref=outs.at[step, which],
            dst_ref=out_ref.at[:, head_columns(me * heads + which)],
            send_sem=send.at[step, which],
            recv_sem=recv.at[step, which],
            device_id={"seq": lax.rem(me + 1 + step, seq)},
            device_id_type=MESH,
        )

    def own_copy(which):
        return pltpu.make_async_copy(
            outs.at[seq - 1, which], out_ref.at[:, head_columns(me * heads + which)], local.at[which]
        )

    @pl.when((i == 0) & (head == 0))
    def _():
        greet("seq")
        cot_relay.start()
        cot_own.start()
        for which in range(kv):
            own = pl.ds(which * HEAD_SIZE, HEAD_SIZE)
            pre = k_pre[:, own]
            k_ref[:, own] = rope(
                pre * inverse_rms(pre) * gain_k[...], cos_k[...], sin_k[...]
            ).astype(BF16)
            v_turned[which] = v_ref[:, own].astype(F32).T.astype(BF16)

    @pl.when((i == n // 2) & (head == 0))
    def _():
        cot_relay.forward()

    @pl.when((head > 0) & (i < n - 1))
    def _():
        out_copy(i, head - 1).start()

    @pl.when((head == 0) & (i > 0))
    def _():
        out_copy(i - 1, heads - 1).start()

    pre = q_pre[...]
    query = rope(pre * inverse_rms(pre) * gain_q[...], cos_q[...], sin_q[...]).astype(BF16)
    q_ref[...] = query
    pair = head // GROUP
    scores = back_matmul(k_ref[:, head_columns(pair)], query) * SCALE
    keys = place_k[...]
    allowed = (keys <= place_q[...]) & (keys >= start_q[...])
    scores = jnp.where(allowed, scores, MASKED)
    top = jnp.max(scores, axis=0, keepdims=True)
    weights = jnp.exp(scores - top)
    total = jnp.sum(weights, axis=0, keepdims=True)
    weights = (weights * (1.0 / total)).astype(BF16)
    p_ref[0] = weights
    outs[i, head] = matrix_product(v_turned[pair], weights).T.astype(BF16)

    @pl.when((i == n - 1) & (head == heads - 1))
    def _():
        for which in range(outs.shape[1]):
            own_copy(which).start()
        cot_relay.finish()
        cot_own.wait()
        for step in range(seq - 1):
            for which in range(outs.shape[1]):
                out_copy(step, which).wait()
        for which in range(outs.shape[1]):
            own_copy(which).wait()


def attend_forward(
    q_pre, k_pre, value, gain_q, gain_k, cosine, sine, place, start, cotangent, n, call_id
):
    rows = q_pre.shape[0]
    heads = q_pre.shape[1] // HEAD_SIZE
    kv = heads // GROUP
    block = rows // n
    width = cotangent.shape[1]
    turn = turned_block(1)
    q_spec = pl.BlockSpec((block, HEAD_SIZE), lambda i, h: (turn(i), h))
    k_spec = pl.BlockSpec((rows, kv * HEAD_SIZE), lambda i, h: (0, 0))
    gain_spec = pl.BlockSpec((1, HEAD_SIZE), lambda i, h: (0, 0))
    trig_q = pl.BlockSpec((block, HEAD_SIZE), lambda i, h: (turn(i), 0))
    trig_k = pl.BlockSpec((rows, HEAD_SIZE), lambda i, h: (0, 0))
    column = pl.BlockSpec((rows, 1), lambda i, h: (0, 0))
    row = pl.BlockSpec((1, block), lambda i, h: (0, turn(i)))
    return pl.pallas_call(
        forward_kernel,
        grid=(n, heads),
        out_shape=(
            jax.ShapeDtypeStruct((block, n * heads * HEAD_SIZE), BF16),
            jax.ShapeDtypeStruct((heads, rows, rows), BF16),
            jax.ShapeDtypeStruct((rows, heads * HEAD_SIZE), BF16),
            jax.ShapeDtypeStruct((rows, kv * HEAD_SIZE), BF16),
            jax.ShapeDtypeStruct((rows, width), BF16),
        ),
        in_specs=[
            q_spec, k_spec, k_spec, gain_spec, gain_spec, trig_q, trig_q, trig_k, trig_k,
            column, row, row, ANY_SPEC,
        ],
        out_specs=(
            ANY_SPEC,
            pl.BlockSpec((1, rows, block), lambda i, h: (h, 0, turn(i))),
            q_spec,
            k_spec,
            ANY_SPEC,
        ),
        scratch_shapes=[
            pltpu.VMEM((kv, HEAD_SIZE, rows), BF16),
            pltpu.VMEM((n, heads, block, HEAD_SIZE), BF16),
            pltpu.SemaphoreType.DMA,
            pltpu.SemaphoreType.DMA((n - 1, heads)),
            pltpu.SemaphoreType.DMA((n - 1, heads)),
            pltpu.SemaphoreType.DMA((heads,)),
        ]
        + RelayGather.semaphores(n),
        compiler_params=communicating(call_id),
        name="attend_forward",
    )(
        q_pre, k_pre, value, gain_q, gain_k, cosine, sine, cosine, sine,
        place[:, None], place[None, :], start[None, :], cotangent,
    )


def backward_kernel(
    p_ref, q_ref, k_ref, v_ref, q_pre, k_pre, gain_q, gain_k, cos_q, sin_q, cos_k, sin_k,
    grad_own, bulk,
    dqkv_ref, dgain_q, dgain_k, bulk_sum,
    k_turned, dk_sum, dv_sum, grads, send, recv, local, *scratch,
):
    i, head = pl.program_id(0), pl.program_id(1)
    n, heads = pl.num_programs(0), pl.num_programs(1)
    seq = lax.axis_size("seq")
    me = lax.axis_index("seq")
    kv = k_turned.shape[0]
    rows = grads.shape[1]
    span = grads.shape[2]
    first = (i == 0) & (head == 0)
    last = (i == n - 1) & (head == heads - 1)

    def grad_copy(step):
        peer = lax.rem(me + step, seq)
        return pltpu.make_async_remote_copy(
            src_ref=grad_own.at[:, block_of(peer, span)],
            dst_ref=grads.at[step],
            send_sem=send.at[step - 1],
            recv_sem=recv.at[step - 1],
            device_id={"seq": peer},
            device_id_type=MESH,
        )

    bulk_relay = RelayScatter(bulk, scratch[:6], scratch[6:])
    own_copy = pltpu.make_async_copy(grad_own.at[:, block_of(me, span)], grads.at[0], local)

    @pl.when(first)
    def _():
        greet("seq")
        own_copy.start()
        for step in range(1, seq):
            grad_copy(step).start()
        bulk_relay.start()
        dgain_q[...] = jnp.zeros_like(dgain_q)
        dgain_k[...] = jnp.zeros_like(dgain_k)
        dk_sum[...] = jnp.zeros_like(dk_sum)
        dv_sum[...] = jnp.zeros_like(dv_sum)
        for which in range(kv):
            own = pl.ds(which * HEAD_SIZE, HEAD_SIZE)
            k_turned[which] = k_ref[:, own].astype(F32).T.astype(BF16)
        own_copy.wait()

    for step in range(1, seq):
        @pl.when((head == 0) & (i == seq - step))
        def _():
            grad_copy(step).wait_recv()

    @pl.when((i == n - 1) & (head == 0))
    def _():
        bulk_relay.forward(bulk_sum)

    slot = lax.rem(seq - i, seq)
    pair = head // GROUP
    rounded = p_ref[0]
    weights = rounded.astype(F32)
    grad = grads[slot, :, head_columns(head)]
    grad_weights = back_matmul(v_ref[:, head_columns(pair)], grad)
    delta = jnp.sum(weights * grad_weights, axis=0, keepdims=True)
    grad_scores = (weights * (grad_weights - delta)).astype(BF16)
    dk_sum[pair] += matrix_product(grad_scores, q_ref[...])
    dv_sum[pair] += matrix_product(rounded, grad)
    dq = (matrix_product(k_turned[pair], grad_scores).T * SCALE).astype(BF16).astype(F32)
    dq, gain_rows = rms_backward(q_pre[...], gain_q[...], rope_back(dq, cos_q[...], sin_q[...]))
    block = block_of(lax.rem(me + i, seq), rows)
    dqkv_ref[block, head_columns(head)] = dq.astype(BF16)
    dgain_q[...] += jnp.sum(gain_rows, axis=0, keepdims=True)

    @pl.when(last)
    def _():
        for which in range(kv):
            own = pl.ds(which * HEAD_SIZE, HEAD_SIZE)
            dk = (dk_sum[which] * SCALE).astype(BF16).astype(F32)
            dk, gain_rows = rms_backward(
                k_pre[:, own], gain_k[...], rope_back(dk, cos_k[...], sin_k[...])
            )
            dqkv_ref[:, head_columns(heads + which)] = dk.astype(BF16)
            dgain_k[...] += jnp.sum(gain_rows, axis=0, keepdims=True)
            dqkv_ref[:, head_columns(heads + kv + which)] = dv_sum[which].astype(BF16)
        for step in range(1, seq):
            grad_copy(step).wait_send()
        bulk_relay.finish(bulk_sum)


def attend_backward(
    weights, query, key, value, grad_own, bulk, q_pre, k_pre, gain_q, gain_k, cosine, sine, n, call_id
):
    rows = q_pre.shape[0]
    heads = q_pre.shape[1] // HEAD_SIZE
    kv = heads // GROUP
    block = rows // n
    turn = turned_block(0)
    q_spec = pl.BlockSpec((block, HEAD_SIZE), lambda i, h: (turn(i), h))
    k_spec = pl.BlockSpec((rows, kv * HEAD_SIZE), lambda i, h: (0, 0))
    gain_spec = pl.BlockSpec((1, HEAD_SIZE), lambda i, h: (0, 0))
    trig_q = pl.BlockSpec((block, HEAD_SIZE), lambda i, h: (turn(i), 0))
    trig_k = pl.BlockSpec((rows, HEAD_SIZE), lambda i, h: (0, 0))
    return pl.pallas_call(
        backward_kernel,
        grid=(n, heads),
        out_shape=(
            jax.ShapeDtypeStruct((rows, (heads + 2 * kv) * HEAD_SIZE), BF16),
            jax.ShapeDtypeStruct((1, HEAD_SIZE), F32),
            jax.ShapeDtypeStruct((1, HEAD_SIZE), F32),
            jax.ShapeDtypeStruct((block, bulk.shape[1]), F32),
        ),
        in_specs=[
            pl.BlockSpec((1, rows, block), lambda i, h: (h, 0, turn(i))),
            q_spec, k_spec, k_spec, q_spec, k_spec, gain_spec, gain_spec,
            trig_q, trig_q, trig_k, trig_k, ANY_SPEC,
            pl.BlockSpec(bulk.shape, lambda i, h: (0, 0)),
        ],
        out_specs=(
            pl.BlockSpec((rows, (heads + 2 * kv) * HEAD_SIZE), lambda i, h: (0, 0)),
            gain_spec, gain_spec,
            pl.BlockSpec((block, bulk.shape[1]), lambda i, h: (0, 0)),
        ),
        scratch_shapes=[
            pltpu.VMEM((kv, HEAD_SIZE, rows), BF16),
            pltpu.VMEM((kv, rows, HEAD_SIZE), F32),
            pltpu.VMEM((kv, rows, HEAD_SIZE), F32),
            pltpu.VMEM((n, block, heads * HEAD_SIZE), BF16),
            pltpu.SemaphoreType.DMA((n - 1,)),
            pltpu.SemaphoreType.DMA((n - 1,)),
            pltpu.SemaphoreType.DMA,
        ]
        + RelayScatter.scratch(n, block, bulk.shape[1]),
        compiler_params=communicating(call_id),
        name="attend_backward",
    )(
        weights, query, key, value, q_pre, k_pre, gain_q, gain_k, cosine, sine, cosine, sine,
        grad_own, bulk,
    )


def on_device(
    tokens, lengths, packing, norm_in, w_query, key_projection, value_projection, norm_query,
    norm_key, w_out, norm_post, w_gate, w_up, w_down, cotangent,
):
    n = lax.axis_size("seq")
    shards = lax.axis_size("fsdp")
    me = lax.axis_index("seq")
    resident = tokens.shape[1]
    width = tokens.shape[2]
    rows = resident * n
    heads = HQ // n
    kv = KEY_VALUE_HEADS // n
    hidden_piece = w_down.shape[0] // n

    def columns(weight, pieces):
        size = weight.shape[1] // pieces
        return lax.dynamic_slice_in_dim(weight, me * size, size, axis=1)

    def spread_columns(weight):
        pieces = weight.reshape(weight.shape[0], shards, n, hidden_piece)
        return lax.dynamic_index_in_dim(pieces, me, axis=2, keepdims=False).reshape(
            weight.shape[0], shards * hidden_piece
        )

    def tile_of(values):
        pad = 1024 - values.shape[-1]
        values = jnp.concatenate([values, jnp.zeros(values.shape[:-1] + (pad,), F32)], axis=-1)
        return values.reshape(values.shape[:-1] + (8, 128))

    part, small = norm_in.shape[0], norm_query.shape[0]
    whole, gains = gather_first(
        tokens[0],
        tile_of(jnp.concatenate([norm_in, norm_post, norm_query, norm_key]).astype(F32)),
        n, shards, 0,
    )
    gains = gains.reshape(shards, -1)
    gain_in = gains[:, :part].reshape(1, -1)
    gain_post = gains[:, part : 2 * part].reshape(1, -1)
    gain_query = gains[:, 2 * part : 2 * part + small].reshape(1, -1)
    gain_key = gains[:, 2 * part + small : 2 * part + 2 * small].reshape(1, -1)

    def gathered(*weights):
        sizes = [weight.shape[0] for weight in weights]
        if len({weight.shape[1] for weight in weights}) > 1:
            return [lax.all_gather(weight, "fsdp", axis=0, tiled=True) for weight in weights]
        joined = lax.all_gather(jnp.concatenate(weights, axis=0), "fsdp", axis=0)
        starts = [sum(sizes[:i]) for i in range(len(sizes))]
        return [
            joined[:, start : start + size].reshape(-1, joined.shape[2])
            for start, size in zip(starts, sizes)
        ]

    qkv_weight, down_weight = gathered(
        jnp.concatenate(
            [columns(w_query, n), columns(key_projection, n), columns(value_projection, n)], axis=1
        ),
        lax.dynamic_slice_in_dim(w_down, me * hidden_piece, hidden_piece, axis=0),
    )
    out_weight = lax.all_gather(w_out, "fsdp", axis=0, tiled=True)
    gate_up_weight = lax.all_gather(
        jnp.concatenate([spread_columns(w_gate), spread_columns(w_up)], axis=1), "fsdp", axis=0, tiled=True
    )

    order = packing[0]
    places = jnp.arange(rows, dtype=jnp.int32)
    place = jnp.sum(jnp.where(order[None, :] == places[:, None], places[None, :], 0), axis=1)
    ends = jnp.cumsum(lengths[0])
    start = jnp.sum(jnp.where(place[:, None] >= ends[None, :], lengths[0][None, :], 0), axis=1)
    half = HEAD_SIZE // 2
    inv_freq = ROPE_BASE ** (-jnp.arange(half, dtype=F32) / half)
    angles = (place - start).astype(F32)[:, None] * inv_freq[None, :]
    cosine, sine = jnp.cos(angles), jnp.sin(angles)
    cosine = jnp.concatenate([cosine, cosine], axis=1)
    sine = jnp.concatenate([-sine, sine], axis=1)

    inputs = tokens[0].astype(F32)
    whole_f32 = whole.astype(F32)
    unit = whole_f32 * inverse_rms(whole_f32)
    normalized = (unit * gain_in).astype(BF16)
    qkv = matrix_product(normalized, qkv_weight)
    split = heads * HEAD_SIZE
    q_pre = qkv[:, :split]
    k_pre = qkv[:, split : split + kv * HEAD_SIZE]
    value = qkv[:, split + kv * HEAD_SIZE :].astype(BF16)
    attended, weights, query, key, grad_mlp = attend_forward(
        q_pre, k_pre, value, gain_query, gain_key, cosine, sine, place, start, cotangent[0], n, 1
    )
    middle = inputs + matrix_product(attended, out_weight)
    normed_post_mine = (middle * inverse_rms(middle) * gain_post).astype(BF16)
    normed_post = gather_rows(normed_post_mine, n, 2)

    grad_hidden = lax.optimization_barrier(back_matmul(grad_mlp, down_weight))
    gate_up = matrix_product(normed_post, gate_up_weight)
    units = shards * hidden_piece
    gate, up = gate_up[:, :units], gate_up[:, units:]
    logistic = 1.0 / (1.0 + jnp.exp(-gate))
    hidden = (gate / (1.0 + jnp.exp(-gate)) * up).astype(BF16)
    grad_gate = (grad_hidden * up * (logistic + gate * logistic * (1.0 - logistic))).astype(BF16)
    grad_up = (grad_hidden * gate * logistic).astype(BF16)
    grad_gate_up = jnp.concatenate([grad_gate, grad_up], axis=1)
    grad_gate_up_weight = outer_sum(normed_post, grad_gate_up).astype(BF16)
    grad_gate_up_weight, grad_gate_up, hidden = lax.optimization_barrier(
        (grad_gate_up_weight, grad_gate_up, hidden)
    )
    mlp_partial = matrix_product(hidden, down_weight).astype(BF16)
    grad_partial, grad_down = lax.optimization_barrier(
        (
            back_matmul(grad_gate_up, gate_up_weight).astype(BF16),
            outer_sum(hidden, grad_mlp).astype(BF16),
        )
    )
    gate_up_share = lax.psum_scatter(grad_gate_up_weight, "fsdp", scatter_dimension=0, tiled=True)
    grad_normed_post = scatter_sum(grad_partial, n, 3)
    grad_middle, gain_rows = rms_backward(middle, gain_post, grad_normed_post)
    grad_middle = cotangent[0].astype(F32) + grad_middle
    grad_gain_post = jnp.sum(gain_rows, axis=0)
    grad_branch = grad_middle.astype(BF16)
    grad_out = outer_sum(attended, grad_branch).astype(BF16)
    out_down_share = lax.psum_scatter(
        jnp.concatenate(
            [grad_out.reshape(shards, -1, width), grad_down.reshape(shards, -1, width)], axis=1
        ).reshape(-1, width),
        "fsdp", scatter_dimension=0, tiled=True,
    )
    grad_attended = back_matmul(grad_branch, out_weight).astype(BF16)
    grad_qkv, grad_gain_query, grad_gain_key, mlp_sum = attend_backward(
        weights, query, key, value, grad_attended, mlp_partial, q_pre, k_pre, gain_query,
        gain_key, cosine, sine, n, 4,
    )
    output = (middle + mlp_sum).astype(BF16)[None]
    grad_qkv_weight = outer_sum(normalized, grad_qkv).astype(BF16)
    qkv_share = lax.psum_scatter(grad_qkv_weight, "fsdp", scatter_dimension=0, tiled=True)
    gate_up_share, _ = lax.optimization_barrier((gate_up_share, grad_qkv))
    gate_up_all = [gate_up_share]
    for step in range(1, n):
        pairs = [(i, (i + step) % n) for i in range(n)]
        gate_up_all.append(lax.ppermute(gate_up_share, "seq", pairs))
    partial = back_matmul(grad_qkv, qkv_weight)
    grad_gain_in = jnp.sum(partial * unit, axis=0)
    small_grads = [grad_gain_in, grad_gain_post, grad_gain_query, grad_gain_key]
    small_grads = tile_of(jnp.concatenate([g.reshape(shards, -1) for g in small_grads], axis=1))
    grad_normed, gain_shares = scatter_last(
        partial.astype(BF16), small_grads, n, shards, 5
    )
    down_share, _ = lax.optimization_barrier((out_down_share[w_out.shape[0] :], gain_shares))
    down_all = [down_share]
    for step in range(1, n):
        pairs = [(i, (i + step) % n) for i in range(n)]
        down_all.append(lax.ppermute(down_share, "seq", pairs))
    gain_shares = gain_shares.reshape(-1)
    grad_inputs, _ = rms_backward(inputs, gain_in, grad_normed)
    input_grad = (grad_middle + grad_inputs).astype(BF16)[None]

    final_gate, final_up = spread_back(gate_up_all, me, hidden_piece)
    qkv_all, out_all = finish(qkv_share, out_down_share, w_out.shape[0], n, 6)
    final_query, final_key, final_value, final_out = widen(
        qkv_all, out_all, (HQ * HEAD_SIZE,) + (KEY_VALUE_HEADS * HEAD_SIZE,) * 2
    )
    final_down = below_each_other(down_all, me)

    return (
        output,
        input_grad,
        gain_shares[:part],
        final_query,
        final_key,
        final_value,
        gain_shares[2 * part : 2 * part + small],
        gain_shares[2 * part + small : 2 * part + 2 * small],
        final_out,
        gain_shares[part : 2 * part],
        final_gate,
        final_up,
        final_down,
    )


def solution(mesh):
    flat, wide = P("fsdp"), P("fsdp", None)
    whole = P("fsdp", "seq", None)
    in_specs = (
        whole, wide, wide, flat, wide, wide, wide, flat, flat, wide, flat, wide, wide, wide, whole,
    )
    out_specs = (whole, whole, flat, wide, wide, wide, flat, flat, wide, flat, wide, wide, wide)

    return jax.shard_map(
        on_device, mesh=mesh, in_specs=in_specs, out_specs=out_specs, check_vma=False
    )
```
